8 devices in a mesh: dp: 1 (over z), cpo: 2 (over y), cp: 4 (over x, core).
Axes of the slice: x: 2, y: 2, z: 1, core: 2. Of those that a mesh axis runs over, the one named last changes fastest.
Arguments:
- queries: bfloat16 [4096, 2, 128], P(('dp', 'cpo', 'cp'))
- keys: bfloat16 [4096, 128], P(('dp', 'cpo', 'cp'))
- values: bfloat16 [4096, 128], P(('dp', 'cpo', 'cp'))
- attn_out: bfloat16 [4096, 2, 128], P(('dp', 'cpo', 'cp'))
- logsumexp: float32 [4096, 2], P(('dp', 'cpo', 'cp'))
- d_out: bfloat16 [4096, 2, 128], P(('dp', 'cpo', 'cp'))
- cu_seqlens: int32 [14], P('dp')
Outputs:
- output 1: bfloat16 [4096, 2, 128], P(('dp', 'cpo', 'cp'))
- output 2: bfloat16 [4096, 128], P(('dp', 'cpo', 'cp'))
- output 3: bfloat16 [4096, 128], P(('dp', 'cpo', 'cp'))
All inputs are finite; a program needn't handle non-finite values.
Results may differ from the reference program's by a relative error of at most 0.001.
Values are sent between devices in bfloat16 or wider.
A program may use at most 1 GiB of HBM per device.

```python
import jax
import jax.numpy as jnp
from jax import lax

CHUNK = 512
GROUP = 8
QHEADS = 2
HEAD_DIM = 128
HOPS = 3
QROWS = 64
SEQ = GROUP * CHUNK
NCUT_RAND = GROUP
NCUT_GRID = GROUP // 3 + 2


def doc_ids(bounds, positions):
    found = jnp.searchsorted(bounds[1:], positions, side="right").astype(jnp.int32)
    return jnp.where((positions >= 0) & (positions < SEQ), found, -1)


def draw_bounds(key):
    key_phase, key_slot, key_cuts = jax.random.split(key, 3)
    span_len = HOPS * CHUNK
    phase = jax.random.randint(key_phase, (), 0, span_len, dtype=jnp.int32)
    grid_cuts = jnp.minimum(phase + span_len * jnp.arange(NCUT_GRID, dtype=jnp.int32), SEQ)
    slot_count = (SEQ - phase) // span_len
    slot = jax.random.randint(key_slot, (), 0, slot_count, dtype=jnp.int32)
    long_start = phase + span_len * slot
    free_cuts = jax.random.randint(key_cuts, (NCUT_RAND,), 1, SEQ, dtype=jnp.int32)
    inside = (free_cuts > long_start) & (free_cuts < long_start + span_len)
    free_cuts = jnp.where(inside, 0, free_cuts)
    every_cut = jnp.concatenate([jnp.zeros((1,), jnp.int32), grid_cuts, free_cuts, jnp.full((1,), SEQ, jnp.int32)])
    return jnp.sort(every_cut).astype(jnp.int32)


def attend_forward(queries, keys, values, ids):
    scale = HEAD_DIM ** -0.5
    span_len = HOPS * CHUNK
    width = span_len + QROWS
    key_pad = jnp.concatenate([jnp.zeros((span_len, HEAD_DIM), jnp.float32), keys.astype(jnp.float32)])
    val_pad = jnp.concatenate([jnp.zeros((span_len, HEAD_DIM), jnp.float32), values.astype(jnp.float32)])
    id_pad = jnp.concatenate([jnp.full((span_len,), -1, jnp.int32), ids])

    def block_fwd(start):
        q_blk = lax.dynamic_slice_in_dim(queries, start, QROWS).astype(jnp.float32)
        id_q = lax.dynamic_slice_in_dim(ids, start, QROWS)
        pos_q = start + jnp.arange(QROWS, dtype=jnp.int32)
        k_blk = lax.dynamic_slice_in_dim(key_pad, start, width)
        v_blk = lax.dynamic_slice_in_dim(val_pad, start, width)
        id_k = lax.dynamic_slice_in_dim(id_pad, start, width)
        pos_k = start - span_len + jnp.arange(width, dtype=jnp.int32)
        keep = (id_q[:, None] == id_k[None, :]) & (pos_k[None, :] <= pos_q[:, None])
        scores = scale * jnp.einsum("qgd,kd->qgk", q_blk, k_blk)
        scores = jnp.where(keep[:, None, :], scores, -1e30)
        top_val = jnp.max(scores, axis=-1, keepdims=True)
        exp_scores = jnp.where(keep[:, None, :], jnp.exp(scores - top_val), 0.0)
        denom = jnp.sum(exp_scores, axis=-1, keepdims=True)
        out_blk = jnp.einsum("qgk,kd->qgd", exp_scores, v_blk) / denom
        return out_blk.astype(jnp.bfloat16), (top_val + jnp.log(denom))[:, :, 0]

    starts = jnp.arange(SEQ // QROWS, dtype=jnp.int32) * QROWS
    out_all, lse_all = lax.map(block_fwd, starts)
    return out_all.reshape(SEQ, QHEADS, HEAD_DIM), lse_all.reshape(SEQ, QHEADS)


def setup_inputs(seed: int = 0, part: int = 0) -> dict:
    part_key = jax.random.fold_in(jax.random.key(seed), part)
    key_q, key_k, key_v, key_do, key_b = jax.random.split(part_key, 5)
    queries = jax.random.normal(key_q, (SEQ, QHEADS, HEAD_DIM), jnp.float32).astype(jnp.bfloat16)
    keys = jax.random.normal(key_k, (SEQ, HEAD_DIM), jnp.float32).astype(jnp.bfloat16)
    values = jax.random.normal(key_v, (SEQ, HEAD_DIM), jnp.float32).astype(jnp.bfloat16)
    d_out = jax.random.normal(key_do, (SEQ, QHEADS, HEAD_DIM), jnp.float32).astype(jnp.bfloat16)
    cu_seqlens = draw_bounds(key_b)
    ids = doc_ids(cu_seqlens, jnp.arange(SEQ, dtype=jnp.int32))
    attn_out, logsumexp = attend_forward(queries, keys, values, ids)
    return {"queries": queries, "keys": keys, "values": values, "attn_out": attn_out, "logsumexp": logsumexp, "d_out": d_out, "cu_seqlens": cu_seqlens}


def reference(queries, keys, values, attn_out, logsumexp, d_out, cu_seqlens):
    scale = HEAD_DIM ** -0.5
    span_len = HOPS * CHUNK
    width = span_len + QROWS
    ids = doc_ids(cu_seqlens, jnp.arange(SEQ, dtype=jnp.int32))
    id_pad = jnp.concatenate([jnp.full((span_len,), -1, jnp.int32), ids])
    key_pad = jnp.concatenate([jnp.zeros((span_len, HEAD_DIM), keys.dtype), keys])
    val_pad = jnp.concatenate([jnp.zeros((span_len, HEAD_DIM), values.dtype), values])
    row_dot = jnp.sum(d_out.astype(jnp.float32) * attn_out.astype(jnp.float32), axis=-1)

    def block_bwd(carry, start):
        dk_acc, dv_acc = carry
        q_blk = lax.dynamic_slice_in_dim(queries, start, QROWS).astype(jnp.float32)
        do_blk = lax.dynamic_slice_in_dim(d_out, start, QROWS).astype(jnp.float32)
        lse_blk = lax.dynamic_slice_in_dim(logsumexp, start, QROWS)
        dot_blk = lax.dynamic_slice_in_dim(row_dot, start, QROWS)
        id_q = lax.dynamic_slice_in_dim(ids, start, QROWS)
        pos_q = start + jnp.arange(QROWS, dtype=jnp.int32)
        k_blk = lax.dynamic_slice_in_dim(key_pad, start, width).astype(jnp.float32)
        v_blk = lax.dynamic_slice_in_dim(val_pad, start, width).astype(jnp.float32)
        id_k = lax.dynamic_slice_in_dim(id_pad, start, width)
        pos_k = start - span_len + jnp.arange(width, dtype=jnp.int32)
        keep = (id_q[:, None] == id_k[None, :]) & (pos_k[None, :] <= pos_q[:, None])
        scores = scale * jnp.einsum("qgd,kd->qgk", q_blk, k_blk)
        p_mat = jnp.where(keep[:, None, :], jnp.exp(scores - lse_blk[:, :, None]), 0.0)
        p_low = p_mat.astype(jnp.bfloat16).astype(jnp.float32)
        dp_mat = jnp.einsum("qgd,kd->qgk", do_blk, v_blk)
        ds_mat = (p_mat * (dp_mat - dot_blk[:, :, None])).astype(jnp.bfloat16).astype(jnp.float32)
        dq_blk = scale * jnp.einsum("qgk,kd->qgd", ds_mat, k_blk)
        dk_part = jnp.einsum("qgk,qgd->kd", ds_mat, q_blk)
        dv_part = jnp.einsum("qgk,qgd->kd", p_low, do_blk)
        dk_acc = lax.dynamic_update_slice_in_dim(dk_acc, lax.dynamic_slice_in_dim(dk_acc, start, width) + dk_part, start, axis=0)
        dv_acc = lax.dynamic_update_slice_in_dim(dv_acc, lax.dynamic_slice_in_dim(dv_acc, start, width) + dv_part, start, axis=0)
        return (dk_acc, dv_acc), dq_blk.astype(jnp.bfloat16)

    init = (jnp.zeros((SEQ + span_len, HEAD_DIM), jnp.float32), jnp.zeros((SEQ + span_len, HEAD_DIM), jnp.float32))
    starts = jnp.arange(SEQ // QROWS, dtype=jnp.int32) * QROWS
    (dk_acc, dv_acc), dq_all = lax.scan(block_bwd, init, starts)
    d_queries = dq_all.reshape(SEQ, QHEADS, HEAD_DIM)
    d_keys = (scale * dk_acc[span_len:]).astype(jnp.bfloat16)
    d_values = dv_acc[span_len:].astype(jnp.bfloat16)
    return d_queries, d_keys, d_values
```

```python
import functools
import math

import jax
import jax.numpy as jnp
from jax import lax
from jax.experimental import pallas as pl
from jax.experimental.pallas import tpu as pltpu
from jax.sharding import PartitionSpec as P

MESH = pl.DeviceIdType.MESH
HOPS = 3
NK = 2
NQ = 4
NONE = 31
NOBODY = 63
FINISH = 18

KV_OWN = {0: [(1, 1), (2, 2)], 1: [(3, 2), (4, 3)], 2: [(3, 1), (0, 1)], 3: [(6, 3)], 4: [(5, 1), (6, 2)], 5: [(7, 2)], 6: [(7, 1)], 7: []}
QD_OWN = {0: [], 1: [(0, 1)], 2: [(0, 2)], 3: [(2, 1), (1, 2)], 4: [(1, 3)], 5: [(4, 1), (7, 1)], 6: [(4, 2), (3, 3)], 7: [(6, 1), (5, 2)]}
KV_REL = {(0, 1): (4, 2), (2, 2): (3, 3), (3, 2): (2, 1), (4, 2): (5, 3), (4, 1): (5, 2), (6, 3): (4, 1), (6, 2): (7, 3), (7, 2): (6, 1)}
QD_REL = {(0, 2): (1, 1), (1, 2): (0, 3), (1, 3): (3, 1), (3, 1): (2, 2), (3, 2): (2, 3), (4, 2): (5, 1), (5, 2): (4, 3), (7, 1): (3, 2)}
ORDER = {
    0: "Q1.0 Q1.1 Q1.2 Q1.3 K1.0 Q3.0 K1.1 Q3.1 Q2.0 Q3.2 Q2.1 Q3.3 Q2.2 Q2.3",
    1: "K1.0 K1.1 F Q3.0 Q2.0 Q3.1 Q3.2 Q2.1 Q3.3 Q2.2 Q1.0 Q2.3 Q1.1 Q1.2 Q1.3",
    2: "Q1.0 Q1.1 Q1.2 Q1.3 K2.0 K1.0 K2.1 K1.1 F Q2.0 Q2.1 Q2.2 Q3.0 Q2.3 Q3.1 Q3.2 Q3.3",
    3: "K1.0 K1.1 Q3.0 K2.0 Q3.1 K3.0 Q3.2 K2.1 Q3.3 K3.1 F Q1.0 Q1.1 Q1.2 Q2.0 Q1.3 Q2.1 Q2.2 Q2.3",
    4: "Q1.0 Q1.1 Q1.2 Q1.3 K3.0 Q2.0 K3.1 Q3.0 Q2.1 K2.0 Q3.1 Q2.2 K2.1 Q3.2 Q2.3 Q3.3 K1.0 K1.1 F",
    5: "K1.0 K1.1 Q2.0 Q1.0 Q2.1 Q1.1 K3.0 Q2.2 Q1.2 K3.1 Q2.3 Q1.3 K2.0 K2.1 F",
    6: "Q1.0 Q1.1 Q1.2 Q1.3 K3.0 K2.0 K3.1 K1.0 K2.1 K1.1 F",
    7: "K1.0 K1.1 K2.0 K3.0 K2.1 K3.1 F Q1.0 Q1.1 Q1.2 Q1.3",
}


def step_codes(text):
    codes = []
    for word in text.split():
        if word == "F":
            codes.append(FINISH)
            continue
        hop, chunk = int(word[1]) - 1, int(word[3])
        codes.append(hop * NK + chunk if word[0] == "K" else 3 * NK + hop * NQ + chunk)
    return codes


def targets_of(table, pick):
    pairs = [table.get(pick(d), NOBODY) for d in range(8)]
    return [p if p == NOBODY else p[0] * 4 + p[1] for p in pairs]


def nth(table, n):
    return [NOBODY if len(table[d]) <= n else table[d][n][0] * 4 + table[d][n][1] for d in range(8)]


def partners():
    near = {d: set() for d in range(8)}
    for table in (KV_OWN, QD_OWN):
        for d, pairs in table.items():
            for target, _ in pairs:
                near[d].add(target)
                near[target].add(d)
    for table in (KV_REL, QD_REL):
        for (d, _), (target, _) in table.items():
            near[d].add(target)
            near[target].add(d)
    return near


def body(
    cu_ref, q_hbm, k_hbm, v_hbm, o_hbm, lse_hbm, do_hbm,
    dq_out, dk_out, dv_out,
    q_loc, k_loc, v_loc, o_loc, lse_loc, do_loc, stat_loc, starts,
    k_buf, v_buf, q_buf, do_buf, stat_buf,
    dqt, dk_acc, dv_acc, dq_st, dk_st, dv_st,
    in_sem, out_sem,
    k_recv, v_recv, q_recv, do_recv, stat_recv,
    k_own, v_own, q_own, do_own, stat_own,
    k_rel, v_rel, q_rel, do_rel, stat_rel,
):
    rows = k_loc.shape[0]
    qrows = q_loc.shape[0]
    head = k_loc.shape[1]
    kc_rows = rows // NK
    qc_rows = qrows // NQ
    scale = head ** -0.5
    factor = scale * math.log2(math.e)
    me = lax.axis_index("cpo") * 4 + lax.axis_index("cp")

    def lut(values):
        out = jnp.int32(values[0])
        for d in range(1, len(values)):
            out = jnp.where(me == d, jnp.int32(values[d]), out)
        return out

    def place(target):
        return {"cpo": target // 4, "cp": target % 4}

    loads = [
        pltpu.make_async_copy(src, dst, in_sem.at[i])
        for i, (src, dst) in enumerate(
            [(k_hbm, k_loc), (v_hbm, v_loc), (q_hbm, q_loc), (do_hbm, do_loc), (o_hbm, o_loc), (lse_hbm, lse_loc)]
        )
    ]
    for load in loads:
        load.start()

    barrier = pltpu.get_barrier_semaphore()
    near = partners()
    for d in range(8):
        @pl.when(me == d)
        def _(d=d):
            for other in sorted(near[d]):
                pl.semaphore_signal(barrier, inc=1, device_id=place(other), device_id_type=MESH)
    lane = lax.broadcasted_iota(jnp.int32, (1, qrows), 1) // 2
    for h in range(HOPS + 1):
        pos = lane + (me + h) * rows
        start = jnp.zeros_like(pos)
        for j in range(cu_ref.shape[0]):
            start = jnp.maximum(start, jnp.where(pos >= cu_ref[j], cu_ref[j], 0))
        starts[h] = start
    for d in range(8):
        @pl.when(me == d)
        def _(d=d):
            pl.semaphore_wait(barrier, len(near[d]))

    def kv_copies(src_k, src_v, sems_k, sems_v, code, slot, chunk):
        target, there = code // 4, code % 4 - 1
        part = pl.ds(chunk * kc_rows, kc_rows)
        return [
            pltpu.make_async_remote_copy(
                src_ref=src.at[part], dst_ref=buf.at[there, part], send_sem=sems.at[slot, chunk], recv_sem=recv.at[there, chunk],
                device_id=place(target), device_id_type=MESH)
            for src, buf, sems, recv in ((src_k, k_buf, sems_k, k_recv), (src_v, v_buf, sems_v, v_recv))
        ]

    def qd_copies(src_q, src_do, sems_q, sems_do, code, slot, chunk):
        target, there = code // 4, code % 4 - 1
        part = pl.ds(chunk * qc_rows, qc_rows)
        return [
            pltpu.make_async_remote_copy(
                src_ref=src.at[part], dst_ref=buf.at[there, part], send_sem=sems.at[slot, chunk], recv_sem=recv.at[there, chunk],
                device_id=place(target), device_id_type=MESH)
            for src, buf, sems, recv in ((src_q, q_buf, sems_q, q_recv), (src_do, do_buf, sems_do, do_recv))
        ]

    def stat_copy(src, sems, code, slot):
        target, there = code // 4, code % 4 - 1
        return pltpu.make_async_remote_copy(
            src_ref=src, dst_ref=stat_buf.at[there], send_sem=sems.at[slot], recv_sem=stat_recv.at[there],
            device_id=place(target), device_id_type=MESH)

    kv_to = [lut(nth(KV_OWN, n)) for n in range(2)]
    qd_to = [lut(nth(QD_OWN, n)) for n in range(2)]

    loads[0].wait()
    loads[1].wait()
    for chunk in range(NK):
        for n in range(2):
            @pl.when(kv_to[n] != NOBODY)
            def _(n=n, chunk=chunk):
                for copy in kv_copies(k_loc, v_loc, k_own, v_own, kv_to[n], n, chunk):
                    copy.start()
    loads[2].wait()
    loads[3].wait()

    def send_qd(chunk):
        for n in range(2):
            @pl.when(qd_to[n] != NOBODY)
            def _(n=n):
                for copy in qd_copies(q_loc, do_loc, q_own, do_own, qd_to[n], n, chunk):
                    copy.start()

    send_qd(0)
    loads[4].wait()
    loads[5].wait()

    wide = lax.broadcasted_iota(jnp.int32, (2, 128), 1)
    for j in range(qrows // 128):
        src = lse_loc[:, 128 * (j // 2):128 * (j // 2 + 1)]
        both = jnp.take_along_axis(src, 64 * (j % 2) + wide // 2, axis=1, mode="promise_in_bounds")
        row = jnp.where(wide[0:1] % 2 == 0, both[0:1], both[1:2])
        stat_loc[0:1, 128 * j:128 * (j + 1)] = row * math.log2(math.e)
    ones = jnp.ones((8, head), jnp.bfloat16)
    for j in range(qrows // 256):
        part = pl.ds(256 * j, 256)
        prod = do_loc[part].astype(jnp.float32) * o_loc[part].astype(jnp.float32)
        hi = prod.astype(jnp.bfloat16)
        lo = (prod - hi.astype(jnp.float32)).astype(jnp.bfloat16)
        dims = (((1,), (1,)), ((), ()))
        total = lax.dot_general(ones, hi, dims, preferred_element_type=jnp.float32)
        total = total + lax.dot_general(ones, lo, dims, preferred_element_type=jnp.float32)
        stat_loc[1:2, 256 * j:256 * (j + 1)] = total[0:1]
    for n in range(2):
        @pl.when(qd_to[n] != NOBODY)
        def _(n=n):
            stat_copy(stat_loc, stat_own, qd_to[n], n).start()
    for chunk in range(1, NQ):
        send_qd(chunk)

    def block(k_blk, v_blk, q_blk, do_blk, lse_row, d_row, keep):
        dims = (((1,), (1,)), ((), ()))
        scores = lax.dot_general(k_blk, q_blk, dims, preferred_element_type=jnp.float32)
        p_mat = jnp.where(keep, jnp.exp2(scores * factor - lse_row), 0.0)
        dp_mat = lax.dot_general(v_blk, do_blk, dims, preferred_element_type=jnp.float32)
        ds_mat = (p_mat * (dp_mat - d_row)).astype(jnp.bfloat16)
        return p_mat.astype(jnp.bfloat16), ds_mat

    def dq_term(k_blk, ds_mat):
        return lax.dot_general(k_blk, ds_mat, (((0,), (0,)), ((), ())), preferred_element_type=jnp.float32)

    kb_rows = 256
    qb_rows = 256
    key_iota = lax.broadcasted_iota(jnp.int32, (kb_rows, qb_rows), 0)
    tok_iota = lax.broadcasted_iota(jnp.int32, (kb_rows, qb_rows), 1) // 2

    for qb in range(qrows // qb_rows):
        cols = pl.ds(qb * qb_rows, qb_rows)
        q_blk, do_blk = q_loc[cols], do_loc[cols]
        dq_sum = None
        for kb in range((qb * qb_rows // 2) // kb_rows + 1):
            keys = pl.ds(kb * kb_rows, kb_rows)
            k_blk = k_loc[keys]
            key_pos = key_iota + (me * rows + kb * kb_rows)
            keep = key_pos >= starts[0, :, cols]
            if kb == (qb * qb_rows // 2) // kb_rows:
                keep = keep & (key_iota + kb * kb_rows <= tok_iota + qb * qb_rows // 2)
            p_low, ds_mat = block(k_blk, v_loc[keys], q_blk, do_blk, stat_loc[0:1, cols], stat_loc[1:2, cols], keep)
            term = dq_term(k_blk, ds_mat)
            dq_sum = term if dq_sum is None else dq_sum + term
            dv_new = jnp.dot(p_low, do_blk, preferred_element_type=jnp.float32)
            dk_new = jnp.dot(ds_mat, q_blk, preferred_element_type=jnp.float32)
            if qb == 0 or kb * kb_rows == qb * qb_rows // 2:
                dv_acc[keys] = dv_new
                dk_acc[keys] = dk_new
            else:
                dv_acc[keys] = dv_acc[keys] + dv_new
                dk_acc[keys] = dk_acc[keys] + dk_new
        dqt[:, cols] = dq_sum

    def kv_unit(slot, chunk):
        keys = pl.ds(chunk * kc_rows, kc_rows)
        k_blk = k_buf[slot, keys]
        v_blk = v_buf[slot, keys]
        base = (me - 1 - slot) * rows + chunk * kc_rows
        for qb in range(qrows // qb_rows):
            cols = pl.ds(qb * qb_rows, qb_rows)
            keep = key_iota >= starts[0, :, cols] - base
            _, ds_mat = block(k_blk, v_blk, q_loc[cols], do_loc[cols], stat_loc[0:1, cols], stat_loc[1:2, cols], keep)
            dqt[:, cols] = dqt[:, cols] + dq_term(k_blk, ds_mat)

    def qd_unit(slot, chunk):
        part = pl.ds(chunk * qc_rows, qc_rows)
        cols = pl.ds(pl.multiple_of(chunk * qc_rows, 128), qc_rows)
        q_blk = q_buf[slot, part]
        do_blk = do_buf[slot, part]
        lse_row = stat_buf[slot, 0:1, cols]
        d_row = stat_buf[slot, 1:2, cols]
        start = starts[slot + 1, :, cols] - me * rows
        for kb in range(rows // kb_rows):
            keys = pl.ds(kb * kb_rows, kb_rows)
            keep = key_iota >= start - kb * kb_rows
            p_low, ds_mat = block(k_loc[keys], v_loc[keys], q_blk, do_blk, lse_row, d_row, keep)
            dv_acc[keys] = dv_acc[keys] + jnp.dot(p_low, do_blk, preferred_element_type=jnp.float32)
            dk_acc[keys] = dk_acc[keys] + jnp.dot(ds_mat, q_blk, preferred_element_type=jnp.float32)

    kv_on = [lut(targets_of(KV_REL, lambda d, h=h: (d, h + 1))) for h in range(HOPS)]
    qd_on = [lut(targets_of(QD_REL, lambda d, h=h: (d, h + 1))) for h in range(HOPS)]

    def pick(values, slot):
        return jnp.where(slot == 0, values[0], jnp.where(slot == 1, values[1], values[2]))

    per_word = 6
    codes = {d: step_codes(ORDER[d]) for d in range(8)}
    steps = max(len(c) for c in codes.values())
    words = -(-steps // per_word)
    packed = []
    for w in range(words):
        values = []
        for d in range(8):
            part = (codes[d] + [NONE] * (words * per_word))[w * per_word:(w + 1) * per_word]
            values.append(sum(c * 32 ** i for i, c in enumerate(part)))
        packed.append(lut(values))

    def step(i, carry):
        code = carry[0] % 32

        @pl.when(code < 3 * NK)
        def _():
            slot, chunk = code // NK, code % NK
            to = pick(kv_on, slot)
            for copy in kv_copies(k_buf.at[slot], v_buf.at[slot], k_rel, v_rel, me * 4 + slot + 1, slot, chunk):
                copy.wait_recv()

            @pl.when(to != NOBODY)
            def _():
                for copy in kv_copies(k_buf.at[slot], v_buf.at[slot], k_rel, v_rel, to, slot, chunk):
                    copy.start()

            @pl.when(me > slot)
            def _():
                kv_unit(slot, chunk)

        @pl.when((code >= 3 * NK) & (code < FINISH))
        def _():
            slot, chunk = (code - 3 * NK) // NQ, (code - 3 * NK) % NQ
            to = pick(qd_on, slot)
            for copy in qd_copies(q_buf.at[slot], do_buf.at[slot], q_rel, do_rel, me * 4 + slot + 1, slot, chunk):
                copy.wait_recv()

            @pl.when(to != NOBODY)
            def _():
                for copy in qd_copies(q_buf.at[slot], do_buf.at[slot], q_rel, do_rel, to, slot, chunk):
                    copy.start()

            @pl.when(chunk == 0)
            def _():
                stat_copy(stat_buf.at[slot], stat_rel, me * 4 + slot + 1, slot).wait_recv()

                @pl.when(to != NOBODY)
                def _():
                    stat_copy(stat_buf.at[slot], stat_rel, to, slot).start()

            @pl.when(me + slot < 7)
            def _():
                qd_unit(slot, chunk)

        last = (i % per_word) == per_word - 1
        rest = [jnp.where(last, (carry + (jnp.int32(0),))[w + 1], carry[w] // 32 if w == 0 else carry[w]) for w in range(words)]
        return tuple(rest)

    lax.fori_loop(0, steps, step, tuple(packed))

    dq_st[...] = (jnp.transpose(dqt[...]) * scale).astype(jnp.bfloat16)
    dk_st[...] = (dk_acc[...] * scale).astype(jnp.bfloat16)
    dv_st[...] = dv_acc[...].astype(jnp.bfloat16)
    stores = [
        pltpu.make_async_copy(src, dst, out_sem.at[i])
        for i, (src, dst) in enumerate([(dq_st, dq_out), (dk_st, dk_out), (dv_st, dv_out)])
    ]
    for store in stores:
        store.start()

    for chunk in range(NK):
        for n in range(2):
            @pl.when(kv_to[n] != NOBODY)
            def _(n=n, chunk=chunk):
                for copy in kv_copies(k_loc, v_loc, k_own, v_own, kv_to[n], n, chunk):
                    copy.wait_send()
        for h in range(HOPS):
            @pl.when(kv_on[h] != NOBODY)
            def _(h=h, chunk=chunk):
                for copy in kv_copies(k_buf.at[h], v_buf.at[h], k_rel, v_rel, kv_on[h], h, chunk):
                    copy.wait_send()
    for n in range(2):
        @pl.when(qd_to[n] != NOBODY)
        def _(n=n):
            stat_copy(stat_loc, stat_own, qd_to[n], n).wait_send()
            for chunk in range(NQ):
                for copy in qd_copies(q_loc, do_loc, q_own, do_own, qd_to[n], n, chunk):
                    copy.wait_send()
    for h in range(HOPS):
        @pl.when(qd_on[h] != NOBODY)
        def _(h=h):
            stat_copy(stat_buf.at[h], stat_rel, qd_on[h], h).wait_send()
            for chunk in range(NQ):
                for copy in qd_copies(q_buf.at[h], do_buf.at[h], q_rel, do_rel, qd_on[h], h, chunk):
                    copy.wait_send()
    for store in stores:
        store.wait()


def solution(mesh):
    def local(queries, keys, values, attn_out, logsumexp, d_out, cu_seqlens):
        rows, heads, head = queries.shape
        qrows = rows * heads
        bf, f32 = jnp.bfloat16, jnp.float32
        dma = pltpu.SemaphoreType.DMA
        any_spec = pl.BlockSpec(memory_space=pl.ANY)
        d_query, d_key, d_value = pl.pallas_call(
            body,
            name="packed_backward",
            out_shape=(
                jax.ShapeDtypeStruct((qrows, head), bf),
                jax.ShapeDtypeStruct((rows, head), bf),
                jax.ShapeDtypeStruct((rows, head), bf),
            ),
            in_specs=[pl.BlockSpec(memory_space=pltpu.SMEM)] + [any_spec] * 6,
            out_specs=(any_spec,) * 3,
            scratch_shapes=[
                pltpu.VMEM((qrows, head), bf), pltpu.VMEM((rows, head), bf), pltpu.VMEM((rows, head), bf),
                pltpu.VMEM((qrows, head), bf), pltpu.VMEM((heads, rows), f32), pltpu.VMEM((qrows, head), bf),
                pltpu.VMEM((2, qrows), f32), pltpu.VMEM((HOPS + 1, 1, qrows), jnp.int32),
                pltpu.VMEM((HOPS, rows, head), bf), pltpu.VMEM((HOPS, rows, head), bf),
                pltpu.VMEM((HOPS, qrows, head), bf), pltpu.VMEM((HOPS, qrows, head), bf), pltpu.VMEM((HOPS, 2, qrows), f32),
                pltpu.VMEM((head, qrows), f32), pltpu.VMEM((rows, head), f32), pltpu.VMEM((rows, head), f32),
                pltpu.VMEM((qrows, head), bf), pltpu.VMEM((rows, head), bf), pltpu.VMEM((rows, head), bf),
                dma((6,)), dma((3,)),
                dma((HOPS, NK)), dma((HOPS, NK)), dma((HOPS, NQ)), dma((HOPS, NQ)), dma((HOPS,)),
                dma((2, NK)), dma((2, NK)), dma((2, NQ)), dma((2, NQ)), dma((2,)),
                dma((HOPS, NK)), dma((HOPS, NK)), dma((HOPS, NQ)), dma((HOPS, NQ)), dma((HOPS,)),
            ],
            compiler_params=pltpu.CompilerParams(collective_id=0, has_side_effects=True),
        )(cu_seqlens, queries.reshape(qrows, head), keys, values, attn_out.reshape(qrows, head), logsumexp.T, d_out.reshape(qrows, head))
        return d_query.reshape(rows, heads, head), d_key, d_value

    seq_spec = P(("dp", "cpo", "cp"))
    return jax.shard_map(local, mesh=mesh, in_specs=(seq_spec,) * 6 + (P("dp"),), out_specs=(seq_spec,) * 3, check_vma=False)
```

```python
import functools
import math

import jax
import jax.numpy as jnp
from jax import lax
from jax.experimental import pallas as pl
from jax.experimental.pallas import tpu as pltpu
from jax.sharding import PartitionSpec as P

MESH = pl.DeviceIdType.MESH
HOPS = 3
NK = 2
NQ = 4
NONE = 31
NOBODY = 63
SEND = 18

KV_OWN = {0: [(1, 1), (2, 2)], 1: [(3, 2), (4, 3)], 2: [(3, 1), (4, 2)], 3: [(6, 3)], 4: [(5, 1), (6, 2)], 5: [(7, 2)], 6: [(7, 1)], 7: []}
QD_OWN = {0: [], 1: [(0, 1)], 2: [(0, 2)], 3: [(2, 1), (1, 2)], 4: [(1, 3)], 5: [(4, 1), (3, 2)], 6: [(4, 2), (3, 3)], 7: [(6, 1), (5, 2)]}
KV_FAR = 2
QD_FAR = 5
FAR_NEWS = ((0, 2, 4), (7, 5, 3))
KV_REL = {(2, 2): (3, 3), (3, 2): (2, 1), (4, 2): (5, 3), (4, 1): (5, 2), (6, 3): (4, 1), (6, 2): (7, 3), (7, 2): (6, 1)}
QD_REL = {(0, 2): (1, 1), (1, 2): (0, 3), (1, 3): (3, 1), (3, 1): (2, 2), (3, 2): (2, 3), (4, 2): (5, 1), (5, 2): (4, 3)}
ORDER = {
    0: (0, 110, 112, 111, 113, 120, 130, 131, 132, 121, 133, 122, 123),
    1: (0, 10, 11, 130, 120, 131, 110, 132, 121, 133, 122, 123, 111, 112, 113),
    2: (0, 110, 112, 111, 113, 20, 10, 21, 11, 120, 130, 121, 122, 131, 132, 123, 133),
    3: (0, 10, 11, 130, 20, 131, 30, 21, 132, 31, 110, 120, 133, 111, 112, 121, 122, 113, 123),
    4: (0, 110, 112, 111, 30, 113, 120, 31, 130, 121, 20, 131, 10, 21, 132, 11, 122, 133, 123),
    5: (0, 10, 11, 120, 110, 121, 111, 30, 122, 20, 31, 123, 21, 112, 113),
    6: (110, 112, 111, 30, 113, 20, 31, 0, 10, 21, 11),
    7: (0, 10, 11, 20, 30, 21, 31),
}


def step_codes(items):
    codes = []
    for item in items:
        if item == 0:
            codes.append(SEND)
            continue
        hop, chunk = item % 100 // 10 - 1, item % 10
        codes.append(hop * NK + chunk if item < 100 else 3 * NK + hop * NQ + chunk)
    return codes


def targets_of(table, pick):
    pairs = [table.get(pick(d), NOBODY) for d in range(8)]
    return [p if p == NOBODY else p[0] * 4 + p[1] for p in pairs]


def nth(table, n):
    return [NOBODY if len(table[d]) <= n else table[d][n][0] * 4 + table[d][n][1] for d in range(8)]


def partners():
    near = {d: set() for d in range(8)}
    for table in (KV_OWN, QD_OWN):
        for d, pairs in table.items():
            for n, (target, _) in enumerate(pairs):
                if n == 1 and d == (KV_FAR if table is KV_OWN else QD_FAR):
                    continue
                near[d].add(target)
                near[target].add(d)
    for messenger, far, target in FAR_NEWS:
        for other in (far, target):
            near[messenger].add(other)
            near[other].add(messenger)
    for table in (KV_REL, QD_REL):
        for (d, _), (target, _) in table.items():
            near[d].add(target)
            near[target].add(d)
    return near


def body(
    cu_ref, q_hbm, k_hbm, v_hbm, o_hbm, lse_hbm, do_hbm,
    dq_out, dk_out, dv_out,
    q_loc, k_loc, v_loc, o_loc, lse_loc, do_loc, stat_loc, starts,
    k_buf, v_buf, q_buf, do_buf, stat_buf,
    dqt, dk_acc, dv_acc, in_sem, far_sem,
    k_recv, v_recv, q_recv, do_recv, stat_recv,
    kv_own, qd_own, stat_own, kv_rel, qd_rel, stat_rel,
):
    rows = k_loc.shape[0]
    qrows = q_loc.shape[0]
    head = k_loc.shape[1]
    kc_rows = rows // NK
    qc_rows = qrows // NQ
    scale = head ** -0.5
    factor = scale * math.log2(math.e)
    me = lax.axis_index("cpo") * 4 + lax.axis_index("cp")

    def lut(values):
        out = jnp.int32(values[0])
        for d in range(1, len(values)):
            out = jnp.where(me == d, jnp.int32(values[d]), out)
        return out

    def place(target):
        return {"cpo": target // 4, "cp": target % 4}

    loads = [
        pltpu.make_async_copy(src, dst, in_sem.at[i])
        for i, (src, dst) in enumerate(
            [(k_hbm, k_loc), (v_hbm, v_loc), (q_hbm, q_loc), (do_hbm, do_loc), (o_hbm, o_loc), (lse_hbm, lse_loc)]
        )
    ]
    for load in loads:
        load.start()

    barrier = pltpu.get_barrier_semaphore()
    near = partners()
    for d in range(8):
        @pl.when(me == d)
        def _(d=d):
            for other in sorted(near[d]):
                pl.semaphore_signal(barrier, inc=1, device_id=place(other), device_id_type=MESH)
    lane = lax.broadcasted_iota(jnp.int32, (1, qrows), 1) // 2
    for h in range(HOPS + 1):
        pos = lane + (me + h) * rows
        start = jnp.zeros_like(pos)
        for j in range(cu_ref.shape[0]):
            start = jnp.maximum(start, jnp.where(pos >= cu_ref[j], cu_ref[j], 0))
        starts[h] = start
    for d in range(8):
        @pl.when(me == d)
        def _(d=d):
            pl.semaphore_wait(barrier, len(near[d]))

    def kv_copies(src_k, src_v, sem, code, chunk):
        target, there = code // 4, code % 4 - 1
        part = pl.ds(chunk * kc_rows, kc_rows)
        return [
            pltpu.make_async_remote_copy(
                src_ref=src.at[part], dst_ref=buf.at[there, part], send_sem=sem, recv_sem=recv.at[there, chunk],
                device_id=place(target), device_id_type=MESH)
            for src, buf, recv in ((src_k, k_buf, k_recv), (src_v, v_buf, v_recv))
        ]

    def qd_copies(src_q, src_do, sem, code, chunk):
        target, there = code // 4, code % 4 - 1
        part = pl.ds(chunk * qc_rows, qc_rows)
        return [
            pltpu.make_async_remote_copy(
                src_ref=src.at[part], dst_ref=buf.at[there, part], send_sem=sem, recv_sem=recv.at[there, chunk],
                device_id=place(target), device_id_type=MESH)
            for src, buf, recv in ((src_q, q_buf, q_recv), (src_do, do_buf, do_recv))
        ]

    def stat_copy(src, sem, code):
        target, there = code // 4, code % 4 - 1
        return pltpu.make_async_remote_copy(
            src_ref=src, dst_ref=stat_buf.at[there], send_sem=sem, recv_sem=stat_recv.at[there],
            device_id=place(target), device_id_type=MESH)

    kv_to = [lut(nth(KV_OWN, n)) for n in range(2)]
    qd_to = [lut(nth(QD_OWN, n)) for n in range(2)]

    def send_kv(n, chunk):
        for copy in kv_copies(k_loc, v_loc, kv_own.at[n], kv_to[n], chunk):
            copy.start()

    def send_qd(n, chunk):
        for copy in qd_copies(q_loc, do_loc, qd_own.at[n], qd_to[n], chunk):
            copy.start()

    kv_near = [kv_to[0] != NOBODY, (kv_to[1] != NOBODY) & (me != KV_FAR)]
    qd_near = [qd_to[0] != NOBODY, (qd_to[1] != NOBODY) & (me != QD_FAR)]
    loads[0].wait()
    loads[1].wait()
    for chunk in range(NK):
        for n in range(2):
            @pl.when(kv_near[n])
            def _(n=n, chunk=chunk):
                send_kv(n, chunk)
    loads[2].wait()
    loads[3].wait()
    for n in range(2):
        @pl.when(qd_near[n])
        def _(n=n):
            send_qd(n, 0)
    for messenger, far, _ in FAR_NEWS:
        @pl.when(me == messenger)
        def _(far=far):
            pl.semaphore_signal(far_sem, inc=1, device_id=place(far), device_id_type=MESH)
    loads[4].wait()
    loads[5].wait()

    wide = lax.broadcasted_iota(jnp.int32, (2, 128), 1)
    for j in range(qrows // 128):
        src = lse_loc[:, 128 * (j // 2):128 * (j // 2 + 1)]
        both = jnp.take_along_axis(src, 64 * (j % 2) + wide // 2, axis=1, mode="promise_in_bounds")
        row = jnp.where(wide[0:1] % 2 == 0, both[0:1], both[1:2])
        stat_loc[0:1, 128 * j:128 * (j + 1)] = row * math.log2(math.e)
    ones = jnp.ones((8, head), jnp.bfloat16)
    for j in range(qrows // 256):
        part = pl.ds(256 * j, 256)
        prod = do_loc[part].astype(jnp.float32) * o_loc[part].astype(jnp.float32)
        hi = prod.astype(jnp.bfloat16)
        lo = (prod - hi.astype(jnp.float32)).astype(jnp.bfloat16)
        dims = (((1,), (1,)), ((), ()))
        total = lax.dot_general(ones, hi, dims, preferred_element_type=jnp.float32)
        total = total + lax.dot_general(ones, lo, dims, preferred_element_type=jnp.float32)
        stat_loc[1:2, 256 * j:256 * (j + 1)] = total[0:1]
    for n in range(2):
        @pl.when(qd_near[n])
        def _(n=n):
            stat_copy(stat_loc, stat_own.at[n], qd_to[n]).start()
            send_qd(n, 1)

    @pl.when(me == KV_FAR)
    def _():
        pl.semaphore_wait(far_sem, 1)
        for chunk in range(NK):
            send_kv(1, chunk)

    @pl.when(me == QD_FAR)
    def _():
        pl.semaphore_wait(far_sem, 1)
        send_qd(1, 0)
        stat_copy(stat_loc, stat_own.at[1], qd_to[1]).start()
        send_qd(1, 1)

    def send_later():
        for chunk in range(2, NQ):
            for n in range(2):
                @pl.when(qd_to[n] != NOBODY)
                def _(n=n, chunk=chunk):
                    send_qd(n, chunk)

    def block(k_blk, v_blk, q_blk, do_blk, lse_row, d_row, keep):
        dims = (((1,), (1,)), ((), ()))
        scores = lax.dot_general(k_blk, q_blk, dims, preferred_element_type=jnp.float32)
        p_mat = jnp.where(keep, jnp.exp2(scores * factor - lse_row), 0.0)
        dp_mat = lax.dot_general(v_blk, do_blk, dims, preferred_element_type=jnp.float32)
        ds_mat = (p_mat * (dp_mat - d_row)).astype(jnp.bfloat16)
        return p_mat.astype(jnp.bfloat16), ds_mat

    def dq_term(k_blk, ds_mat):
        return lax.dot_general(k_blk, ds_mat, (((0,), (0,)), ((), ())), preferred_element_type=jnp.float32)

    def key_iota(keys, width):
        return lax.broadcasted_iota(jnp.int32, (keys, width), 0)

    half = qrows // 2

    def own_half(first, keys):
        cols = pl.ds(first, half)
        q_blk, do_blk, k_blk = q_loc[cols], do_loc[cols], k_loc[0:keys]
        key_pos = key_iota(keys, half)
        tok = lax.broadcasted_iota(jnp.int32, (keys, half), 1) // 2 + first // 2
        keep = (key_pos >= starts[0, :, cols] - me * rows) & (key_pos <= tok)
        p_low, ds_mat = block(k_blk, v_loc[0:keys], q_blk, do_blk, stat_loc[0:1, cols], stat_loc[1:2, cols], keep)
        dqt[:, cols] = dq_term(k_blk, ds_mat)
        dv_new = jnp.dot(p_low, do_blk, preferred_element_type=jnp.float32)
        dk_new = jnp.dot(ds_mat, q_blk, preferred_element_type=jnp.float32)
        if keys == rows:
            dv_acc[...] = dv_new
            dk_acc[...] = dk_new
        else:
            dv_acc[0:keys] = dv_acc[0:keys] + dv_new
            dk_acc[0:keys] = dk_acc[0:keys] + dk_new

    own_half(half, rows)
    own_half(0, rows // 2)

    def kv_unit(slot):
        base = (me - 1 - slot) * rows
        keep = key_iota(rows, qrows) >= starts[0] - base
        k_blk = k_buf[slot]
        _, ds_mat = block(k_blk, v_buf[slot], q_loc[...], do_loc[...], stat_loc[0:1], stat_loc[1:2], keep)
        dqt[...] = dqt[...] + dq_term(k_blk, ds_mat)

    def qd_unit(slot, part):
        cols = pl.ds(pl.multiple_of(part * half, 128), half)
        q_blk = q_buf[slot, cols]
        do_blk = do_buf[slot, cols]
        keep = key_iota(rows, half) >= starts[slot + 1, :, cols] - me * rows
        p_low, ds_mat = block(k_loc[...], v_loc[...], q_blk, do_blk, stat_buf[slot, 0:1, cols], stat_buf[slot, 1:2, cols], keep)
        dv_acc[...] = dv_acc[...] + jnp.dot(p_low, do_blk, preferred_element_type=jnp.float32)
        dk_acc[...] = dk_acc[...] + jnp.dot(ds_mat, q_blk, preferred_element_type=jnp.float32)

    kv_on = [lut(targets_of(KV_REL, lambda d, h=h: (d, h + 1))) for h in range(HOPS)]
    qd_on = [lut(targets_of(QD_REL, lambda d, h=h: (d, h + 1))) for h in range(HOPS)]

    def pick(values, slot):
        return jnp.where(slot == 0, values[0], jnp.where(slot == 1, values[1], values[2]))

    per_word = 6
    codes = {d: step_codes(ORDER[d]) for d in range(8)}
    steps = max(len(c) for c in codes.values())
    words = -(-steps // per_word)
    packed = []
    for w in range(words):
        values = []
        for d in range(8):
            part = (codes[d] + [NONE] * (words * per_word))[w * per_word:(w + 1) * per_word]
            values.append(sum(c * 32 ** i for i, c in enumerate(part)))
        packed.append(lut(values))

    def step(i, carry):
        code = carry[0] % 32

        @pl.when(code < 3 * NK)
        def _():
            slot, chunk = code // NK, code % NK
            to = pick(kv_on, slot)
            for copy in kv_copies(k_buf.at[slot], v_buf.at[slot], kv_rel.at[slot], me * 4 + slot + 1, chunk):
                copy.wait_recv()

            @pl.when(to != NOBODY)
            def _():
                for copy in kv_copies(k_buf.at[slot], v_buf.at[slot], kv_rel.at[slot], to, chunk):
                    copy.start()

            @pl.when((me > slot) & (chunk == NK - 1))
            def _():
                kv_unit(slot)

        @pl.when((code >= 3 * NK) & (code < SEND))
        def _():
            slot, chunk = (code - 3 * NK) // NQ, (code - 3 * NK) % NQ
            to = pick(qd_on, slot)
            for copy in qd_copies(q_buf.at[slot], do_buf.at[slot], qd_rel.at[slot], me * 4 + slot + 1, chunk):
                copy.wait_recv()

            @pl.when(to != NOBODY)
            def _():
                for copy in qd_copies(q_buf.at[slot], do_buf.at[slot], qd_rel.at[slot], to, chunk):
                    copy.start()

            @pl.when(chunk == 0)
            def _():
                stat_copy(stat_buf.at[slot], stat_rel.at[slot], me * 4 + slot + 1).wait_recv()

                @pl.when(to != NOBODY)
                def _():
                    stat_copy(stat_buf.at[slot], stat_rel.at[slot], to).start()

            @pl.when((me + slot < 7) & (chunk % 2 == 1))
            def _():
                qd_unit(slot, chunk // 2)

        @pl.when(code == SEND)
        def _():
            send_later()

        last = (i % per_word) == per_word - 1
        rest = [jnp.where(last, (carry + (jnp.int32(0),))[w + 1], carry[w] // 32 if w == 0 else carry[w]) for w in range(words)]
        return tuple(rest)

    lax.fori_loop(0, steps, step, tuple(packed))

    dq_out[...] = (jnp.transpose(dqt[...]) * scale).astype(jnp.bfloat16)
    dk_out[...] = (dk_acc[...] * scale).astype(jnp.bfloat16)
    dv_out[...] = dv_acc[...].astype(jnp.bfloat16)

    def sent(ref, sem):
        pltpu.make_async_remote_copy(src_ref=ref, dst_ref=ref, send_sem=sem, recv_sem=sem, device_id=place(me), device_id_type=MESH).wait_send()

    for targets, kv_sem in ((kv_to, kv_own), (kv_on, kv_rel)):
        for n, target in enumerate(targets):
            @pl.when(target != NOBODY)
            def _(n=n, kv_sem=kv_sem):
                sent(q_buf.at[0], kv_sem.at[n])
    for targets, qd_sem, stat_sem in ((qd_to, qd_own, stat_own), (qd_on, qd_rel, stat_rel)):
        for n, target in enumerate(targets):
            @pl.when(target != NOBODY)
            def _(n=n, qd_sem=qd_sem, stat_sem=stat_sem):
                sent(q_buf.at[0:2], qd_sem.at[n])
                sent(stat_loc, stat_sem.at[n])


def store_body(dq_ref, dk_ref, dv_ref, dq_out, dk_out, dv_out, sems):
    pairs = ((dq_ref, dq_out), (dk_ref, dk_out), (dv_ref, dv_out))
    copies = [pltpu.make_async_copy(src, dst, sems.at[i]) for i, (src, dst) in enumerate(pairs)]
    for copy in copies:
        copy.start()
    for copy in copies:
        copy.wait()


def solution(mesh):
    def local(queries, keys, values, attn_out, logsumexp, d_out, cu_seqlens):
        rows, heads, head = queries.shape
        qrows = rows * heads
        bf, f32 = jnp.bfloat16, jnp.float32
        dma = pltpu.SemaphoreType.DMA
        any_spec = pl.BlockSpec(memory_space=pl.ANY)
        vmem_spec = pl.BlockSpec(memory_space=pltpu.VMEM)
        shapes = ((qrows, head), (rows, head), (rows, head))
        results = pl.pallas_call(
            body,
            name="packed_backward",
            out_shape=tuple(pltpu.VMEM(shape, bf) for shape in shapes),
            in_specs=[pl.BlockSpec(memory_space=pltpu.SMEM)] + [any_spec] * 6,
            out_specs=(vmem_spec,) * 3,
            scratch_shapes=[
                pltpu.VMEM((qrows, head), bf), pltpu.VMEM((rows, head), bf), pltpu.VMEM((rows, head), bf),
                pltpu.VMEM((qrows, head), bf), pltpu.VMEM((heads, rows), f32), pltpu.VMEM((qrows, head), bf),
                pltpu.VMEM((2, qrows), f32), pltpu.VMEM((HOPS + 1, 1, qrows), jnp.int32),
                pltpu.VMEM((HOPS, rows, head), bf), pltpu.VMEM((HOPS, rows, head), bf),
                pltpu.VMEM((HOPS, qrows, head), bf), pltpu.VMEM((HOPS, qrows, head), bf), pltpu.VMEM((HOPS, 2, qrows), f32),
                pltpu.VMEM((head, qrows), f32), pltpu.VMEM((rows, head), f32), pltpu.VMEM((rows, head), f32),
                dma((6,)), pltpu.SemaphoreType.REGULAR,
                dma((HOPS, NK)), dma((HOPS, NK)), dma((HOPS, NQ)), dma((HOPS, NQ)), dma((HOPS,)),
                dma((2,)), dma((2,)), dma((2,)), dma((HOPS,)), dma((HOPS,)), dma((HOPS,)),
            ],
            compiler_params=pltpu.CompilerParams(collective_id=0, has_side_effects=True),
        )(cu_seqlens, queries.reshape(qrows, head), keys, values, attn_out.reshape(qrows, head), logsumexp.T, d_out.reshape(qrows, head))
        d_query, d_key, d_value = pl.pallas_call(
            store_body,
            name="store",
            out_shape=tuple(jax.ShapeDtypeStruct(shape, bf) for shape in shapes),
            in_specs=[vmem_spec] * 3,
            out_specs=(any_spec,) * 3,
            scratch_shapes=[dma((3,))],
        )(*[pltpu.with_memory_space_constraint(x, pltpu.VMEM) for x in results])
        return d_query.reshape(rows, heads, head), d_key, d_value

    seq_spec = P(("dp", "cpo", "cp"))
    return jax.shard_map(local, mesh=mesh, in_specs=(seq_spec,) * 6 + (P("dp"),), out_specs=(seq_spec,) * 3, check_vma=False)
```

```python
import functools
import math

import jax
import jax.numpy as jnp
from jax import lax
from jax.experimental import pallas as pl
from jax.experimental.pallas import tpu as pltpu
from jax.sharding import PartitionSpec as P

MESH = pl.DeviceIdType.MESH
HOPS = 3
NK = 2
NQ = 4
NONE = 31
NOBODY = 63
SEND = 18

KV_OWN = {0: [(1, 1), (2, 2)], 1: [(3, 2), (4, 3)], 2: [(3, 1), (4, 2)], 3: [(6, 3)], 4: [(5, 1), (6, 2)], 5: [(7, 2)], 6: [(7, 1)], 7: []}
QD_OWN = {0: [], 1: [(0, 1)], 2: [(0, 2)], 3: [(2, 1), (1, 2)], 4: [(1, 3)], 5: [(4, 1), (3, 2)], 6: [(4, 2), (3, 3)], 7: [(6, 1), (5, 2)]}
KV_FAR = 2
QD_FAR = 5
FIRST = {
    0: (0, 10, 1, 11),
    1: (0, 10, 1, 11, 100),
    2: (0, 1, 100),
    3: (0, 1, 100, 110),
    4: (0, 10, 1, 11, 100),
    5: (0, 100),
    6: (0, 1, 110, 100),
    7: (100, 110),
}
REST = {
    1: (101, 102, 103),
    2: (10, 11, 101, 102, 103),
    3: (101, 111, 102, 112, 103, 113),
    4: (101, 102, 103),
    5: (110, 1, 101, 102, 103, 111, 112, 113),
    6: (111, 101, 112, 113),
    7: (101, 111, 102, 112, 103, 113),
}
LATER = {
    6: (102, 103),
}
TAIL = (2, 1, 3, 2, 2, 1, 0, 0)
FAR_NEWS = ((0, 2, 4), (7, 5, 3))
KV_REL = {(2, 2): (3, 3), (3, 2): (2, 1), (4, 2): (5, 3), (4, 1): (5, 2), (6, 3): (4, 1), (6, 2): (7, 3), (7, 2): (6, 1)}
QD_REL = {(0, 2): (1, 1), (1, 2): (0, 3), (1, 3): (3, 1), (3, 1): (2, 2), (3, 2): (2, 3), (4, 2): (5, 1), (5, 2): (4, 3)}
ORDER = ("sghijkopqlrmn", "sabokpgqlrmnhij", "sghijcadboklpmqnr", "sabocpedkqgfrhlimjn", "sghiejkfolpcaqdbmrn", "sabkglhmecfndij", "ghiejcfsadb", "sabcefd")


def step_codes(letters):
    return [ord(x) - ord("a") for x in letters]


def targets_of(table, pick):
    pairs = [table.get(pick(d), NOBODY) for d in range(8)]
    return [p if p == NOBODY else p[0] * 4 + p[1] for p in pairs]


def nth(table, n):
    return [NOBODY if len(table[d]) <= n else table[d][n][0] * 4 + table[d][n][1] for d in range(8)]


def partners():
    near = {d: set() for d in range(8)}
    for table in (KV_OWN, QD_OWN):
        for d, pairs in table.items():
            for n, (target, _) in enumerate(pairs):
                if n == 1 and d == (KV_FAR if table is KV_OWN else QD_FAR):
                    continue
                near[d].add(target)
                near[target].add(d)
    for messenger, far, target in FAR_NEWS:
        for other in (far, target):
            near[messenger].add(other)
            near[other].add(messenger)
    for table in (KV_REL, QD_REL):
        for (d, _), (target, _) in table.items():
            near[d].add(target)
            near[target].add(d)
    return near


def body(
    cu_hbm, q_hbm, k_hbm, v_hbm, o_hbm, lse_hbm, do_hbm,
    dq_out, dk_out, dv_out,
    q_loc, k_loc, v_loc, o_loc, lse_loc, do_loc, stat_loc, starts,
    k_buf, v_buf, q_buf, do_buf, stat_buf,
    dqt, dk_acc, dv_acc, cu_ref, in_sem, far_sem,
    k_recv, v_recv, q_recv, do_recv, stat_recv,
    kv_own, qd_own, stat_own, kv_rel, qd_rel, stat_rel,
):
    rows = k_loc.shape[0]
    qrows = q_loc.shape[0]
    head = k_loc.shape[1]
    kc_rows = rows // NK
    qc_rows = qrows // NQ
    scale = head ** -0.5
    factor = scale * math.log2(math.e)
    me = lax.axis_index("cpo") * 4 + lax.axis_index("cp")

    def lut(values):
        out = jnp.int32(values[0])
        for d in range(1, len(values)):
            out = jnp.where(me == d, jnp.int32(values[d]), out)
        return out

    def place(target):
        return {"cpo": target // 4, "cp": target % 4}

    barrier = pltpu.get_barrier_semaphore()
    near = partners()
    for d in range(8):
        @pl.when(me == d)
        def _(d=d):
            for other in sorted(near[d]):
                pl.semaphore_signal(barrier, inc=1, device_id=place(other), device_id_type=MESH)
    loads = [
        pltpu.make_async_copy(src, dst, in_sem.at[i])
        for i, (src, dst) in enumerate(
            [(k_hbm, k_loc), (v_hbm, v_loc), (q_hbm, q_loc), (do_hbm, do_loc), (o_hbm, o_loc), (lse_hbm, lse_loc), (cu_hbm, cu_ref)]
        )
    ]
    for load in loads:
        load.start()
    for d in range(8):
        @pl.when(me == d)
        def _(d=d):
            pl.semaphore_wait(barrier, len(near[d]))

    def kv_copies(src_k, src_v, sem, code, chunk):
        target, there = code // 4, code % 4 - 1
        part = pl.ds(chunk * kc_rows, kc_rows)
        return [
            pltpu.make_async_remote_copy(
                src_ref=src.at[part], dst_ref=buf.at[there, part], send_sem=sem, recv_sem=recv.at[there, chunk],
                device_id=place(target), device_id_type=MESH)
            for src, buf, recv in ((src_k, k_buf, k_recv), (src_v, v_buf, v_recv))
        ]

    def qd_copies(src_q, src_do, sem, code, chunk):
        target, there = code // 4, code % 4 - 1
        part = pl.ds(chunk * qc_rows, qc_rows)
        return [
            pltpu.make_async_remote_copy(
                src_ref=src.at[part], dst_ref=buf.at[there, part], send_sem=sem, recv_sem=recv.at[there, chunk],
                device_id=place(target), device_id_type=MESH)
            for src, buf, recv in ((src_q, q_buf, q_recv), (src_do, do_buf, do_recv))
        ]

    def stat_copy(src, sem, code):
        target, there = code // 4, code % 4 - 1
        return pltpu.make_async_remote_copy(
            src_ref=src, dst_ref=stat_buf.at[there], send_sem=sem, recv_sem=stat_recv.at[there],
            device_id=place(target), device_id_type=MESH)

    kv_to = [lut(nth(KV_OWN, n)) for n in range(2)]
    qd_to = [lut(nth(QD_OWN, n)) for n in range(2)]

    def send(d, item):
        kind, n, chunk = item // 100, item // 10 % 10, item % 10
        target, there = (KV_OWN, QD_OWN)[kind][d][n]
        code = target * 4 + there
        if kind == 0:
            copies = kv_copies(k_loc, v_loc, kv_own.at[n], code, chunk)
        else:
            copies = qd_copies(q_loc, do_loc, qd_own.at[n], code, chunk)
        for copy in copies:
            copy.start()

    def send_stat(d, n):
        target, there = QD_OWN[d][n]
        stat_copy(stat_loc, stat_own.at[n], target * 4 + there).start()

    loads[0].wait()
    loads[1].wait()
    for d in range(8):
        @pl.when(me == d)
        def _(d=d):
            for item in FIRST[d]:
                if item < 100:
                    send(d, item)
    loads[2].wait()
    loads[3].wait()
    for d in range(8):
        @pl.when(me == d)
        def _(d=d):
            for item in FIRST[d]:
                if item >= 100:
                    send(d, item)
            for messenger, far, _ in FAR_NEWS:
                if messenger == d:
                    pl.semaphore_signal(far_sem, inc=1, device_id=place(far), device_id_type=MESH)
    loads[4].wait()
    loads[5].wait()

    wide = lax.broadcasted_iota(jnp.int32, (2, 128), 1)
    for j in range(qrows // 128):
        src = lse_loc[:, 128 * (j // 2):128 * (j // 2 + 1)]
        both = jnp.take_along_axis(src, 64 * (j % 2) + wide // 2, axis=1, mode="promise_in_bounds")
        row = jnp.where(wide[0:1] % 2 == 0, both[0:1], both[1:2])
        stat_loc[0:1, 128 * j:128 * (j + 1)] = row * math.log2(math.e)
    ones = jnp.ones((8, head), jnp.bfloat16)
    for j in range(qrows // 256):
        part = pl.ds(256 * j, 256)
        prod = do_loc[part].astype(jnp.float32) * o_loc[part].astype(jnp.float32)
        hi = prod.astype(jnp.bfloat16)
        lo = (prod - hi.astype(jnp.float32)).astype(jnp.bfloat16)
        dims = (((1,), (1,)), ((), ()))
        total = lax.dot_general(ones, hi, dims, preferred_element_type=jnp.float32)
        total = total + lax.dot_general(ones, lo, dims, preferred_element_type=jnp.float32)
        stat_loc[1:2, 256 * j:256 * (j + 1)] = total[0:1]
    for d in range(8):
        @pl.when(me == d)
        def _(d=d):
            for n in range(len(QD_OWN[d])):
                if not (d == QD_FAR and n == 1):
                    send_stat(d, n)
            if d in (KV_FAR, QD_FAR):
                pl.semaphore_wait(far_sem, 1)
            if d == QD_FAR:
                send_stat(d, 1)
            for item in REST.get(d, ()):
                send(d, item)

    loads[6].wait()
    lane = lax.broadcasted_iota(jnp.int32, (1, qrows), 1) // 2
    for h in range(HOPS + 1):
        pos = lane + (me + h) * rows
        start = jnp.zeros_like(pos)
        for j in range(cu_ref.shape[0]):
            start = jnp.maximum(start, jnp.where(pos >= cu_ref[j], cu_ref[j], 0))
        starts[h] = start

    def send_later():
        for d in LATER:
            @pl.when(me == d)
            def _(d=d):
                for item in LATER[d]:
                    send(d, item)

    def block(k_blk, v_blk, q_blk, do_blk, lse_row, d_row, keep):
        dims = (((1,), (1,)), ((), ()))
        scores = lax.dot_general(k_blk, q_blk, dims, preferred_element_type=jnp.float32)
        p_mat = jnp.where(keep, jnp.exp2(scores * factor - lse_row), 0.0)
        dp_mat = lax.dot_general(v_blk, do_blk, dims, preferred_element_type=jnp.float32)
        ds_mat = (p_mat * (dp_mat - d_row)).astype(jnp.bfloat16)
        return p_mat.astype(jnp.bfloat16), ds_mat

    def dq_term(k_blk, ds_mat):
        return lax.dot_general(k_blk, ds_mat, (((0,), (0,)), ((), ())), preferred_element_type=jnp.float32)

    def key_iota(keys, width):
        return lax.broadcasted_iota(jnp.int32, (keys, width), 0)

    half = qrows // 2

    def own_half(first, keys):
        cols = pl.ds(first, half)
        q_blk, do_blk, k_blk = q_loc[cols], do_loc[cols], k_loc[0:keys]
        key_pos = key_iota(keys, half)
        tok = lax.broadcasted_iota(jnp.int32, (keys, half), 1) // 2 + first // 2
        keep = (key_pos >= starts[0, :, cols] - me * rows) & (key_pos <= tok)
        p_low, ds_mat = block(k_blk, v_loc[0:keys], q_blk, do_blk, stat_loc[0:1, cols], stat_loc[1:2, cols], keep)
        dqt[:, cols] = dq_term(k_blk, ds_mat)
        dv_new = jnp.dot(p_low, do_blk, preferred_element_type=jnp.float32)
        dk_new = jnp.dot(ds_mat, q_blk, preferred_element_type=jnp.float32)
        if keys == rows:
            dv_acc[...] = dv_new
            dk_acc[...] = dk_new
        else:
            dv_acc[0:keys] = dv_acc[0:keys] + dv_new
            dk_acc[0:keys] = dk_acc[0:keys] + dk_new

    own_half(half, rows)
    own_half(0, rows // 2)

    def finish_dq():
        dq_out[...] = (jnp.transpose(dqt[...]) * scale).astype(jnp.bfloat16)

    def kv_block(slot, first_row, count, first_key):
        cols = pl.ds(first_row, count)
        keys = pl.ds(first_key, rows - first_key)
        base = (me - 1 - slot) * rows + first_key
        keep = key_iota(rows - first_key, count) >= starts[0, :, cols] - base
        k_blk = k_buf[slot, keys]
        _, ds_mat = block(k_blk, v_buf[slot, keys], q_loc[cols], do_loc[cols], stat_loc[0:1, cols], stat_loc[1:2, cols], keep)
        dqt[:, cols] = dqt[:, cols] + dq_term(k_blk, ds_mat)

    def kv_unit(slot):
        @pl.when(slot < HOPS - 1)
        def _():
            kv_block(slot, 0, qrows, 0)

        @pl.when(slot == HOPS - 1)
        def _():
            kv_block(slot, 0, half, 0)
            kv_block(slot, half, half, rows // 2)

    def qd_block(slot, first_row, count, first_key):
        cols = pl.ds(pl.multiple_of(first_row, 128), count)
        keys = pl.ds(first_key, rows - first_key)
        q_blk = q_buf[slot, cols]
        do_blk = do_buf[slot, cols]
        keep = key_iota(rows - first_key, count) >= starts[slot + 1, :, cols] - (me * rows + first_key)
        p_low, ds_mat = block(k_loc[keys], v_loc[keys], q_blk, do_blk, stat_buf[slot, 0:1, cols], stat_buf[slot, 1:2, cols], keep)
        dv_acc[keys] = dv_acc[keys] + jnp.dot(p_low, do_blk, preferred_element_type=jnp.float32)
        dk_acc[keys] = dk_acc[keys] + jnp.dot(ds_mat, q_blk, preferred_element_type=jnp.float32)

    def qd_unit(slot, chunk):
        quarters = (slot == tail) & (chunk >= 2)
        short = (slot == HOPS - 1) & (chunk == 3)

        @pl.when(quarters)
        def _():
            qd_block(slot, chunk * qc_rows, qc_rows, 0)

        @pl.when((chunk % 2 == 1) & jnp.logical_not(quarters) & jnp.logical_not(short))
        def _():
            qd_block(slot, (chunk - 1) * qc_rows, half, 0)

        @pl.when(short & jnp.logical_not(quarters))
        def _():
            qd_block(slot, half, half, rows // 2)

    tail = lut([t - 1 for t in TAIL])
    last_kv = lut([max([-1] + [i for i, c in enumerate(step_codes(ORDER[d])) if c < 3 * NK and d > c // NK]) for d in range(8)])

    @pl.when(me == 0)
    def _():
        finish_dq()

    kv_on = [lut(targets_of(KV_REL, lambda d, h=h: (d, h + 1))) for h in range(HOPS)]
    qd_on = [lut(targets_of(QD_REL, lambda d, h=h: (d, h + 1))) for h in range(HOPS)]

    def pick(values, slot):
        return jnp.where(slot == 0, values[0], jnp.where(slot == 1, values[1], values[2]))

    per_word = 6
    codes = {d: step_codes(ORDER[d]) for d in range(8)}
    steps = max(len(c) for c in codes.values())
    words = -(-steps // per_word)
    packed = []
    for w in range(words):
        values = []
        for d in range(8):
            part = (codes[d] + [NONE] * (words * per_word))[w * per_word:(w + 1) * per_word]
            values.append(sum(c * 32 ** i for i, c in enumerate(part)))
        packed.append(lut(values))

    def step(i, carry):
        code = carry[0] % 32

        @pl.when(code < 3 * NK)
        def _():
            slot, chunk = code // NK, code % NK
            to = pick(kv_on, slot)
            for copy in kv_copies(k_buf.at[slot], v_buf.at[slot], kv_rel.at[slot], me * 4 + slot + 1, chunk):
                copy.wait_recv()

            @pl.when(to != NOBODY)
            def _():
                for copy in kv_copies(k_buf.at[slot], v_buf.at[slot], kv_rel.at[slot], to, chunk):
                    copy.start()

            @pl.when((me > slot) & (chunk == NK - 1))
            def _():
                kv_unit(slot)

            @pl.when(i == last_kv)
            def _():
                finish_dq()

        @pl.when((code >= 3 * NK) & (code < SEND))
        def _():
            slot, chunk = (code - 3 * NK) // NQ, (code - 3 * NK) % NQ
            to = pick(qd_on, slot)
            for copy in qd_copies(q_buf.at[slot], do_buf.at[slot], qd_rel.at[slot], me * 4 + slot + 1, chunk):
                copy.wait_recv()

            @pl.when(to != NOBODY)
            def _():
                for copy in qd_copies(q_buf.at[slot], do_buf.at[slot], qd_rel.at[slot], to, chunk):
                    copy.start()

            @pl.when(chunk == 0)
            def _():
                stat_copy(stat_buf.at[slot], stat_rel.at[slot], me * 4 + slot + 1).wait_recv()

                @pl.when(to != NOBODY)
                def _():
                    stat_copy(stat_buf.at[slot], stat_rel.at[slot], to).start()

            @pl.when(me + slot < 7)
            def _():
                qd_unit(slot, chunk)

        @pl.when(code == SEND)
        def _():
            send_later()

        last = (i % per_word) == per_word - 1
        rest = [jnp.where(last, (carry + (jnp.int32(0),))[w + 1], carry[w] // 32 if w == 0 else carry[w]) for w in range(words)]
        return tuple(rest)

    lax.fori_loop(0, steps, step, tuple(packed))

    dk_out[...] = (dk_acc[...] * scale).astype(jnp.bfloat16)
    dv_out[...] = dv_acc[...].astype(jnp.bfloat16)

    def sent(ref, sem):
        pltpu.make_async_remote_copy(src_ref=ref, dst_ref=ref, send_sem=sem, recv_sem=sem, device_id=place(me), device_id_type=MESH).wait_send()

    for targets, kv_sem in ((kv_to, kv_own), (kv_on, kv_rel)):
        for n, target in enumerate(targets):
            @pl.when(target != NOBODY)
            def _(n=n, kv_sem=kv_sem):
                sent(q_buf.at[0], kv_sem.at[n])
    for targets, qd_sem, stat_sem in ((qd_to, qd_own, stat_own), (qd_on, qd_rel, stat_rel)):
        for n, target in enumerate(targets):
            @pl.when(target != NOBODY)
            def _(n=n, qd_sem=qd_sem, stat_sem=stat_sem):
                sent(q_buf.at[0:2], qd_sem.at[n])
                sent(stat_loc, stat_sem.at[n])


def store_body(dq_ref, dk_ref, dv_ref, dq_out, dk_out, dv_out, sems):
    pairs = ((dq_ref, dq_out), (dk_ref, dk_out), (dv_ref, dv_out))
    copies = [pltpu.make_async_copy(src, dst, sems.at[i]) for i, (src, dst) in enumerate(pairs)]
    for copy in copies:
        copy.start()
    for copy in copies:
        copy.wait()


def solution(mesh):
    def local(queries, keys, values, attn_out, logsumexp, d_out, cu_seqlens):
        rows, heads, head = queries.shape
        qrows = rows * heads
        bf, f32 = jnp.bfloat16, jnp.float32
        dma = pltpu.SemaphoreType.DMA
        any_spec = pl.BlockSpec(memory_space=pl.ANY)
        vmem_spec = pl.BlockSpec(memory_space=pltpu.VMEM)
        shapes = ((qrows, head), (rows, head), (rows, head))
        results = pl.pallas_call(
            body,
            name="packed_backward",
            out_shape=tuple(pltpu.VMEM(shape, bf) for shape in shapes),
            in_specs=[any_spec] * 7,
            out_specs=(vmem_spec,) * 3,
            scratch_shapes=[
                pltpu.VMEM((qrows, head), bf), pltpu.VMEM((rows, head), bf), pltpu.VMEM((rows, head), bf),
                pltpu.VMEM((qrows, head), bf), pltpu.VMEM((heads, rows), f32), pltpu.VMEM((qrows, head), bf),
                pltpu.VMEM((2, qrows), f32), pltpu.VMEM((HOPS + 1, 1, qrows), jnp.int32),
                pltpu.VMEM((HOPS, rows, head), bf), pltpu.VMEM((HOPS, rows, head), bf),
                pltpu.VMEM((HOPS, qrows, head), bf), pltpu.VMEM((HOPS, qrows, head), bf), pltpu.VMEM((HOPS, 2, qrows), f32),
                pltpu.VMEM((head, qrows), f32), pltpu.VMEM((rows, head), f32), pltpu.VMEM((rows, head), f32),
                pltpu.SMEM(cu_seqlens.shape, jnp.int32), dma((7,)), pltpu.SemaphoreType.REGULAR,
                dma((HOPS, NK)), dma((HOPS, NK)), dma((HOPS, NQ)), dma((HOPS, NQ)), dma((HOPS,)),
                dma((2,)), dma((2,)), dma((2,)), dma((HOPS,)), dma((HOPS,)), dma((HOPS,)),
            ],
            compiler_params=pltpu.CompilerParams(collective_id=0, has_side_effects=True),
        )(cu_seqlens, queries.reshape(qrows, head), keys, values, attn_out.reshape(qrows, head), logsumexp.T, d_out.reshape(qrows, head))
        d_query, d_key, d_value = pl.pallas_call(
            store_body,
            name="store",
            out_shape=tuple(jax.ShapeDtypeStruct(shape, bf) for shape in shapes),
            in_specs=[vmem_spec] * 3,
            out_specs=(any_spec,) * 3,
            scratch_shapes=[dma((3,))],
        )(*[pltpu.with_memory_space_constraint(x, pltpu.VMEM) for x in results])
        return d_query.reshape(rows, heads, head), d_key, d_value

    seq_spec = P(("dp", "cpo", "cp"))
    return jax.shard_map(local, mesh=mesh, in_specs=(seq_spec,) * 6 + (P("dp"),), out_specs=(seq_spec,) * 3, check_vma=False)
```

```python
import functools
import math

import jax
import jax.numpy as jnp
from jax import lax
from jax.experimental import pallas as pl
from jax.experimental.pallas import tpu as pltpu
from jax.sharding import PartitionSpec as P

MESH = pl.DeviceIdType.MESH
HOPS = 3
NK = 2
NQ = 4
NONE = 31
NOBODY = 63
SEND = 18

KV_OWN = {0: [(1, 1), (2, 2)], 1: [(3, 2), (4, 3)], 2: [(3, 1), (4, 2)], 3: [(6, 3)], 4: [(5, 1), (6, 2)], 5: [(7, 2)], 6: [(7, 1)], 7: []}
QD_OWN = {0: [], 1: [(0, 1)], 2: [(0, 2)], 3: [(2, 1), (1, 2)], 4: [(1, 3)], 5: [(4, 1), (3, 2)], 6: [(4, 2), (3, 3)], 7: [(6, 1), (5, 2)]}
KV_FAR = 2
QD_FAR = 5
FIRST = {
    0: (0, 10, 1, 11),
    1: (0, 10, 1, 11, 100),
    2: (0, 1, 100),
    3: (0, 1, 100, 110),
    4: (0, 10, 1, 11, 100),
    5: (0, 100),
    6: (0, 1, 110, 100),
    7: (100, 110),
}
REST = {
    1: (101, 102, 103),
    3: (101, 111, 102, 112, 103, 113),
    4: (101, 102, 103),
    5: (110, 1, 101, 102, 103, 111, 112, 113),
    6: (111, 101, 112, 113),
    7: (101, 111, 102, 112, 103, 113),
}
LATER = {
    2: (10, 11, 101, 102, 103),
    6: (102, 103),
}
TAIL = (2, 1, 3, 2, 2, 1, 0, 0)
FAR_NEWS = ((0, 2, 4), (7, 5, 3))
KV_REL = {(2, 2): (3, 3), (3, 2): (2, 1), (4, 2): (5, 3), (4, 1): (5, 2), (6, 3): (4, 1), (6, 2): (7, 3), (7, 2): (6, 1)}
QD_REL = {(0, 2): (1, 1), (1, 2): (0, 3), (1, 3): (3, 1), (3, 1): (2, 2), (3, 2): (2, 3), (4, 2): (5, 1), (5, 2): (4, 3)}
ORDER = ("sghijkopqlrmn", "saobkpqglrmnhij", "sghijcadboklmpqnr", "saobcpedkgqfrhilmjn", "sgheijkfolpcaqdbmrn", "sabkglhmecfndij", "gehijcfsadb", "sabcefd")


def step_codes(letters):
    return [ord(x) - ord("a") for x in letters]


def targets_of(table, pick):
    pairs = [table.get(pick(d), NOBODY) for d in range(8)]
    return [p if p == NOBODY else p[0] * 4 + p[1] for p in pairs]


def nth(table, n):
    return [NOBODY if len(table[d]) <= n else table[d][n][0] * 4 + table[d][n][1] for d in range(8)]


def partners():
    near = {d: set() for d in range(8)}
    for table in (KV_OWN, QD_OWN):
        for d, pairs in table.items():
            for n, (target, _) in enumerate(pairs):
                if n == 1 and d == (KV_FAR if table is KV_OWN else QD_FAR):
                    continue
                near[d].add(target)
                near[target].add(d)
    for messenger, far, target in FAR_NEWS:
        for other in (far, target):
            near[messenger].add(other)
            near[other].add(messenger)
    for table in (KV_REL, QD_REL):
        for (d, _), (target, _) in table.items():
            near[d].add(target)
            near[target].add(d)
    return near


def body(
    cu_hbm, q_hbm, k_hbm, v_hbm, o_hbm, lse_hbm, do_hbm,
    dq_out, dk_out, dv_out,
    q_loc, k_loc, v_loc, o_loc, lse_loc, do_loc, stat_loc, starts,
    k_buf, v_buf, q_buf, do_buf, stat_buf,
    dqt, dk_acc, dv_acc, cu_ref, in_sem, far_sem,
    k_recv, v_recv, q_recv, do_recv, stat_recv,
    kv_own, qd_own, stat_own, kv_rel, qd_rel, stat_rel,
):
    rows = k_loc.shape[0]
    qrows = q_loc.shape[0]
    head = k_loc.shape[1]
    kc_rows = rows // NK
    qc_rows = qrows // NQ
    scale = head ** -0.5
    factor = scale * math.log2(math.e)
    me = lax.axis_index("cpo") * 4 + lax.axis_index("cp")

    def lut(values):
        out = jnp.int32(values[0])
        for d in range(1, len(values)):
            out = jnp.where(me == d, jnp.int32(values[d]), out)
        return out

    def place(target):
        return {"cpo": target // 4, "cp": target % 4}

    barrier = pltpu.get_barrier_semaphore()
    near = partners()
    for d in range(8):
        @pl.when(me == d)
        def _(d=d):
            for other in sorted(near[d]):
                pl.semaphore_signal(barrier, inc=1, device_id=place(other), device_id_type=MESH)
    loads = [
        pltpu.make_async_copy(src, dst, in_sem.at[i])
        for i, (src, dst) in enumerate(
            [(k_hbm, k_loc), (v_hbm, v_loc), (q_hbm, q_loc), (do_hbm, do_loc), (o_hbm, o_loc), (lse_hbm, lse_loc), (cu_hbm, cu_ref)]
        )
    ]
    for load in loads:
        load.start()
    for d in range(8):
        @pl.when(me == d)
        def _(d=d):
            pl.semaphore_wait(barrier, len(near[d]))
            for messenger, far, _ in FAR_NEWS:
                if messenger == d:
                    pl.semaphore_signal(far_sem, inc=1, device_id=place(far), device_id_type=MESH)

    def kv_copies(src_k, src_v, sem, code, chunk):
        target, there = code // 4, code % 4 - 1
        part = pl.ds(chunk * kc_rows, kc_rows)
        return [
            pltpu.make_async_remote_copy(
                src_ref=src.at[part], dst_ref=buf.at[there, part], send_sem=sem, recv_sem=recv.at[there, chunk],
                device_id=place(target), device_id_type=MESH)
            for src, buf, recv in ((src_k, k_buf, k_recv), (src_v, v_buf, v_recv))
        ]

    def qd_copies(src_q, src_do, sem, code, chunk):
        target, there = code // 4, code % 4 - 1
        part = pl.ds(chunk * qc_rows, qc_rows)
        return [
            pltpu.make_async_remote_copy(
                src_ref=src.at[part], dst_ref=buf.at[there, part], send_sem=sem, recv_sem=recv.at[there, chunk],
                device_id=place(target), device_id_type=MESH)
            for src, buf, recv in ((src_q, q_buf, q_recv), (src_do, do_buf, do_recv))
        ]

    def stat_copy(src, sem, code):
        target, there = code // 4, code % 4 - 1
        return pltpu.make_async_remote_copy(
            src_ref=src, dst_ref=stat_buf.at[there], send_sem=sem, recv_sem=stat_recv.at[there],
            device_id=place(target), device_id_type=MESH)

    kv_to = [lut(nth(KV_OWN, n)) for n in range(2)]
    qd_to = [lut(nth(QD_OWN, n)) for n in range(2)]

    def send(d, item):
        kind, n, chunk = item // 100, item // 10 % 10, item % 10
        target, there = (KV_OWN, QD_OWN)[kind][d][n]
        code = target * 4 + there
        if kind == 0:
            copies = kv_copies(k_loc, v_loc, kv_own.at[n], code, chunk)
        else:
            copies = qd_copies(q_loc, do_loc, qd_own.at[n], code, chunk)
        for copy in copies:
            copy.start()

    def send_stat(d, n):
        target, there = QD_OWN[d][n]
        stat_copy(stat_loc, stat_own.at[n], target * 4 + there).start()

    loads[0].wait()
    loads[1].wait()
    for d in range(8):
        @pl.when(me == d)
        def _(d=d):
            for item in FIRST[d]:
                if item < 100:
                    send(d, item)
    loads[2].wait()
    loads[3].wait()
    for d in range(8):
        @pl.when(me == d)
        def _(d=d):
            for item in FIRST[d]:
                if item >= 100:
                    send(d, item)
    loads[4].wait()
    loads[5].wait()

    wide = lax.broadcasted_iota(jnp.int32, (2, 128), 1)
    for j in range(qrows // 128):
        src = lse_loc[:, 128 * (j // 2):128 * (j // 2 + 1)]
        both = jnp.take_along_axis(src, 64 * (j % 2) + wide // 2, axis=1, mode="promise_in_bounds")
        row = jnp.where(wide[0:1] % 2 == 0, both[0:1], both[1:2])
        stat_loc[0:1, 128 * j:128 * (j + 1)] = row * math.log2(math.e)
    ones = jnp.ones((8, head), jnp.bfloat16)
    for j in range(qrows // 256):
        part = pl.ds(256 * j, 256)
        prod = do_loc[part].astype(jnp.float32) * o_loc[part].astype(jnp.float32)
        hi = prod.astype(jnp.bfloat16)
        lo = (prod - hi.astype(jnp.float32)).astype(jnp.bfloat16)
        dims = (((1,), (1,)), ((), ()))
        total = lax.dot_general(ones, hi, dims, preferred_element_type=jnp.float32)
        total = total + lax.dot_general(ones, lo, dims, preferred_element_type=jnp.float32)
        stat_loc[1:2, 256 * j:256 * (j + 1)] = total[0:1]
    for d in range(8):
        @pl.when(me == d)
        def _(d=d):
            for n in range(len(QD_OWN[d])):
                if not (d == QD_FAR and n == 1):
                    send_stat(d, n)
            if d == QD_FAR:
                pl.semaphore_wait(far_sem, 1)
                send_stat(d, 1)
            for item in REST.get(d, ()):
                send(d, item)

    loads[6].wait()
    lane = lax.broadcasted_iota(jnp.int32, (1, qrows), 1) // 2
    for h in range(HOPS + 1):
        pos = lane + (me + h) * rows
        start = jnp.zeros_like(pos)
        for j in range(cu_ref.shape[0]):
            start = jnp.maximum(start, jnp.where(pos >= cu_ref[j], cu_ref[j], 0))
        starts[h] = start

    def send_later():
        for d in LATER:
            @pl.when(me == d)
            def _(d=d):
                if d == KV_FAR:
                    pl.semaphore_wait(far_sem, 1)
                for item in LATER[d]:
                    send(d, item)

    def block(k_blk, v_blk, q_blk, do_blk, lse_row, d_row, keep):
        dims = (((1,), (1,)), ((), ()))
        scores = lax.dot_general(k_blk, q_blk, dims, preferred_element_type=jnp.float32)
        p_mat = jnp.where(keep, jnp.exp2(scores * factor - lse_row), 0.0)
        dp_mat = lax.dot_general(v_blk, do_blk, dims, preferred_element_type=jnp.float32)
        ds_mat = (p_mat * (dp_mat - d_row)).astype(jnp.bfloat16)
        return p_mat.astype(jnp.bfloat16), ds_mat

    def dq_term(k_blk, ds_mat):
        return lax.dot_general(k_blk, ds_mat, (((0,), (0,)), ((), ())), preferred_element_type=jnp.float32)

    def key_iota(keys, width):
        return lax.broadcasted_iota(jnp.int32, (keys, width), 0)

    half = qrows // 2

    def own_half(first, keys):
        cols = pl.ds(first, half)
        q_blk, do_blk, k_blk = q_loc[cols], do_loc[cols], k_loc[0:keys]
        key_pos = key_iota(keys, half)
        tok = lax.broadcasted_iota(jnp.int32, (keys, half), 1) // 2 + first // 2
        keep = (key_pos >= starts[0, :, cols] - me * rows) & (key_pos <= tok)
        p_low, ds_mat = block(k_blk, v_loc[0:keys], q_blk, do_blk, stat_loc[0:1, cols], stat_loc[1:2, cols], keep)
        dqt[:, cols] = dq_term(k_blk, ds_mat)
        dv_new = jnp.dot(p_low, do_blk, preferred_element_type=jnp.float32)
        dk_new = jnp.dot(ds_mat, q_blk, preferred_element_type=jnp.float32)
        if keys == rows:
            dv_acc[...] = dv_new
            dk_acc[...] = dk_new
        else:
            dv_acc[0:keys] = dv_acc[0:keys] + dv_new
            dk_acc[0:keys] = dk_acc[0:keys] + dk_new

    own_half(half, rows)
    own_half(0, rows // 2)

    def finish_dq():
        dq_out[...] = (jnp.transpose(dqt[...]) * scale).astype(jnp.bfloat16)

    def kv_block(slot, first_row, count, first_key):
        cols = pl.ds(first_row, count)
        keys = pl.ds(first_key, rows - first_key)
        base = (me - 1 - slot) * rows + first_key
        keep = key_iota(rows - first_key, count) >= starts[0, :, cols] - base
        k_blk = k_buf[slot, keys]
        _, ds_mat = block(k_blk, v_buf[slot, keys], q_loc[cols], do_loc[cols], stat_loc[0:1, cols], stat_loc[1:2, cols], keep)
        dqt[:, cols] = dqt[:, cols] + dq_term(k_blk, ds_mat)

    def kv_unit(slot):
        @pl.when(slot < HOPS - 1)
        def _():
            kv_block(slot, 0, qrows, 0)

        @pl.when(slot == HOPS - 1)
        def _():
            kv_block(slot, 0, half, 0)
            kv_block(slot, half, half, rows // 2)

    def qd_block(slot, first_row, count, first_key):
        cols = pl.ds(pl.multiple_of(first_row, 128), count)
        keys = pl.ds(first_key, rows - first_key)
        q_blk = q_buf[slot, cols]
        do_blk = do_buf[slot, cols]
        keep = key_iota(rows - first_key, count) >= starts[slot + 1, :, cols] - (me * rows + first_key)
        p_low, ds_mat = block(k_loc[keys], v_loc[keys], q_blk, do_blk, stat_buf[slot, 0:1, cols], stat_buf[slot, 1:2, cols], keep)
        dv_acc[keys] = dv_acc[keys] + jnp.dot(p_low, do_blk, preferred_element_type=jnp.float32)
        dk_acc[keys] = dk_acc[keys] + jnp.dot(ds_mat, q_blk, preferred_element_type=jnp.float32)

    def qd_unit(slot, chunk):
        quarters = (slot == tail) & (chunk >= 2)
        short = (slot == HOPS - 1) & (chunk == 3)

        @pl.when(quarters)
        def _():
            qd_block(slot, chunk * qc_rows, qc_rows, 0)

        @pl.when((chunk % 2 == 1) & jnp.logical_not(quarters) & jnp.logical_not(short))
        def _():
            qd_block(slot, (chunk - 1) * qc_rows, half, 0)

        @pl.when(short & jnp.logical_not(quarters))
        def _():
            qd_block(slot, half, half, rows // 2)

    tail = lut([t - 1 for t in TAIL])
    last_kv = lut([max([-1] + [i for i, c in enumerate(step_codes(ORDER[d])) if c < 3 * NK and d > c // NK]) for d in range(8)])

    @pl.when(me == 0)
    def _():
        finish_dq()

    kv_on = [lut(targets_of(KV_REL, lambda d, h=h: (d, h + 1))) for h in range(HOPS)]
    qd_on = [lut(targets_of(QD_REL, lambda d, h=h: (d, h + 1))) for h in range(HOPS)]

    def pick(values, slot):
        return jnp.where(slot == 0, values[0], jnp.where(slot == 1, values[1], values[2]))

    per_word = 6
    codes = {d: step_codes(ORDER[d]) for d in range(8)}
    steps = max(len(c) for c in codes.values())
    words = -(-steps // per_word)
    packed = []
    for w in range(words):
        values = []
        for d in range(8):
            part = (codes[d] + [NONE] * (words * per_word))[w * per_word:(w + 1) * per_word]
            values.append(sum(c * 32 ** i for i, c in enumerate(part)))
        packed.append(lut(values))

    def step(i, carry):
        code = carry[0] % 32

        @pl.when(code < 3 * NK)
        def _():
            slot, chunk = code // NK, code % NK
            to = pick(kv_on, slot)
            for copy in kv_copies(k_buf.at[slot], v_buf.at[slot], kv_rel.at[slot], me * 4 + slot + 1, chunk):
                copy.wait_recv()

            @pl.when(to != NOBODY)
            def _():
                for copy in kv_copies(k_buf.at[slot], v_buf.at[slot], kv_rel.at[slot], to, chunk):
                    copy.start()

            @pl.when((me > slot) & (chunk == NK - 1))
            def _():
                kv_unit(slot)

            @pl.when(i == last_kv)
            def _():
                finish_dq()

        @pl.when((code >= 3 * NK) & (code < SEND))
        def _():
            slot, chunk = (code - 3 * NK) // NQ, (code - 3 * NK) % NQ
            to = pick(qd_on, slot)
            for copy in qd_copies(q_buf.at[slot], do_buf.at[slot], qd_rel.at[slot], me * 4 + slot + 1, chunk):
                copy.wait_recv()

            @pl.when(to != NOBODY)
            def _():
                for copy in qd_copies(q_buf.at[slot], do_buf.at[slot], qd_rel.at[slot], to, chunk):
                    copy.start()

            @pl.when(chunk == 0)
            def _():
                stat_copy(stat_buf.at[slot], stat_rel.at[slot], me * 4 + slot + 1).wait_recv()

                @pl.when(to != NOBODY)
                def _():
                    stat_copy(stat_buf.at[slot], stat_rel.at[slot], to).start()

            @pl.when(me + slot < 7)
            def _():
                qd_unit(slot, chunk)

        @pl.when(code == SEND)
        def _():
            send_later()

        last = (i % per_word) == per_word - 1
        rest = [jnp.where(last, (carry + (jnp.int32(0),))[w + 1], carry[w] // 32 if w == 0 else carry[w]) for w in range(words)]
        return tuple(rest)

    lax.fori_loop(0, steps, step, tuple(packed))

    dk_out[...] = (dk_acc[...] * scale).astype(jnp.bfloat16)
    dv_out[...] = dv_acc[...].astype(jnp.bfloat16)

    def sent(ref, sem):
        pltpu.make_async_remote_copy(src_ref=ref, dst_ref=ref, send_sem=sem, recv_sem=sem, device_id=place(me), device_id_type=MESH).wait_send()

    for targets, kv_sem in ((kv_to, kv_own), (kv_on, kv_rel)):
        for n, target in enumerate(targets):
            @pl.when(target != NOBODY)
            def _(n=n, kv_sem=kv_sem):
                sent(q_buf.at[0], kv_sem.at[n])
    for targets, qd_sem, stat_sem in ((qd_to, qd_own, stat_own), (qd_on, qd_rel, stat_rel)):
        for n, target in enumerate(targets):
            @pl.when(target != NOBODY)
            def _(n=n, qd_sem=qd_sem, stat_sem=stat_sem):
                sent(q_buf.at[0:2], qd_sem.at[n])
                sent(stat_loc, stat_sem.at[n])


def store_body(dq_ref, dk_ref, dv_ref, dq_out, dk_out, dv_out, sems):
    pairs = ((dq_ref, dq_out), (dk_ref, dk_out), (dv_ref, dv_out))
    copies = [pltpu.make_async_copy(src, dst, sems.at[i]) for i, (src, dst) in enumerate(pairs)]
    for copy in copies:
        copy.start()
    for copy in copies:
        copy.wait()


def solution(mesh):
    def local(queries, keys, values, attn_out, logsumexp, d_out, cu_seqlens):
        rows, heads, head = queries.shape
        qrows = rows * heads
        bf, f32 = jnp.bfloat16, jnp.float32
        dma = pltpu.SemaphoreType.DMA
        any_spec = pl.BlockSpec(memory_space=pl.ANY)
        vmem_spec = pl.BlockSpec(memory_space=pltpu.VMEM)
        shapes = ((qrows, head), (rows, head), (rows, head))
        results = pl.pallas_call(
            body,
            name="packed_backward",
            out_shape=tuple(pltpu.VMEM(shape, bf) for shape in shapes),
            in_specs=[any_spec] * 7,
            out_specs=(vmem_spec,) * 3,
            scratch_shapes=[
                pltpu.VMEM((qrows, head), bf), pltpu.VMEM((rows, head), bf), pltpu.VMEM((rows, head), bf),
                pltpu.VMEM((qrows, head), bf), pltpu.VMEM((heads, rows), f32), pltpu.VMEM((qrows, head), bf),
                pltpu.VMEM((2, qrows), f32), pltpu.VMEM((HOPS + 1, 1, qrows), jnp.int32),
                pltpu.VMEM((HOPS, rows, head), bf), pltpu.VMEM((HOPS, rows, head), bf),
                pltpu.VMEM((HOPS, qrows, head), bf), pltpu.VMEM((HOPS, qrows, head), bf), pltpu.VMEM((HOPS, 2, qrows), f32),
                pltpu.VMEM((head, qrows), f32), pltpu.VMEM((rows, head), f32), pltpu.VMEM((rows, head), f32),
                pltpu.SMEM(cu_seqlens.shape, jnp.int32), dma((7,)), pltpu.SemaphoreType.REGULAR,
                dma((HOPS, NK)), dma((HOPS, NK)), dma((HOPS, NQ)), dma((HOPS, NQ)), dma((HOPS,)),
                dma((2,)), dma((2,)), dma((2,)), dma((HOPS,)), dma((HOPS,)), dma((HOPS,)),
            ],
            compiler_params=pltpu.CompilerParams(collective_id=0, has_side_effects=True),
        )(cu_seqlens, queries.reshape(qrows, head), keys, values, attn_out.reshape(qrows, head), logsumexp.T, d_out.reshape(qrows, head))
        d_query, d_key, d_value = pl.pallas_call(
            store_body,
            name="store",
            out_shape=tuple(jax.ShapeDtypeStruct(shape, bf) for shape in shapes),
            in_specs=[vmem_spec] * 3,
            out_specs=(any_spec,) * 3,
            scratch_shapes=[dma((3,))],
        )(*[pltpu.with_memory_space_constraint(x, pltpu.VMEM) for x in results])
        return d_query.reshape(rows, heads, head), d_key, d_value

    seq_spec = P(("dp", "cpo", "cp"))
    return jax.shard_map(local, mesh=mesh, in_specs=(seq_spec,) * 6 + (P("dp"),), out_specs=(seq_spec,) * 3, check_vma=False)
```

```python
import functools
import math

import jax
import jax.numpy as jnp
from jax import lax
from jax.experimental import pallas as pl
from jax.experimental.pallas import tpu as pltpu
from jax.sharding import PartitionSpec as P

MESH = pl.DeviceIdType.MESH
HOPS = 3
NK = 2
NQ = 4
NONE = 31
NOBODY = 63
SEND = 18

KV_OWN = {0: [(1, 1), (2, 2)], 1: [(3, 2), (4, 3)], 2: [(3, 1), (4, 2)], 3: [(6, 3)], 4: [(5, 1), (6, 2)], 5: [(7, 2)], 6: [(7, 1)], 7: []}
QD_OWN = {0: [], 1: [(0, 1)], 2: [(0, 2)], 3: [(2, 1), (1, 2)], 4: [(1, 3)], 5: [(4, 1), (3, 2)], 6: [(4, 2), (3, 3)], 7: [(6, 1), (5, 2)]}
KV_FAR = 2
QD_FAR = 5
FIRST = {
    0: (0, 10, 1, 11),
    1: (0, 10, 1, 11, 100),
    2: (0, 1, 100),
    3: (0, 1, 100, 110),
    4: (0, 10, 1, 11, 100),
    5: (0, 100),
    6: (0, 1, 110, 100),
    7: (100, 110),
}
REST = {
    1: (101, 102, 103),
    3: (101, 111, 102, 103),
    4: (101, 102, 103),
    5: (110, 1, 101, 102, 103, 111, 112, 113),
    6: (111, 112, 113, 101),
    7: (101, 111, 102, 103),
}
LATER = {
    2: (10, 11, 101, 102, 103),
    3: (112, 113),
    6: (102, 103),
    7: (112, 113),
}
TAIL = (2, 3, 0, 0, 2, 3, 0, 0)
FAR_NEWS = ((0, 2, 4), (7, 5, 3))
KV_REL = {(2, 2): (3, 3), (3, 2): (2, 1), (4, 2): (5, 3), (4, 1): (5, 2), (6, 3): (4, 1), (6, 2): (7, 3), (7, 2): (6, 1)}
QD_REL = {(0, 2): (1, 1), (1, 2): (0, 3), (1, 3): (3, 1), (3, 1): (2, 2), (3, 2): (2, 3), (4, 2): (5, 1), (5, 2): (4, 3)}
ORDER = ("sghijkoplmnqr", "saobkpqlrghminj", "sghijcadbkolpmqnr", "abcedfsgkhlimjnopqr", "sgheijkfolpcadbmnqr", "sabkglhecfdminj", "gehijcfsadb", "abcefds")


def step_codes(letters):
    return [ord(x) - ord("a") for x in letters]


def targets_of(table, pick):
    pairs = [table.get(pick(d), NOBODY) for d in range(8)]
    return [p if p == NOBODY else p[0] * 4 + p[1] for p in pairs]


def nth(table, n):
    return [NOBODY if len(table[d]) <= n else table[d][n][0] * 4 + table[d][n][1] for d in range(8)]


def partners():
    near = {d: set() for d in range(8)}
    for table in (KV_OWN, QD_OWN):
        for d, pairs in table.items():
            for n, (target, _) in enumerate(pairs):
                if n == 1 and d == (KV_FAR if table is KV_OWN else QD_FAR):
                    continue
                near[d].add(target)
                near[target].add(d)
    for messenger, far, target in FAR_NEWS:
        for other in (far, target):
            near[messenger].add(other)
            near[other].add(messenger)
    for table in (KV_REL, QD_REL):
        for (d, _), (target, _) in table.items():
            near[d].add(target)
            near[target].add(d)
    return near


def body(
    cu_hbm, q_hbm, k_hbm, v_hbm, o_hbm, lse_hbm, do_hbm,
    dq_out, dk_out, dv_out,
    q_loc, k_loc, v_loc, o_loc, lse_loc, do_loc, stat_loc, starts,
    k_buf, v_buf, q_buf, do_buf, stat_buf,
    dqt, dk_acc, dv_acc, cu_ref, in_sem, far_sem,
    k_recv, v_recv, q_recv, do_recv, stat_recv,
    kv_own, qd_own, stat_own, kv_rel, qd_rel, stat_rel,
):
    rows = k_loc.shape[0]
    qrows = q_loc.shape[0]
    head = k_loc.shape[1]
    kc_rows = rows // NK
    qc_rows = qrows // NQ
    scale = head ** -0.5
    factor = scale * math.log2(math.e)
    me = lax.axis_index("cpo") * 4 + lax.axis_index("cp")

    def lut(values):
        out = jnp.int32(values[0])
        for d in range(1, len(values)):
            out = jnp.where(me == d, jnp.int32(values[d]), out)
        return out

    def place(target):
        return {"cpo": target // 4, "cp": target % 4}

    barrier = pltpu.get_barrier_semaphore()
    near = partners()
    for d in range(8):
        @pl.when(me == d)
        def _(d=d):
            for other in sorted(near[d]):
                pl.semaphore_signal(barrier, inc=1, device_id=place(other), device_id_type=MESH)
    loads = [
        pltpu.make_async_copy(src, dst, in_sem.at[i])
        for i, (src, dst) in enumerate(
            [(k_hbm, k_loc), (v_hbm, v_loc), (q_hbm, q_loc), (do_hbm, do_loc), (o_hbm, o_loc), (lse_hbm, lse_loc), (cu_hbm, cu_ref)]
        )
    ]
    for load in loads:
        load.start()
    for d in range(8):
        @pl.when(me == d)
        def _(d=d):
            pl.semaphore_wait(barrier, len(near[d]))
            for messenger, far, _ in FAR_NEWS:
                if messenger == d:
                    pl.semaphore_signal(far_sem, inc=1, device_id=place(far), device_id_type=MESH)

    def kv_copies(src_k, src_v, sem, code, chunk):
        target, there = code // 4, code % 4 - 1
        part = pl.ds(chunk * kc_rows, kc_rows)
        return [
            pltpu.make_async_remote_copy(
                src_ref=src.at[part], dst_ref=buf.at[there, part], send_sem=sem, recv_sem=recv.at[there, chunk],
                device_id=place(target), device_id_type=MESH)
            for src, buf, recv in ((src_k, k_buf, k_recv), (src_v, v_buf, v_recv))
        ]

    def qd_copies(src_q, src_do, sem, code, chunk):
        target, there = code // 4, code % 4 - 1
        part = pl.ds(chunk * qc_rows, qc_rows)
        return [
            pltpu.make_async_remote_copy(
                src_ref=src.at[part], dst_ref=buf.at[there, part], send_sem=sem, recv_sem=recv.at[there, chunk],
                device_id=place(target), device_id_type=MESH)
            for src, buf, recv in ((src_q, q_buf, q_recv), (src_do, do_buf, do_recv))
        ]

    def stat_copy(src, sem, code):
        target, there = code // 4, code % 4 - 1
        return pltpu.make_async_remote_copy(
            src_ref=src, dst_ref=stat_buf.at[there], send_sem=sem, recv_sem=stat_recv.at[there],
            device_id=place(target), device_id_type=MESH)

    kv_to = [lut(nth(KV_OWN, n)) for n in range(2)]
    qd_to = [lut(nth(QD_OWN, n)) for n in range(2)]

    def send(d, item):
        kind, n, chunk = item // 100, item // 10 % 10, item % 10
        target, there = (KV_OWN, QD_OWN)[kind][d][n]
        code = target * 4 + there
        if kind == 0:
            copies = kv_copies(k_loc, v_loc, kv_own.at[n], code, chunk)
        else:
            copies = qd_copies(q_loc, do_loc, qd_own.at[n], code, chunk)
        for copy in copies:
            copy.start()

    def send_stat(d, n):
        target, there = QD_OWN[d][n]
        stat_copy(stat_loc, stat_own.at[n], target * 4 + there).start()

    loads[0].wait()
    loads[1].wait()
    for d in range(8):
        @pl.when(me == d)
        def _(d=d):
            for item in FIRST[d]:
                if item < 100:
                    send(d, item)
    loads[2].wait()
    loads[3].wait()
    for d in range(8):
        @pl.when(me == d)
        def _(d=d):
            for item in FIRST[d]:
                if item >= 100:
                    send(d, item)
    loads[4].wait()
    loads[5].wait()

    wide = lax.broadcasted_iota(jnp.int32, (2, 128), 1)
    for j in range(qrows // 128):
        src = lse_loc[:, 128 * (j // 2):128 * (j // 2 + 1)]
        both = jnp.take_along_axis(src, 64 * (j % 2) + wide // 2, axis=1, mode="promise_in_bounds")
        row = jnp.where(wide[0:1] % 2 == 0, both[0:1], both[1:2])
        stat_loc[0:1, 128 * j:128 * (j + 1)] = row * math.log2(math.e)
    ones = jnp.ones((8, head), jnp.bfloat16)
    for j in range(qrows // 256):
        part = pl.ds(256 * j, 256)
        prod = do_loc[part].astype(jnp.float32) * o_loc[part].astype(jnp.float32)
        hi = prod.astype(jnp.bfloat16)
        lo = (prod - hi.astype(jnp.float32)).astype(jnp.bfloat16)
        dims = (((1,), (1,)), ((), ()))
        total = lax.dot_general(ones, hi, dims, preferred_element_type=jnp.float32)
        total = total + lax.dot_general(ones, lo, dims, preferred_element_type=jnp.float32)
        stat_loc[1:2, 256 * j:256 * (j + 1)] = total[0:1]
    for d in range(8):
        @pl.when(me == d)
        def _(d=d):
            for n in range(len(QD_OWN[d])):
                if not (d == QD_FAR and n == 1):
                    send_stat(d, n)
            if d == QD_FAR:
                pl.semaphore_wait(far_sem, 1)
                send_stat(d, 1)
            for item in REST.get(d, ()):
                send(d, item)

    loads[6].wait()
    lane = lax.broadcasted_iota(jnp.int32, (1, qrows), 1) // 2
    for h in range(HOPS + 1):
        pos = lane + (me + h) * rows
        start = jnp.zeros_like(pos)
        for j in range(cu_ref.shape[0]):
            start = jnp.maximum(start, jnp.where(pos >= cu_ref[j], cu_ref[j], 0))
        starts[h] = start

    def send_later():
        for d in LATER:
            @pl.when(me == d)
            def _(d=d):
                if d == KV_FAR:
                    pl.semaphore_wait(far_sem, 1)
                for item in LATER[d]:
                    send(d, item)

    def block(k_blk, v_blk, q_blk, do_blk, lse_row, d_row, keep):
        dims = (((1,), (1,)), ((), ()))
        scores = lax.dot_general(k_blk, q_blk, dims, preferred_element_type=jnp.float32)
        p_mat = jnp.where(keep, jnp.exp2(scores * factor - lse_row), 0.0)
        dp_mat = lax.dot_general(v_blk, do_blk, dims, preferred_element_type=jnp.float32)
        ds_mat = (p_mat * (dp_mat - d_row)).astype(jnp.bfloat16)
        return p_mat.astype(jnp.bfloat16), ds_mat

    def dq_term(k_blk, ds_mat):
        return lax.dot_general(k_blk, ds_mat, (((0,), (0,)), ((), ())), preferred_element_type=jnp.float32)

    def key_iota(keys, width):
        return lax.broadcasted_iota(jnp.int32, (keys, width), 0)

    half = qrows // 2

    def own_half(first, keys):
        cols = pl.ds(first, half)
        q_blk, do_blk, k_blk = q_loc[cols], do_loc[cols], k_loc[0:keys]
        key_pos = key_iota(keys, half)
        tok = lax.broadcasted_iota(jnp.int32, (keys, half), 1) // 2 + first // 2
        keep = (key_pos >= starts[0, :, cols] - me * rows) & (key_pos <= tok)
        p_low, ds_mat = block(k_blk, v_loc[0:keys], q_blk, do_blk, stat_loc[0:1, cols], stat_loc[1:2, cols], keep)
        dqt[:, cols] = dq_term(k_blk, ds_mat)
        dv_new = jnp.dot(p_low, do_blk, preferred_element_type=jnp.float32)
        dk_new = jnp.dot(ds_mat, q_blk, preferred_element_type=jnp.float32)
        if keys == rows:
            dv_acc[...] = dv_new
            dk_acc[...] = dk_new
        else:
            dv_acc[0:keys] = dv_acc[0:keys] + dv_new
            dk_acc[0:keys] = dk_acc[0:keys] + dk_new

    own_half(half, rows)
    own_half(0, rows // 2)

    def finish_dq():
        dq_out[...] = (jnp.transpose(dqt[...]) * scale).astype(jnp.bfloat16)

    def kv_block(slot, first_row, count, first_key):
        cols = pl.ds(first_row, count)
        keys = pl.ds(first_key, rows - first_key)
        base = (me - 1 - slot) * rows + first_key
        keep = key_iota(rows - first_key, count) >= starts[0, :, cols] - base
        k_blk = k_buf[slot, keys]
        _, ds_mat = block(k_blk, v_buf[slot, keys], q_loc[cols], do_loc[cols], stat_loc[0:1, cols], stat_loc[1:2, cols], keep)
        dqt[:, cols] = dqt[:, cols] + dq_term(k_blk, ds_mat)

    def kv_unit(slot):
        @pl.when(slot < HOPS - 1)
        def _():
            kv_block(slot, 0, qrows, 0)

        @pl.when(slot == HOPS - 1)
        def _():
            kv_block(slot, 0, half, 0)
            kv_block(slot, half, half, rows // 2)

    def qd_block(slot, first_row, count, first_key):
        cols = pl.ds(pl.multiple_of(first_row, 128), count)
        keys = pl.ds(first_key, rows - first_key)
        q_blk = q_buf[slot, cols]
        do_blk = do_buf[slot, cols]
        keep = key_iota(rows - first_key, count) >= starts[slot + 1, :, cols] - (me * rows + first_key)
        p_low, ds_mat = block(k_loc[keys], v_loc[keys], q_blk, do_blk, stat_buf[slot, 0:1, cols], stat_buf[slot, 1:2, cols], keep)
        dv_acc[keys] = dv_acc[keys] + jnp.dot(p_low, do_blk, preferred_element_type=jnp.float32)
        dk_acc[keys] = dk_acc[keys] + jnp.dot(ds_mat, q_blk, preferred_element_type=jnp.float32)

    def qd_unit(slot, chunk):
        quarters = (pick(tail, slot) == 1) & (chunk >= 2)
        short = (slot == HOPS - 1) & (chunk == 3)

        @pl.when(quarters)
        def _():
            qd_block(slot, chunk * qc_rows, qc_rows, 0)

        @pl.when((chunk % 2 == 1) & jnp.logical_not(quarters) & jnp.logical_not(short))
        def _():
            qd_block(slot, (chunk - 1) * qc_rows, half, 0)

        @pl.when(short & jnp.logical_not(quarters))
        def _():
            qd_block(slot, half, half, rows // 2)

    tail = [lut([(t >> h) % 2 for t in TAIL]) for h in range(HOPS)]
    last_kv = lut([max([-1] + [i for i, c in enumerate(step_codes(ORDER[d])) if c < 3 * NK and d > c // NK]) for d in range(8)])

    @pl.when(me == 0)
    def _():
        finish_dq()

    kv_on = [lut(targets_of(KV_REL, lambda d, h=h: (d, h + 1))) for h in range(HOPS)]
    qd_on = [lut(targets_of(QD_REL, lambda d, h=h: (d, h + 1))) for h in range(HOPS)]

    def pick(values, slot):
        return jnp.where(slot == 0, values[0], jnp.where(slot == 1, values[1], values[2]))

    per_word = 6
    codes = {d: step_codes(ORDER[d]) for d in range(8)}
    steps = max(len(c) for c in codes.values())
    words = -(-steps // per_word)
    packed = []
    for w in range(words):
        values = []
        for d in range(8):
            part = (codes[d] + [NONE] * (words * per_word))[w * per_word:(w + 1) * per_word]
            values.append(sum(c * 32 ** i for i, c in enumerate(part)))
        packed.append(lut(values))

    def step(i, carry):
        code = carry[0] % 32

        @pl.when(code < 3 * NK)
        def _():
            slot, chunk = code // NK, code % NK
            to = pick(kv_on, slot)
            for copy in kv_copies(k_buf.at[slot], v_buf.at[slot], kv_rel.at[slot], me * 4 + slot + 1, chunk):
                copy.wait_recv()

            @pl.when(to != NOBODY)
            def _():
                for copy in kv_copies(k_buf.at[slot], v_buf.at[slot], kv_rel.at[slot], to, chunk):
                    copy.start()

            @pl.when((me > slot) & (chunk == NK - 1))
            def _():
                kv_unit(slot)

            @pl.when(i == last_kv)
            def _():
                finish_dq()

        @pl.when((code >= 3 * NK) & (code < SEND))
        def _():
            slot, chunk = (code - 3 * NK) // NQ, (code - 3 * NK) % NQ
            to = pick(qd_on, slot)
            for copy in qd_copies(q_buf.at[slot], do_buf.at[slot], qd_rel.at[slot], me * 4 + slot + 1, chunk):
                copy.wait_recv()

            @pl.when(to != NOBODY)
            def _():
                for copy in qd_copies(q_buf.at[slot], do_buf.at[slot], qd_rel.at[slot], to, chunk):
                    copy.start()

            @pl.when(chunk == 0)
            def _():
                stat_copy(stat_buf.at[slot], stat_rel.at[slot], me * 4 + slot + 1).wait_recv()

                @pl.when(to != NOBODY)
                def _():
                    stat_copy(stat_buf.at[slot], stat_rel.at[slot], to).start()

            @pl.when(me + slot < 7)
            def _():
                qd_unit(slot, chunk)

        @pl.when(code == SEND)
        def _():
            send_later()

        last = (i % per_word) == per_word - 1
        rest = [jnp.where(last, (carry + (jnp.int32(0),))[w + 1], carry[w] // 32 if w == 0 else carry[w]) for w in range(words)]
        return tuple(rest)

    lax.fori_loop(0, steps, step, tuple(packed))

    dk_out[...] = (dk_acc[...] * scale).astype(jnp.bfloat16)
    dv_out[...] = dv_acc[...].astype(jnp.bfloat16)

    def sent(ref, sem):
        pltpu.make_async_remote_copy(src_ref=ref, dst_ref=ref, send_sem=sem, recv_sem=sem, device_id=place(me), device_id_type=MESH).wait_send()

    for targets, kv_sem in ((kv_to, kv_own), (kv_on, kv_rel)):
        for n, target in enumerate(targets):
            @pl.when(target != NOBODY)
            def _(n=n, kv_sem=kv_sem):
                sent(q_buf.at[0], kv_sem.at[n])
    for targets, qd_sem, stat_sem in ((qd_to, qd_own, stat_own), (qd_on, qd_rel, stat_rel)):
        for n, target in enumerate(targets):
            @pl.when(target != NOBODY)
            def _(n=n, qd_sem=qd_sem, stat_sem=stat_sem):
                sent(q_buf.at[0:2], qd_sem.at[n])
                sent(stat_loc, stat_sem.at[n])


def store_body(dq_ref, dk_ref, dv_ref, dq_out, dk_out, dv_out, sems):
    pairs = ((dq_ref, dq_out), (dk_ref, dk_out), (dv_ref, dv_out))
    copies = [pltpu.make_async_copy(src, dst, sems.at[i]) for i, (src, dst) in enumerate(pairs)]
    for copy in copies:
        copy.start()
    for copy in copies:
        copy.wait()


def solution(mesh):
    def local(queries, keys, values, attn_out, logsumexp, d_out, cu_seqlens):
        rows, heads, head = queries.shape
        qrows = rows * heads
        bf, f32 = jnp.bfloat16, jnp.float32
        dma = pltpu.SemaphoreType.DMA
        any_spec = pl.BlockSpec(memory_space=pl.ANY)
        vmem_spec = pl.BlockSpec(memory_space=pltpu.VMEM)
        shapes = ((qrows, head), (rows, head), (rows, head))
        results = pl.pallas_call(
            body,
            name="packed_backward",
            out_shape=tuple(pltpu.VMEM(shape, bf) for shape in shapes),
            in_specs=[any_spec] * 7,
            out_specs=(vmem_spec,) * 3,
            scratch_shapes=[
                pltpu.VMEM((qrows, head), bf), pltpu.VMEM((rows, head), bf), pltpu.VMEM((rows, head), bf),
                pltpu.VMEM((qrows, head), bf), pltpu.VMEM((heads, rows), f32), pltpu.VMEM((qrows, head), bf),
                pltpu.VMEM((2, qrows), f32), pltpu.VMEM((HOPS + 1, 1, qrows), jnp.int32),
                pltpu.VMEM((HOPS, rows, head), bf), pltpu.VMEM((HOPS, rows, head), bf),
                pltpu.VMEM((HOPS, qrows, head), bf), pltpu.VMEM((HOPS, qrows, head), bf), pltpu.VMEM((HOPS, 2, qrows), f32),
                pltpu.VMEM((head, qrows), f32), pltpu.VMEM((rows, head), f32), pltpu.VMEM((rows, head), f32),
                pltpu.SMEM(cu_seqlens.shape, jnp.int32), dma((7,)), pltpu.SemaphoreType.REGULAR,
                dma((HOPS, NK)), dma((HOPS, NK)), dma((HOPS, NQ)), dma((HOPS, NQ)), dma((HOPS,)),
                dma((2,)), dma((2,)), dma((2,)), dma((HOPS,)), dma((HOPS,)), dma((HOPS,)),
            ],
            compiler_params=pltpu.CompilerParams(collective_id=0, has_side_effects=True),
        )(cu_seqlens, queries.reshape(qrows, head), keys, values, attn_out.reshape(qrows, head), logsumexp.T, d_out.reshape(qrows, head))
        d_query, d_key, d_value = pl.pallas_call(
            store_body,
            name="store",
            out_shape=tuple(jax.ShapeDtypeStruct(shape, bf) for shape in shapes),
            in_specs=[vmem_spec] * 3,
            out_specs=(any_spec,) * 3,
            scratch_shapes=[dma((3,))],
        )(*[pltpu.with_memory_space_constraint(x, pltpu.VMEM) for x in results])
        return d_query.reshape(rows, heads, head), d_key, d_value

    seq_spec = P(("dp", "cpo", "cp"))
    return jax.shard_map(local, mesh=mesh, in_specs=(seq_spec,) * 6 + (P("dp"),), out_specs=(seq_spec,) * 3, check_vma=False)
```

```python
import functools
import math

import jax
import jax.numpy as jnp
from jax import lax
from jax.experimental import pallas as pl
from jax.experimental.pallas import tpu as pltpu
from jax.sharding import PartitionSpec as P

MESH = pl.DeviceIdType.MESH
HOPS = 3
NK = 2
NQ = 4
NONE = 31
NOBODY = 63
SEND = 18

KV_OWN = {0: [(1, 1), (2, 2)], 1: [(3, 2), (4, 3)], 2: [(3, 1), (4, 2)], 3: [(6, 3)], 4: [(5, 1), (6, 2)], 5: [(7, 2)], 6: [(7, 1)], 7: []}
QD_OWN = {0: [], 1: [(0, 1)], 2: [(0, 2)], 3: [(2, 1), (1, 2)], 4: [(1, 3)], 5: [(4, 1), (3, 2)], 6: [(4, 2), (3, 3)], 7: [(6, 1), (5, 2)]}
FIRST = {
    0: (0, 10, 1, 11),
    1: (0, 1, 100),
    2: (0, 1, 100),
    3: (100, 110),
    4: (0, 10, 1, 11, 100),
    5: (0, 100),
    6: (0, 1, 110, 100),
    7: (100, 110),
}
REST = {
    1: (101, 102, 103),
    2: (),
    3: (101, 111, 102, 112, 103),
    4: (101, 102, 103),
    5: (110, 101, 1, 111, 112, 113, 102, 103),
    6: (111, 112, 113, 101),
    7: (101, 111, 102, 112, 103),
}
AFTER = {
    1: (10, 11),
    2: (10, 11, 101, 102, 103),
    3: (0, 1),
}
LATER = {
    3: (113,),
    6: (102, 103),
    7: (113,),
}
TAIL = (2, 3, 0, 0, 2, 3, 0, 0)
GO = ((4, 1), (4, 2), (6, 3))
KV_REL = {(2, 2): (3, 3), (3, 2): (2, 1), (4, 2): (5, 3), (4, 1): (5, 2), (6, 3): (4, 1), (6, 2): (7, 3), (7, 2): (6, 1)}
QD_REL = {(0, 2): (1, 1), (1, 2): (0, 3), (1, 3): (3, 1), (3, 1): (2, 2), (3, 2): (2, 3), (4, 2): (5, 1), (5, 2): (4, 3)}
ORDER = ("ghijkoplmqnr", "aobkpqlrghminj", "ghijcadbkolpmqnr", "abcedfsgkhlimjnopqr", "gheijkfolpcadbmqnr", "abkglhecfdminj", "ghijceafsdb", "abcefds")


def step_codes(letters):
    return [ord(x) - ord("a") for x in letters]


def targets_of(table, pick):
    pairs = [table.get(pick(d), NOBODY) for d in range(8)]
    return [p if p == NOBODY else p[0] * 4 + p[1] for p in pairs]


def nth(table, n):
    return [NOBODY if len(table[d]) <= n else table[d][n][0] * 4 + table[d][n][1] for d in range(8)]


def partners():
    near = {d: set() for d in range(8)}
    pairs = [(d, target) for table in (KV_OWN, QD_OWN) for d in table for target, _ in table[d]]
    pairs += [(d, target) for table in (KV_REL, QD_REL) for (d, _), (target, _) in table.items()]
    for a, b in pairs:
        for here, there in ((a, b), (b, a)):
            if here >= 4 or there < 4:
                near[here].add(there)
    return near


def body(
    cu_hbm, q_hbm, k_hbm, v_hbm, o_hbm, lse_hbm, do_hbm,
    dq_out, dk_out, dv_out,
    q_loc, k_loc, v_loc, o_loc, lse_loc, do_loc, stat_loc, starts,
    k_buf, v_buf, q_buf, do_buf, stat_buf,
    dqt, dk_acc, dv_acc, cu_ref, in_sem, go_sem,
    k_recv, v_recv, q_recv, do_recv, stat_recv,
    kv_own, qd_own, stat_own, kv_rel, qd_rel, stat_rel,
):
    rows = k_loc.shape[0]
    qrows = q_loc.shape[0]
    head = k_loc.shape[1]
    kc_rows = rows // NK
    qc_rows = qrows // NQ
    scale = head ** -0.5
    factor = scale * math.log2(math.e)
    me = lax.axis_index("cpo") * 4 + lax.axis_index("cp")

    def lut(values):
        out = jnp.int32(values[0])
        for d in range(1, len(values)):
            out = jnp.where(me == d, jnp.int32(values[d]), out)
        return out

    def place(target):
        return {"cpo": target // 4, "cp": target % 4}

    barrier = pltpu.get_barrier_semaphore()
    near = partners()
    for d in range(8):
        @pl.when(me == d)
        def _(d=d):
            for other in [x for x in range(8) if d in near[x]]:
                pl.semaphore_signal(barrier, inc=1, device_id=place(other), device_id_type=MESH)
    loads = [
        pltpu.make_async_copy(src, dst, in_sem.at[i])
        for i, (src, dst) in enumerate(
            [(k_hbm, k_loc), (v_hbm, v_loc), (q_hbm, q_loc), (do_hbm, do_loc), (o_hbm, o_loc), (lse_hbm, lse_loc), (cu_hbm, cu_ref)]
        )
    ]
    for load in loads:
        load.start()
    for d in range(8):
        @pl.when(me == d)
        def _(d=d):
            pl.semaphore_wait(barrier, len(near[d]))
            for teller, told in GO:
                if teller == d:
                    pl.semaphore_signal(go_sem, inc=1, device_id=place(told), device_id_type=MESH)

    def kv_copies(src_k, src_v, sem, code, chunk):
        target, there = code // 4, code % 4 - 1
        part = pl.ds(chunk * kc_rows, kc_rows)
        return [
            pltpu.make_async_remote_copy(
                src_ref=src.at[part], dst_ref=buf.at[there, part], send_sem=sem, recv_sem=recv.at[there, chunk],
                device_id=place(target), device_id_type=MESH)
            for src, buf, recv in ((src_k, k_buf, k_recv), (src_v, v_buf, v_recv))
        ]

    def qd_copies(src_q, src_do, sem, code, chunk):
        target, there = code // 4, code % 4 - 1
        part = pl.ds(chunk * qc_rows, qc_rows)
        return [
            pltpu.make_async_remote_copy(
                src_ref=src.at[part], dst_ref=buf.at[there, part], send_sem=sem, recv_sem=recv.at[there, chunk],
                device_id=place(target), device_id_type=MESH)
            for src, buf, recv in ((src_q, q_buf, q_recv), (src_do, do_buf, do_recv))
        ]

    def stat_copy(src, sem, code):
        target, there = code // 4, code % 4 - 1
        return pltpu.make_async_remote_copy(
            src_ref=src, dst_ref=stat_buf.at[there], send_sem=sem, recv_sem=stat_recv.at[there],
            device_id=place(target), device_id_type=MESH)

    kv_to = [lut(nth(KV_OWN, n)) for n in range(2)]
    qd_to = [lut(nth(QD_OWN, n)) for n in range(2)]

    def send(d, item):
        kind, n, chunk = item // 100, item // 10 % 10, item % 10
        target, there = (KV_OWN, QD_OWN)[kind][d][n]
        code = target * 4 + there
        if kind == 0:
            copies = kv_copies(k_loc, v_loc, kv_own.at[n], code, chunk)
        else:
            copies = qd_copies(q_loc, do_loc, qd_own.at[n], code, chunk)
        for copy in copies:
            copy.start()

    def send_stat(d, n):
        target, there = QD_OWN[d][n]
        stat_copy(stat_loc, stat_own.at[n], target * 4 + there).start()

    loads[0].wait()
    loads[1].wait()
    for d in range(8):
        @pl.when(me == d)
        def _(d=d):
            for item in FIRST[d]:
                if item < 100:
                    send(d, item)
    loads[2].wait()
    loads[3].wait()
    for d in range(8):
        @pl.when(me == d)
        def _(d=d):
            for item in FIRST[d]:
                if item >= 100:
                    send(d, item)
    loads[4].wait()
    loads[5].wait()

    wide = lax.broadcasted_iota(jnp.int32, (2, 128), 1)
    for j in range(qrows // 128):
        src = lse_loc[:, 128 * (j // 2):128 * (j // 2 + 1)]
        both = jnp.take_along_axis(src, 64 * (j % 2) + wide // 2, axis=1, mode="promise_in_bounds")
        row = jnp.where(wide[0:1] % 2 == 0, both[0:1], both[1:2])
        stat_loc[0:1, 128 * j:128 * (j + 1)] = row * math.log2(math.e)
    ones = jnp.ones((8, head), jnp.bfloat16)
    for j in range(qrows // 256):
        part = pl.ds(256 * j, 256)
        prod = do_loc[part].astype(jnp.float32) * o_loc[part].astype(jnp.float32)
        hi = prod.astype(jnp.bfloat16)
        lo = (prod - hi.astype(jnp.float32)).astype(jnp.bfloat16)
        dims = (((1,), (1,)), ((), ()))
        total = lax.dot_general(ones, hi, dims, preferred_element_type=jnp.float32)
        total = total + lax.dot_general(ones, lo, dims, preferred_element_type=jnp.float32)
        stat_loc[1:2, 256 * j:256 * (j + 1)] = total[0:1]
    for d in range(8):
        @pl.when(me == d)
        def _(d=d):
            for n in range(len(QD_OWN[d])):
                send_stat(d, n)
            for item in REST.get(d, ()):
                send(d, item)

    loads[6].wait()
    lane = lax.broadcasted_iota(jnp.int32, (1, qrows), 1) // 2
    for h in range(HOPS + 1):
        pos = lane + (me + h) * rows
        start = jnp.zeros_like(pos)
        for j in range(cu_ref.shape[0]):
            start = jnp.maximum(start, jnp.where(pos >= cu_ref[j], cu_ref[j], 0))
        starts[h] = start

    def send_later():
        for d in LATER:
            @pl.when(me == d)
            def _(d=d):
                for item in LATER[d]:
                    send(d, item)

    def block(k_blk, v_blk, q_blk, do_blk, lse_row, d_row, keep):
        dims = (((1,), (1,)), ((), ()))
        scores = lax.dot_general(k_blk, q_blk, dims, preferred_element_type=jnp.float32)
        p_mat = jnp.where(keep, jnp.exp2(scores * factor - lse_row), 0.0)
        dp_mat = lax.dot_general(v_blk, do_blk, dims, preferred_element_type=jnp.float32)
        ds_mat = (p_mat * (dp_mat - d_row)).astype(jnp.bfloat16)
        return p_mat.astype(jnp.bfloat16), ds_mat

    def dq_term(k_blk, ds_mat):
        return lax.dot_general(k_blk, ds_mat, (((0,), (0,)), ((), ())), preferred_element_type=jnp.float32)

    def key_iota(keys, width):
        return lax.broadcasted_iota(jnp.int32, (keys, width), 0)

    half = qrows // 2

    def own_half(first, keys):
        cols = pl.ds(first, half)
        q_blk, do_blk, k_blk = q_loc[cols], do_loc[cols], k_loc[0:keys]
        key_pos = key_iota(keys, half)
        tok = lax.broadcasted_iota(jnp.int32, (keys, half), 1) // 2 + first // 2
        keep = (key_pos >= starts[0, :, cols] - me * rows) & (key_pos <= tok)
        p_low, ds_mat = block(k_blk, v_loc[0:keys], q_blk, do_blk, stat_loc[0:1, cols], stat_loc[1:2, cols], keep)
        dqt[:, cols] = dq_term(k_blk, ds_mat)
        dv_new = jnp.dot(p_low, do_blk, preferred_element_type=jnp.float32)
        dk_new = jnp.dot(ds_mat, q_blk, preferred_element_type=jnp.float32)
        if keys == rows:
            dv_acc[...] = dv_new
            dk_acc[...] = dk_new
        else:
            dv_acc[0:keys] = dv_acc[0:keys] + dv_new
            dk_acc[0:keys] = dk_acc[0:keys] + dk_new

    own_half(half, rows)
    for d in AFTER:
        @pl.when(me == d)
        def _(d=d):
            pl.semaphore_wait(go_sem, 1)
            for item in AFTER[d]:
                send(d, item)
    own_half(0, rows // 2)

    def finish_dq():
        dq_out[...] = (jnp.transpose(dqt[...]) * scale).astype(jnp.bfloat16)

    def kv_block(slot, first_row, count, first_key):
        cols = pl.ds(first_row, count)
        keys = pl.ds(first_key, rows - first_key)
        base = (me - 1 - slot) * rows + first_key
        keep = key_iota(rows - first_key, count) >= starts[0, :, cols] - base
        k_blk = k_buf[slot, keys]
        _, ds_mat = block(k_blk, v_buf[slot, keys], q_loc[cols], do_loc[cols], stat_loc[0:1, cols], stat_loc[1:2, cols], keep)
        dqt[:, cols] = dqt[:, cols] + dq_term(k_blk, ds_mat)

    def kv_unit(slot):
        @pl.when(slot < HOPS - 1)
        def _():
            kv_block(slot, 0, qrows, 0)

        @pl.when(slot == HOPS - 1)
        def _():
            kv_block(slot, 0, half, 0)
            kv_block(slot, half, half, rows // 2)

    def qd_block(slot, first_row, count, first_key):
        cols = pl.ds(pl.multiple_of(first_row, 128), count)
        keys = pl.ds(first_key, rows - first_key)
        q_blk = q_buf[slot, cols]
        do_blk = do_buf[slot, cols]
        keep = key_iota(rows - first_key, count) >= starts[slot + 1, :, cols] - (me * rows + first_key)
        p_low, ds_mat = block(k_loc[keys], v_loc[keys], q_blk, do_blk, stat_buf[slot, 0:1, cols], stat_buf[slot, 1:2, cols], keep)
        dv_acc[keys] = dv_acc[keys] + jnp.dot(p_low, do_blk, preferred_element_type=jnp.float32)
        dk_acc[keys] = dk_acc[keys] + jnp.dot(ds_mat, q_blk, preferred_element_type=jnp.float32)

    def qd_unit(slot, chunk):
        quarters = (pick(tail, slot) == 1) & (chunk >= 2)
        short = (slot == HOPS - 1) & (chunk == 3)

        @pl.when(quarters)
        def _():
            qd_block(slot, chunk * qc_rows, qc_rows, 0)

        @pl.when((chunk % 2 == 1) & jnp.logical_not(quarters) & jnp.logical_not(short))
        def _():
            qd_block(slot, (chunk - 1) * qc_rows, half, 0)

        @pl.when(short & jnp.logical_not(quarters))
        def _():
            qd_block(slot, half, half, rows // 2)

    tail = [lut([(t >> h) % 2 for t in TAIL]) for h in range(HOPS)]
    last_kv = lut([max([-1] + [i for i, c in enumerate(step_codes(ORDER[d])) if c < 3 * NK and d > c // NK]) for d in range(8)])

    @pl.when(me == 0)
    def _():
        finish_dq()

    kv_on = [lut(targets_of(KV_REL, lambda d, h=h: (d, h + 1))) for h in range(HOPS)]
    qd_on = [lut(targets_of(QD_REL, lambda d, h=h: (d, h + 1))) for h in range(HOPS)]

    def pick(values, slot):
        return jnp.where(slot == 0, values[0], jnp.where(slot == 1, values[1], values[2]))

    per_word = 6
    codes = {d: step_codes(ORDER[d]) for d in range(8)}
    steps = max(len(c) for c in codes.values())
    words = -(-steps // per_word)
    packed = []
    for w in range(words):
        values = []
        for d in range(8):
            part = (codes[d] + [NONE] * (words * per_word))[w * per_word:(w + 1) * per_word]
            values.append(sum(c * 32 ** i for i, c in enumerate(part)))
        packed.append(lut(values))

    def step(i, carry):
        code = carry[0] % 32

        @pl.when(code < 3 * NK)
        def _():
            slot, chunk = code // NK, code % NK
            to = pick(kv_on, slot)
            for copy in kv_copies(k_buf.at[slot], v_buf.at[slot], kv_rel.at[slot], me * 4 + slot + 1, chunk):
                copy.wait_recv()

            @pl.when(to != NOBODY)
            def _():
                for copy in kv_copies(k_buf.at[slot], v_buf.at[slot], kv_rel.at[slot], to, chunk):
                    copy.start()

            @pl.when((me > slot) & (chunk == NK - 1))
            def _():
                kv_unit(slot)

            @pl.when(i == last_kv)
            def _():
                finish_dq()

        @pl.when((code >= 3 * NK) & (code < SEND))
        def _():
            slot, chunk = (code - 3 * NK) // NQ, (code - 3 * NK) % NQ
            to = pick(qd_on, slot)
            for copy in qd_copies(q_buf.at[slot], do_buf.at[slot], qd_rel.at[slot], me * 4 + slot + 1, chunk):
                copy.wait_recv()

            @pl.when(to != NOBODY)
            def _():
                for copy in qd_copies(q_buf.at[slot], do_buf.at[slot], qd_rel.at[slot], to, chunk):
                    copy.start()

            @pl.when(chunk == 0)
            def _():
                stat_copy(stat_buf.at[slot], stat_rel.at[slot], me * 4 + slot + 1).wait_recv()

                @pl.when(to != NOBODY)
                def _():
                    stat_copy(stat_buf.at[slot], stat_rel.at[slot], to).start()

            @pl.when(me + slot < 7)
            def _():
                qd_unit(slot, chunk)

        @pl.when(code == SEND)
        def _():
            send_later()

        last = (i % per_word) == per_word - 1
        rest = [jnp.where(last, (carry + (jnp.int32(0),))[w + 1], carry[w] // 32 if w == 0 else carry[w]) for w in range(words)]
        return tuple(rest)

    lax.fori_loop(0, steps, step, tuple(packed))

    dk_out[...] = (dk_acc[...] * scale).astype(jnp.bfloat16)
    dv_out[...] = dv_acc[...].astype(jnp.bfloat16)

    def sent(ref, sem):
        pltpu.make_async_remote_copy(src_ref=ref, dst_ref=ref, send_sem=sem, recv_sem=sem, device_id=place(me), device_id_type=MESH).wait_send()

    for targets, kv_sem in ((kv_to, kv_own), (kv_on, kv_rel)):
        for n, target in enumerate(targets):
            @pl.when(target != NOBODY)
            def _(n=n, kv_sem=kv_sem):
                sent(q_buf.at[0], kv_sem.at[n])
    for targets, qd_sem, stat_sem in ((qd_to, qd_own, stat_own), (qd_on, qd_rel, stat_rel)):
        for n, target in enumerate(targets):
            @pl.when(target != NOBODY)
            def _(n=n, qd_sem=qd_sem, stat_sem=stat_sem):
                sent(q_buf.at[0:2], qd_sem.at[n])
                sent(stat_loc, stat_sem.at[n])


def store_body(dq_ref, dk_ref, dv_ref, dq_out, dk_out, dv_out, sems):
    pairs = ((dq_ref, dq_out), (dk_ref, dk_out), (dv_ref, dv_out))
    copies = [pltpu.make_async_copy(src, dst, sems.at[i]) for i, (src, dst) in enumerate(pairs)]
    for copy in copies:
        copy.start()
    for copy in copies:
        copy.wait()


def solution(mesh):
    def local(queries, keys, values, attn_out, logsumexp, d_out, cu_seqlens):
        rows, heads, head = queries.shape
        qrows = rows * heads
        bf, f32 = jnp.bfloat16, jnp.float32
        dma = pltpu.SemaphoreType.DMA
        any_spec = pl.BlockSpec(memory_space=pl.ANY)
        vmem_spec = pl.BlockSpec(memory_space=pltpu.VMEM)
        shapes = ((qrows, head), (rows, head), (rows, head))
        results = pl.pallas_call(
            body,
            name="packed_backward",
            out_shape=tuple(pltpu.VMEM(shape, bf) for shape in shapes),
            in_specs=[any_spec] * 7,
            out_specs=(vmem_spec,) * 3,
            scratch_shapes=[
                pltpu.VMEM((qrows, head), bf), pltpu.VMEM((rows, head), bf), pltpu.VMEM((rows, head), bf),
                pltpu.VMEM((qrows, head), bf), pltpu.VMEM((heads, rows), f32), pltpu.VMEM((qrows, head), bf),
                pltpu.VMEM((2, qrows), f32), pltpu.VMEM((HOPS + 1, 1, qrows), jnp.int32),
                pltpu.VMEM((HOPS, rows, head), bf), pltpu.VMEM((HOPS, rows, head), bf),
                pltpu.VMEM((HOPS, qrows, head), bf), pltpu.VMEM((HOPS, qrows, head), bf), pltpu.VMEM((HOPS, 2, qrows), f32),
                pltpu.VMEM((head, qrows), f32), pltpu.VMEM((rows, head), f32), pltpu.VMEM((rows, head), f32),
                pltpu.SMEM(cu_seqlens.shape, jnp.int32), dma((7,)), pltpu.SemaphoreType.REGULAR,
                dma((HOPS, NK)), dma((HOPS, NK)), dma((HOPS, NQ)), dma((HOPS, NQ)), dma((HOPS,)),
                dma((2,)), dma((2,)), dma((2,)), dma((HOPS,)), dma((HOPS,)), dma((HOPS,)),
            ],
            compiler_params=pltpu.CompilerParams(collective_id=0, has_side_effects=True),
        )(cu_seqlens, queries.reshape(qrows, head), keys, values, attn_out.reshape(qrows, head), logsumexp.T, d_out.reshape(qrows, head))
        d_query, d_key, d_value = pl.pallas_call(
            store_body,
            name="store",
            out_shape=tuple(jax.ShapeDtypeStruct(shape, bf) for shape in shapes),
            in_specs=[vmem_spec] * 3,
            out_specs=(any_spec,) * 3,
            scratch_shapes=[dma((3,))],
        )(*[pltpu.with_memory_space_constraint(x, pltpu.VMEM) for x in results])
        return d_query.reshape(rows, heads, head), d_key, d_value

    seq_spec = P(("dp", "cpo", "cp"))
    return jax.shard_map(local, mesh=mesh, in_specs=(seq_spec,) * 6 + (P("dp"),), out_specs=(seq_spec,) * 3, check_vma=False)
```

```python
import functools
import math

import jax
import jax.numpy as jnp
from jax import lax
from jax.experimental import pallas as pl
from jax.experimental.pallas import tpu as pltpu
from jax.sharding import PartitionSpec as P

MESH = pl.DeviceIdType.MESH
HOPS = 3
NK = 2
NQ = 4
NONE = 31
NOBODY = 63
SEND = 18

KV_OWN = {0: [(1, 1), (2, 2)], 1: [(3, 2), (4, 3)], 2: [(3, 1), (4, 2)], 3: [(6, 3)], 4: [(5, 1), (6, 2)], 5: [(7, 2)], 6: [(7, 1)], 7: []}
QD_OWN = {0: [], 1: [(0, 1)], 2: [(0, 2)], 3: [(2, 1), (1, 2)], 4: [(1, 3)], 5: [(4, 1), (3, 2)], 6: [(4, 2), (3, 3)], 7: [(6, 1), (5, 2)]}
FIRST = {
    0: (0, 10, 1, 11),
    1: (0, 1, 100),
    2: (0, 1, 100),
    3: (100, 110),
    4: (0, 10, 1, 11, 100),
    5: (0, 100),
    6: (0, 1, 110, 100),
    7: (100, 110),
}
REST = {
    1: (101, 102, 103),
    2: (),
    3: (101, 111, 102, 112, 103),
    4: (101, 102, 103),
    5: (110, 101, 1, 111, 112, 113, 102, 103),
    6: (111, 112, 113, 101),
    7: (101, 111, 102, 112, 103),
}
AFTER = {
    1: (10, 11),
    2: (10, 101, 102, 103, 11),
    3: (0, 1),
}
LATER = {
    3: (113,),
    6: (102, 103),
    7: (113,),
}
TAIL = (2, 3, 0, 0, 2, 3, 0, 0)
GO = ((4, 1), (4, 2), (6, 3))
KV_REL = {(2, 2): (3, 3), (3, 2): (2, 1), (4, 2): (5, 3), (4, 1): (5, 2), (6, 3): (4, 1), (6, 2): (7, 3), (7, 2): (6, 1)}
QD_REL = {(0, 2): (1, 1), (1, 2): (0, 3), (1, 3): (3, 1), (3, 1): (2, 2), (3, 2): (2, 3), (4, 2): (5, 1), (5, 2): (4, 3)}
ORDER = ("ghijkoplmqnr", "aobkpqlrghminj", "ghijcadbkolpmqnr", "abcedfsgkhlimjnopqr", "gheijkfolpcabmnqdr", "abkglhecdminjf", "ghijceafsdb", "abcefds")


def step_codes(letters):
    return [ord(x) - ord("a") for x in letters]


def targets_of(table, pick):
    pairs = [table.get(pick(d), NOBODY) for d in range(8)]
    return [p if p == NOBODY else p[0] * 4 + p[1] for p in pairs]


def nth(table, n):
    return [NOBODY if len(table[d]) <= n else table[d][n][0] * 4 + table[d][n][1] for d in range(8)]


def partners():
    near = {d: set() for d in range(8)}
    pairs = [(d, target) for table in (KV_OWN, QD_OWN) for d in table for target, _ in table[d]]
    pairs += [(d, target) for table in (KV_REL, QD_REL) for (d, _), (target, _) in table.items()]
    for a, b in pairs:
        for here, there in ((a, b), (b, a)):
            if here >= 4 or there < 4:
                near[here].add(there)
    return near


def body(
    cu_hbm, q_hbm, k_hbm, v_hbm, o_hbm, lse_hbm, do_hbm,
    dq_out, dk_out, dv_out,
    q_loc, k_loc, v_loc, o_loc, lse_loc, do_loc, stat_loc, starts,
    k_buf, v_buf, q_buf, do_buf, stat_buf,
    dqt, dk_acc, dv_acc, cu_ref, in_sem, go_sem,
    k_recv, v_recv, q_recv, do_recv, stat_recv,
    kv_own, qd_own, stat_own, kv_rel, qd_rel, stat_rel,
):
    rows = k_loc.shape[0]
    qrows = q_loc.shape[0]
    head = k_loc.shape[1]
    kc_rows = rows // NK
    qc_rows = qrows // NQ
    scale = head ** -0.5
    factor = scale * math.log2(math.e)
    me = lax.axis_index("cpo") * 4 + lax.axis_index("cp")

    def lut(values):
        out = jnp.int32(values[0])
        for d in range(1, len(values)):
            out = jnp.where(me == d, jnp.int32(values[d]), out)
        return out

    def place(target):
        return {"cpo": target // 4, "cp": target % 4}

    barrier = pltpu.get_barrier_semaphore()
    near = partners()
    for d in range(8):
        @pl.when(me == d)
        def _(d=d):
            for other in [x for x in range(8) if d in near[x]]:
                pl.semaphore_signal(barrier, inc=1, device_id=place(other), device_id_type=MESH)
    loads = [
        pltpu.make_async_copy(src, dst, in_sem.at[i])
        for i, (src, dst) in enumerate(
            [(k_hbm, k_loc), (v_hbm, v_loc), (q_hbm, q_loc), (do_hbm, do_loc), (o_hbm, o_loc), (lse_hbm, lse_loc), (cu_hbm, cu_ref)]
        )
    ]
    for load in loads:
        load.start()
    for d in range(8):
        @pl.when(me == d)
        def _(d=d):
            pl.semaphore_wait(barrier, len(near[d]))
            for teller, told in GO:
                if teller == d:
                    pl.semaphore_signal(go_sem, inc=1, device_id=place(told), device_id_type=MESH)

    def kv_copies(src_k, src_v, sem, code, chunk):
        target, there = code // 4, code % 4 - 1
        part = pl.ds(chunk * kc_rows, kc_rows)
        return [
            pltpu.make_async_remote_copy(
                src_ref=src.at[part], dst_ref=buf.at[there, part], send_sem=sem, recv_sem=recv.at[there, chunk],
                device_id=place(target), device_id_type=MESH)
            for src, buf, recv in ((src_k, k_buf, k_recv), (src_v, v_buf, v_recv))
        ]

    def qd_copies(src_q, src_do, sem, code, chunk):
        target, there = code // 4, code % 4 - 1
        part = pl.ds(chunk * qc_rows, qc_rows)
        return [
            pltpu.make_async_remote_copy(
                src_ref=src.at[part], dst_ref=buf.at[there, part], send_sem=sem, recv_sem=recv.at[there, chunk],
                device_id=place(target), device_id_type=MESH)
            for src, buf, recv in ((src_q, q_buf, q_recv), (src_do, do_buf, do_recv))
        ]

    def stat_copy(src, sem, code):
        target, there = code // 4, code % 4 - 1
        return pltpu.make_async_remote_copy(
            src_ref=src, dst_ref=stat_buf.at[there], send_sem=sem, recv_sem=stat_recv.at[there],
            device_id=place(target), device_id_type=MESH)

    kv_to = [lut(nth(KV_OWN, n)) for n in range(2)]
    qd_to = [lut(nth(QD_OWN, n)) for n in range(2)]

    def send(d, item):
        kind, n, chunk = item // 100, item // 10 % 10, item % 10
        target, there = (KV_OWN, QD_OWN)[kind][d][n]
        code = target * 4 + there
        if kind == 0:
            copies = kv_copies(k_loc, v_loc, kv_own.at[n], code, chunk)
        else:
            copies = qd_copies(q_loc, do_loc, qd_own.at[n], code, chunk)
        for copy in copies:
            copy.start()

    def send_stat(d, n):
        target, there = QD_OWN[d][n]
        stat_copy(stat_loc, stat_own.at[n], target * 4 + there).start()

    loads[0].wait()
    loads[1].wait()
    for d in range(8):
        @pl.when(me == d)
        def _(d=d):
            for item in FIRST[d]:
                if item < 100:
                    send(d, item)
    loads[2].wait()
    loads[3].wait()
    for d in range(8):
        @pl.when(me == d)
        def _(d=d):
            for item in FIRST[d]:
                if item >= 100:
                    send(d, item)
    loads[4].wait()
    loads[5].wait()

    wide = lax.broadcasted_iota(jnp.int32, (2, 128), 1)
    for j in range(qrows // 128):
        src = lse_loc[:, 128 * (j // 2):128 * (j // 2 + 1)]
        both = jnp.take_along_axis(src, 64 * (j % 2) + wide // 2, axis=1, mode="promise_in_bounds")
        row = jnp.where(wide[0:1] % 2 == 0, both[0:1], both[1:2])
        stat_loc[0:1, 128 * j:128 * (j + 1)] = row * math.log2(math.e)
    ones = jnp.ones((8, head), jnp.bfloat16)
    for j in range(qrows // 256):
        part = pl.ds(256 * j, 256)
        prod = do_loc[part].astype(jnp.float32) * o_loc[part].astype(jnp.float32)
        hi = prod.astype(jnp.bfloat16)
        lo = (prod - hi.astype(jnp.float32)).astype(jnp.bfloat16)
        dims = (((1,), (1,)), ((), ()))
        total = lax.dot_general(ones, hi, dims, preferred_element_type=jnp.float32)
        total = total + lax.dot_general(ones, lo, dims, preferred_element_type=jnp.float32)
        stat_loc[1:2, 256 * j:256 * (j + 1)] = total[0:1]
    for d in range(8):
        @pl.when(me == d)
        def _(d=d):
            for n in range(len(QD_OWN[d])):
                send_stat(d, n)
            for item in REST.get(d, ()):
                send(d, item)

    loads[6].wait()
    lane = lax.broadcasted_iota(jnp.int32, (1, qrows), 1) // 2
    for h in range(HOPS + 1):
        pos = lane + (me + h) * rows
        start = jnp.zeros_like(pos)
        for j in range(cu_ref.shape[0]):
            start = jnp.maximum(start, jnp.where(pos >= cu_ref[j], cu_ref[j], 0))
        starts[h] = start

    def send_later():
        for d in LATER:
            @pl.when(me == d)
            def _(d=d):
                for item in LATER[d]:
                    send(d, item)

    def block(k_blk, v_blk, q_blk, do_blk, lse_row, d_row, keep):
        dims = (((1,), (1,)), ((), ()))
        scores = lax.dot_general(k_blk, q_blk, dims, preferred_element_type=jnp.float32)
        p_mat = jnp.where(keep, jnp.exp2(scores * factor - lse_row), 0.0)
        dp_mat = lax.dot_general(v_blk, do_blk, dims, preferred_element_type=jnp.float32)
        ds_mat = (p_mat * (dp_mat - d_row)).astype(jnp.bfloat16)
        return p_mat.astype(jnp.bfloat16), ds_mat

    def dq_term(k_blk, ds_mat):
        return lax.dot_general(k_blk, ds_mat, (((0,), (0,)), ((), ())), preferred_element_type=jnp.float32)

    def key_iota(keys, width):
        return lax.broadcasted_iota(jnp.int32, (keys, width), 0)

    half = qrows // 2

    def own_half(first, keys):
        cols = pl.ds(first, half)
        q_blk, do_blk, k_blk = q_loc[cols], do_loc[cols], k_loc[0:keys]
        key_pos = key_iota(keys, half)
        tok = lax.broadcasted_iota(jnp.int32, (keys, half), 1) // 2 + first // 2
        keep = (key_pos >= starts[0, :, cols] - me * rows) & (key_pos <= tok)
        p_low, ds_mat = block(k_blk, v_loc[0:keys], q_blk, do_blk, stat_loc[0:1, cols], stat_loc[1:2, cols], keep)
        dqt[:, cols] = dq_term(k_blk, ds_mat)
        dv_new = jnp.dot(p_low, do_blk, preferred_element_type=jnp.float32)
        dk_new = jnp.dot(ds_mat, q_blk, preferred_element_type=jnp.float32)
        if keys == rows:
            dv_acc[...] = dv_new
            dk_acc[...] = dk_new
        else:
            dv_acc[0:keys] = dv_acc[0:keys] + dv_new
            dk_acc[0:keys] = dk_acc[0:keys] + dk_new

    own_half(half, rows)
    for d in AFTER:
        @pl.when(me == d)
        def _(d=d):
            pl.semaphore_wait(go_sem, 1)
            for item in AFTER[d]:
                send(d, item)
    own_half(0, rows // 2)

    def finish_dq():
        dq_out[...] = (jnp.transpose(dqt[...]) * scale).astype(jnp.bfloat16)

    def kv_block(slot, first_row, count, first_key):
        cols = pl.ds(first_row, count)
        keys = pl.ds(first_key, rows - first_key)
        base = (me - 1 - slot) * rows + first_key
        keep = key_iota(rows - first_key, count) >= starts[0, :, cols] - base
        k_blk = k_buf[slot, keys]
        _, ds_mat = block(k_blk, v_buf[slot, keys], q_loc[cols], do_loc[cols], stat_loc[0:1, cols], stat_loc[1:2, cols], keep)
        dqt[:, cols] = dqt[:, cols] + dq_term(k_blk, ds_mat)

    def kv_unit(slot):
        @pl.when(slot < HOPS - 1)
        def _():
            kv_block(slot, 0, qrows, 0)

        @pl.when(slot == HOPS - 1)
        def _():
            kv_block(slot, 0, half, 0)
            kv_block(slot, half, half, rows // 2)

    def qd_block(slot, first_row, count, first_key):
        cols = pl.ds(pl.multiple_of(first_row, 128), count)
        keys = pl.ds(first_key, rows - first_key)
        q_blk = q_buf[slot, cols]
        do_blk = do_buf[slot, cols]
        keep = key_iota(rows - first_key, count) >= starts[slot + 1, :, cols] - (me * rows + first_key)
        p_low, ds_mat = block(k_loc[keys], v_loc[keys], q_blk, do_blk, stat_buf[slot, 0:1, cols], stat_buf[slot, 1:2, cols], keep)
        dv_acc[keys] = dv_acc[keys] + jnp.dot(p_low, do_blk, preferred_element_type=jnp.float32)
        dk_acc[keys] = dk_acc[keys] + jnp.dot(ds_mat, q_blk, preferred_element_type=jnp.float32)

    def qd_unit(slot, chunk):
        quarters = (pick(tail, slot) == 1) & (chunk >= 2)
        short = (slot == HOPS - 1) & (chunk == 3)

        @pl.when(quarters)
        def _():
            qd_block(slot, chunk * qc_rows, qc_rows, 0)

        @pl.when((chunk % 2 == 1) & jnp.logical_not(quarters) & jnp.logical_not(short))
        def _():
            qd_block(slot, (chunk - 1) * qc_rows, half, 0)

        @pl.when(short & jnp.logical_not(quarters))
        def _():
            qd_block(slot, half, half, rows // 2)

    tail = [lut([(t >> h) % 2 for t in TAIL]) for h in range(HOPS)]
    last_kv = lut([max([-1] + [i for i, c in enumerate(step_codes(ORDER[d])) if c < 3 * NK and d > c // NK]) for d in range(8)])

    @pl.when(me == 0)
    def _():
        finish_dq()

    kv_on = [lut(targets_of(KV_REL, lambda d, h=h: (d, h + 1))) for h in range(HOPS)]
    qd_on = [lut(targets_of(QD_REL, lambda d, h=h: (d, h + 1))) for h in range(HOPS)]

    def pick(values, slot):
        return jnp.where(slot == 0, values[0], jnp.where(slot == 1, values[1], values[2]))

    per_word = 6
    codes = {d: step_codes(ORDER[d]) for d in range(8)}
    steps = max(len(c) for c in codes.values())
    words = -(-steps // per_word)
    packed = []
    for w in range(words):
        values = []
        for d in range(8):
            part = (codes[d] + [NONE] * (words * per_word))[w * per_word:(w + 1) * per_word]
            values.append(sum(c * 32 ** i for i, c in enumerate(part)))
        packed.append(lut(values))

    def step(i, carry):
        code = carry[0] % 32

        @pl.when(code < 3 * NK)
        def _():
            slot, chunk = code // NK, code % NK
            to = pick(kv_on, slot)
            for copy in kv_copies(k_buf.at[slot], v_buf.at[slot], kv_rel.at[slot], me * 4 + slot + 1, chunk):
                copy.wait_recv()

            @pl.when(to != NOBODY)
            def _():
                for copy in kv_copies(k_buf.at[slot], v_buf.at[slot], kv_rel.at[slot], to, chunk):
                    copy.start()

            @pl.when((me > slot) & (chunk == NK - 1))
            def _():
                kv_unit(slot)

            @pl.when(i == last_kv)
            def _():
                finish_dq()

        @pl.when((code >= 3 * NK) & (code < SEND))
        def _():
            slot, chunk = (code - 3 * NK) // NQ, (code - 3 * NK) % NQ
            to = pick(qd_on, slot)
            for copy in qd_copies(q_buf.at[slot], do_buf.at[slot], qd_rel.at[slot], me * 4 + slot + 1, chunk):
                copy.wait_recv()

            @pl.when(to != NOBODY)
            def _():
                for copy in qd_copies(q_buf.at[slot], do_buf.at[slot], qd_rel.at[slot], to, chunk):
                    copy.start()

            @pl.when(chunk == 0)
            def _():
                stat_copy(stat_buf.at[slot], stat_rel.at[slot], me * 4 + slot + 1).wait_recv()

                @pl.when(to != NOBODY)
                def _():
                    stat_copy(stat_buf.at[slot], stat_rel.at[slot], to).start()

            @pl.when(me + slot < 7)
            def _():
                qd_unit(slot, chunk)

        @pl.when(code == SEND)
        def _():
            send_later()

        last = (i % per_word) == per_word - 1
        rest = [jnp.where(last, (carry + (jnp.int32(0),))[w + 1], carry[w] // 32 if w == 0 else carry[w]) for w in range(words)]
        return tuple(rest)

    lax.fori_loop(0, steps, step, tuple(packed))

    dk_out[...] = (dk_acc[...] * scale).astype(jnp.bfloat16)
    dv_out[...] = dv_acc[...].astype(jnp.bfloat16)

    def sent(ref, sem):
        pltpu.make_async_remote_copy(src_ref=ref, dst_ref=ref, send_sem=sem, recv_sem=sem, device_id=place(me), device_id_type=MESH).wait_send()

    for targets, kv_sem in ((kv_to, kv_own), (kv_on, kv_rel)):
        for n, target in enumerate(targets):
            @pl.when(target != NOBODY)
            def _(n=n, kv_sem=kv_sem):
                sent(q_buf.at[0], kv_sem.at[n])
    for targets, qd_sem, stat_sem in ((qd_to, qd_own, stat_own), (qd_on, qd_rel, stat_rel)):
        for n, target in enumerate(targets):
            @pl.when(target != NOBODY)
            def _(n=n, qd_sem=qd_sem, stat_sem=stat_sem):
                sent(q_buf.at[0:2], qd_sem.at[n])
                sent(stat_loc, stat_sem.at[n])


def store_body(dq_ref, dk_ref, dv_ref, dq_out, dk_out, dv_out, sems):
    pairs = ((dq_ref, dq_out), (dk_ref, dk_out), (dv_ref, dv_out))
    copies = [pltpu.make_async_copy(src, dst, sems.at[i]) for i, (src, dst) in enumerate(pairs)]
    for copy in copies:
        copy.start()
    for copy in copies:
        copy.wait()


def solution(mesh):
    def local(queries, keys, values, attn_out, logsumexp, d_out, cu_seqlens):
        rows, heads, head = queries.shape
        qrows = rows * heads
        bf, f32 = jnp.bfloat16, jnp.float32
        dma = pltpu.SemaphoreType.DMA
        any_spec = pl.BlockSpec(memory_space=pl.ANY)
        vmem_spec = pl.BlockSpec(memory_space=pltpu.VMEM)
        shapes = ((qrows, head), (rows, head), (rows, head))
        results = pl.pallas_call(
            body,
            name="packed_backward",
            out_shape=tuple(pltpu.VMEM(shape, bf) for shape in shapes),
            in_specs=[any_spec] * 7,
            out_specs=(vmem_spec,) * 3,
            scratch_shapes=[
                pltpu.VMEM((qrows, head), bf), pltpu.VMEM((rows, head), bf), pltpu.VMEM((rows, head), bf),
                pltpu.VMEM((qrows, head), bf), pltpu.VMEM((heads, rows), f32), pltpu.VMEM((qrows, head), bf),
                pltpu.VMEM((2, qrows), f32), pltpu.VMEM((HOPS + 1, 1, qrows), jnp.int32),
                pltpu.VMEM((HOPS, rows, head), bf), pltpu.VMEM((HOPS, rows, head), bf),
                pltpu.VMEM((HOPS, qrows, head), bf), pltpu.VMEM((HOPS, qrows, head), bf), pltpu.VMEM((HOPS, 2, qrows), f32),
                pltpu.VMEM((head, qrows), f32), pltpu.VMEM((rows, head), f32), pltpu.VMEM((rows, head), f32),
                pltpu.SMEM(cu_seqlens.shape, jnp.int32), dma((7,)), pltpu.SemaphoreType.REGULAR,
                dma((HOPS, NK)), dma((HOPS, NK)), dma((HOPS, NQ)), dma((HOPS, NQ)), dma((HOPS,)),
                dma((2,)), dma((2,)), dma((2,)), dma((HOPS,)), dma((HOPS,)), dma((HOPS,)),
            ],
            compiler_params=pltpu.CompilerParams(collective_id=0, has_side_effects=True),
        )(cu_seqlens, queries.reshape(qrows, head), keys, values, attn_out.reshape(qrows, head), logsumexp.T, d_out.reshape(qrows, head))
        d_query, d_key, d_value = pl.pallas_call(
            store_body,
            name="store",
            out_shape=tuple(jax.ShapeDtypeStruct(shape, bf) for shape in shapes),
            in_specs=[vmem_spec] * 3,
            out_specs=(any_spec,) * 3,
            scratch_shapes=[dma((3,))],
        )(*[pltpu.with_memory_space_constraint(x, pltpu.VMEM) for x in results])
        return d_query.reshape(rows, heads, head), d_key, d_value

    seq_spec = P(("dp", "cpo", "cp"))
    return jax.shard_map(local, mesh=mesh, in_specs=(seq_spec,) * 6 + (P("dp"),), out_specs=(seq_spec,) * 3, check_vma=False)
```

```python
import functools
import math

import jax
import jax.numpy as jnp
from jax import lax
from jax.experimental import pallas as pl
from jax.experimental.pallas import tpu as pltpu
from jax.sharding import PartitionSpec as P

MESH = pl.DeviceIdType.MESH
HOPS = 3
NK = 2
NQ = 4
NONE = 31
NOBODY = 63
SEND = 18

KV_OWN = {0: [(1, 1), (2, 2)], 1: [(3, 2), (4, 3)], 2: [(3, 1), (5, 3)], 3: [(6, 3)], 4: [(5, 1), (6, 2)], 5: [(7, 2)], 6: [(7, 1)], 7: []}
QD_OWN = {0: [], 1: [(0, 1)], 2: [(0, 2)], 3: [(2, 1), (1, 2)], 4: [(1, 3)], 5: [(4, 1), (3, 2)], 6: [(4, 2), (3, 3)], 7: [(6, 1), (5, 2)]}
FIRST = {
    0: (0, 10, 1, 11),
    1: (0, 1, 100),
    2: (0, 1, 100),
    3: (100, 110),
    4: (0, 10, 1, 11, 100),
    5: (0, 100),
    6: (0, 1, 110, 100),
    7: (100, 110),
}
REST = {
    1: (101, 102, 103),
    2: (),
    3: (101, 111, 102, 112, 103),
    4: (101, 102, 103),
    5: (110, 101, 1, 111, 112, 113, 102, 103),
    6: (111, 112, 113, 101),
    7: (101, 111, 102, 112, 103),
}
AFTER = {
    1: (10, 11),
    2: (10, 101, 102, 103, 11),
    3: (0, 1),
}
LATER = {
    3: (113,),
    6: (102, 103),
    7: (113,),
}
TAIL = (2, 3, 0, 0, 2, 3, 0, 0)
LATE_KEYS = 4
GO = ((4, 1), (5, 2), (6, 3))
KV_REL = {(2, 2): (3, 3), (3, 2): (2, 1), (5, 3): (4, 2), (4, 1): (5, 2), (6, 3): (4, 1), (6, 2): (7, 3), (7, 2): (6, 1)}
QD_REL = {(0, 2): (1, 1), (1, 2): (0, 3), (1, 3): (3, 1), (3, 1): (2, 2), (3, 2): (2, 3), (4, 2): (5, 1), (5, 2): (4, 3)}
ORDER = ("ghijkoplmqnr", "aobkpqlrghminj", "ghijcadbkolpmqnr", "abcedfsgkhlimjnopqr", "gheijkfolpcabmnqrd", "abkglhecdminfj", "ghijceafsdb", "abcefds")


def step_codes(letters):
    return [ord(x) - ord("a") for x in letters]


def targets_of(table, pick):
    pairs = [table.get(pick(d), NOBODY) for d in range(8)]
    return [p if p == NOBODY else p[0] * 4 + p[1] for p in pairs]


def nth(table, n):
    return [NOBODY if len(table[d]) <= n else table[d][n][0] * 4 + table[d][n][1] for d in range(8)]


def partners():
    near = {d: set() for d in range(8)}
    pairs = [(d, target) for table in (KV_OWN, QD_OWN) for d in table for target, _ in table[d]]
    pairs += [(d, target) for table in (KV_REL, QD_REL) for (d, _), (target, _) in table.items()]
    for a, b in pairs:
        for here, there in ((a, b), (b, a)):
            if here >= 4 or there < 4:
                near[here].add(there)
    return near


def body(
    cu_hbm, q_hbm, k_hbm, v_hbm, o_hbm, lse_hbm, do_hbm,
    dq_out, dk_out, dv_out,
    q_loc, k_loc, v_loc, o_loc, lse_loc, do_loc, stat_loc, starts,
    k_buf, v_buf, q_buf, do_buf, stat_buf,
    dqt, dk_acc, dv_acc, cu_ref, in_sem, go_sem,
    k_recv, v_recv, q_recv, do_recv, stat_recv,
    kv_own, qd_own, stat_own, kv_rel, qd_rel, stat_rel,
):
    rows = k_loc.shape[0]
    qrows = q_loc.shape[0]
    head = k_loc.shape[1]
    kc_rows = rows // NK
    qc_rows = qrows // NQ
    scale = head ** -0.5
    factor = scale * math.log2(math.e)
    me = lax.axis_index("cpo") * 4 + lax.axis_index("cp")

    def lut(values):
        out = jnp.int32(values[0])
        for d in range(1, len(values)):
            out = jnp.where(me == d, jnp.int32(values[d]), out)
        return out

    def place(target):
        return {"cpo": target // 4, "cp": target % 4}

    barrier = pltpu.get_barrier_semaphore()
    near = partners()
    for d in range(8):
        @pl.when(me == d)
        def _(d=d):
            for other in [x for x in range(8) if d in near[x]]:
                pl.semaphore_signal(barrier, inc=1, device_id=place(other), device_id_type=MESH)
    loads = [
        pltpu.make_async_copy(src, dst, in_sem.at[i])
        for i, (src, dst) in enumerate(
            [(k_hbm, k_loc), (v_hbm, v_loc), (q_hbm, q_loc), (do_hbm, do_loc), (o_hbm, o_loc), (lse_hbm, lse_loc), (cu_hbm, cu_ref)]
        )
    ]
    for load in loads:
        load.start()
    for d in range(8):
        @pl.when(me == d)
        def _(d=d):
            pl.semaphore_wait(barrier, len(near[d]))
            for teller, told in GO:
                if teller == d:
                    pl.semaphore_signal(go_sem, inc=1, device_id=place(told), device_id_type=MESH)

    def kv_copies(src_k, src_v, sem, code, chunk):
        target, there = code // 4, code % 4 - 1
        part = pl.ds(chunk * kc_rows, kc_rows)
        return [
            pltpu.make_async_remote_copy(
                src_ref=src.at[part], dst_ref=buf.at[there, part], send_sem=sem, recv_sem=recv.at[there, chunk],
                device_id=place(target), device_id_type=MESH)
            for src, buf, recv in ((src_k, k_buf, k_recv), (src_v, v_buf, v_recv))
        ]

    def qd_copies(src_q, src_do, sem, code, chunk):
        target, there = code // 4, code % 4 - 1
        part = pl.ds(chunk * qc_rows, qc_rows)
        return [
            pltpu.make_async_remote_copy(
                src_ref=src.at[part], dst_ref=buf.at[there, part], send_sem=sem, recv_sem=recv.at[there, chunk],
                device_id=place(target), device_id_type=MESH)
            for src, buf, recv in ((src_q, q_buf, q_recv), (src_do, do_buf, do_recv))
        ]

    def stat_copy(src, sem, code):
        target, there = code // 4, code % 4 - 1
        return pltpu.make_async_remote_copy(
            src_ref=src, dst_ref=stat_buf.at[there], send_sem=sem, recv_sem=stat_recv.at[there],
            device_id=place(target), device_id_type=MESH)

    kv_to = [lut(nth(KV_OWN, n)) for n in range(2)]
    qd_to = [lut(nth(QD_OWN, n)) for n in range(2)]

    def send(d, item):
        kind, n, chunk = item // 100, item // 10 % 10, item % 10
        target, there = (KV_OWN, QD_OWN)[kind][d][n]
        code = target * 4 + there
        if kind == 0:
            copies = kv_copies(k_loc, v_loc, kv_own.at[n], code, chunk)
        else:
            copies = qd_copies(q_loc, do_loc, qd_own.at[n], code, chunk)
        for copy in copies:
            copy.start()

    def send_stat(d, n):
        target, there = QD_OWN[d][n]
        stat_copy(stat_loc, stat_own.at[n], target * 4 + there).start()

    loads[0].wait()
    loads[1].wait()
    for d in range(8):
        @pl.when(me == d)
        def _(d=d):
            for item in FIRST[d]:
                if item < 100:
                    send(d, item)
    loads[2].wait()
    loads[3].wait()
    for d in range(8):
        @pl.when(me == d)
        def _(d=d):
            for item in FIRST[d]:
                if item >= 100:
                    send(d, item)
    loads[4].wait()
    loads[5].wait()

    wide = lax.broadcasted_iota(jnp.int32, (2, 128), 1)
    for j in range(qrows // 128):
        src = lse_loc[:, 128 * (j // 2):128 * (j // 2 + 1)]
        both = jnp.take_along_axis(src, 64 * (j % 2) + wide // 2, axis=1, mode="promise_in_bounds")
        row = jnp.where(wide[0:1] % 2 == 0, both[0:1], both[1:2])
        stat_loc[0:1, 128 * j:128 * (j + 1)] = row * math.log2(math.e)
    ones = jnp.ones((8, head), jnp.bfloat16)
    for j in range(qrows // 256):
        part = pl.ds(256 * j, 256)
        prod = do_loc[part].astype(jnp.float32) * o_loc[part].astype(jnp.float32)
        hi = prod.astype(jnp.bfloat16)
        lo = (prod - hi.astype(jnp.float32)).astype(jnp.bfloat16)
        dims = (((1,), (1,)), ((), ()))
        total = lax.dot_general(ones, hi, dims, preferred_element_type=jnp.float32)
        total = total + lax.dot_general(ones, lo, dims, preferred_element_type=jnp.float32)
        stat_loc[1:2, 256 * j:256 * (j + 1)] = total[0:1]
    for d in range(8):
        @pl.when(me == d)
        def _(d=d):
            for n in range(len(QD_OWN[d])):
                send_stat(d, n)
            for item in REST.get(d, ()):
                send(d, item)

    loads[6].wait()
    lane = lax.broadcasted_iota(jnp.int32, (1, qrows), 1) // 2
    for h in range(HOPS + 1):
        pos = lane + (me + h) * rows
        start = jnp.zeros_like(pos)
        for j in range(cu_ref.shape[0]):
            start = jnp.maximum(start, jnp.where(pos >= cu_ref[j], cu_ref[j], 0))
        starts[h] = start

    def send_later():
        for d in LATER:
            @pl.when(me == d)
            def _(d=d):
                for item in LATER[d]:
                    send(d, item)

    def block(k_blk, v_blk, q_blk, do_blk, lse_row, d_row, keep):
        dims = (((1,), (1,)), ((), ()))
        scores = lax.dot_general(k_blk, q_blk, dims, preferred_element_type=jnp.float32)
        p_mat = jnp.where(keep, jnp.exp2(scores * factor - lse_row), 0.0)
        dp_mat = lax.dot_general(v_blk, do_blk, dims, preferred_element_type=jnp.float32)
        ds_mat = (p_mat * (dp_mat - d_row)).astype(jnp.bfloat16)
        return p_mat.astype(jnp.bfloat16), ds_mat

    def dq_term(k_blk, ds_mat):
        return lax.dot_general(k_blk, ds_mat, (((0,), (0,)), ((), ())), preferred_element_type=jnp.float32)

    def key_iota(keys, width):
        return lax.broadcasted_iota(jnp.int32, (keys, width), 0)

    half = qrows // 2

    def own_half(first, keys):
        cols = pl.ds(first, half)
        q_blk, do_blk, k_blk = q_loc[cols], do_loc[cols], k_loc[0:keys]
        key_pos = key_iota(keys, half)
        tok = lax.broadcasted_iota(jnp.int32, (keys, half), 1) // 2 + first // 2
        keep = (key_pos >= starts[0, :, cols] - me * rows) & (key_pos <= tok)
        p_low, ds_mat = block(k_blk, v_loc[0:keys], q_blk, do_blk, stat_loc[0:1, cols], stat_loc[1:2, cols], keep)
        dqt[:, cols] = dq_term(k_blk, ds_mat)
        dv_new = jnp.dot(p_low, do_blk, preferred_element_type=jnp.float32)
        dk_new = jnp.dot(ds_mat, q_blk, preferred_element_type=jnp.float32)
        if keys == rows:
            dv_acc[...] = dv_new
            dk_acc[...] = dk_new
        else:
            dv_acc[0:keys] = dv_acc[0:keys] + dv_new
            dk_acc[0:keys] = dk_acc[0:keys] + dk_new

    own_half(half, rows)
    for d in AFTER:
        @pl.when(me == d)
        def _(d=d):
            pl.semaphore_wait(go_sem, 1)
            for item in AFTER[d]:
                send(d, item)
    own_half(0, rows // 2)

    def finish_dq():
        dq_out[...] = (jnp.transpose(dqt[...]) * scale).astype(jnp.bfloat16)

    def kv_block(slot, count, first_key, width):
        cols = pl.ds(0, count)
        keys = pl.ds(first_key, width)
        base = (me - 1 - slot) * rows + first_key
        keep = key_iota(width, count) >= starts[0, :, cols] - base
        k_blk = k_buf[slot, keys]
        _, ds_mat = block(k_blk, v_buf[slot, keys], q_loc[cols], do_loc[cols], stat_loc[0:1, cols], stat_loc[1:2, cols], keep)
        dqt[:, cols] = dqt[:, cols] + dq_term(k_blk, ds_mat)

    def kv_unit(slot, chunk):
        far = slot == HOPS - 1
        late = (slot == 1) & (me == LATE_KEYS)

        @pl.when(far & (chunk == 0))
        def _():
            kv_block(slot, half, 0, kc_rows)

        @pl.when(late & (chunk == 0))
        def _():
            kv_block(slot, qrows, 0, kc_rows)

        @pl.when((far | late) & (chunk == 1))
        def _():
            kv_block(slot, qrows, kc_rows, kc_rows)

        @pl.when(jnp.logical_not(far | late) & (chunk == 1))
        def _():
            kv_block(slot, qrows, 0, rows)

    def qd_block(slot, first_row, count, first_key):
        cols = pl.ds(pl.multiple_of(first_row, 128), count)
        keys = pl.ds(first_key, rows - first_key)
        q_blk = q_buf[slot, cols]
        do_blk = do_buf[slot, cols]
        keep = key_iota(rows - first_key, count) >= starts[slot + 1, :, cols] - (me * rows + first_key)
        p_low, ds_mat = block(k_loc[keys], v_loc[keys], q_blk, do_blk, stat_buf[slot, 0:1, cols], stat_buf[slot, 1:2, cols], keep)
        dv_acc[keys] = dv_acc[keys] + jnp.dot(p_low, do_blk, preferred_element_type=jnp.float32)
        dk_acc[keys] = dk_acc[keys] + jnp.dot(ds_mat, q_blk, preferred_element_type=jnp.float32)

    def qd_unit(slot, chunk):
        quarters = (pick(tail, slot) == 1) & (chunk >= 2)
        short = (slot == HOPS - 1) & (chunk == 3)

        @pl.when(quarters)
        def _():
            qd_block(slot, chunk * qc_rows, qc_rows, 0)

        @pl.when((chunk % 2 == 1) & jnp.logical_not(quarters) & jnp.logical_not(short))
        def _():
            qd_block(slot, (chunk - 1) * qc_rows, half, 0)

        @pl.when(short & jnp.logical_not(quarters))
        def _():
            qd_block(slot, half, half, rows // 2)

    tail = [lut([(t >> h) % 2 for t in TAIL]) for h in range(HOPS)]
    last_kv = lut([max([-1] + [i for i, c in enumerate(step_codes(ORDER[d])) if c < 3 * NK and d > c // NK]) for d in range(8)])

    @pl.when(me == 0)
    def _():
        finish_dq()

    kv_on = [lut(targets_of(KV_REL, lambda d, h=h: (d, h + 1))) for h in range(HOPS)]
    qd_on = [lut(targets_of(QD_REL, lambda d, h=h: (d, h + 1))) for h in range(HOPS)]

    def pick(values, slot):
        return jnp.where(slot == 0, values[0], jnp.where(slot == 1, values[1], values[2]))

    per_word = 6
    codes = {d: step_codes(ORDER[d]) for d in range(8)}
    steps = max(len(c) for c in codes.values())
    words = -(-steps // per_word)
    packed = []
    for w in range(words):
        values = []
        for d in range(8):
            part = (codes[d] + [NONE] * (words * per_word))[w * per_word:(w + 1) * per_word]
            values.append(sum(c * 32 ** i for i, c in enumerate(part)))
        packed.append(lut(values))

    def step(i, carry):
        code = carry[0] % 32

        @pl.when(code < 3 * NK)
        def _():
            slot, chunk = code // NK, code % NK
            to = pick(kv_on, slot)
            for copy in kv_copies(k_buf.at[slot], v_buf.at[slot], kv_rel.at[slot], me * 4 + slot + 1, chunk):
                copy.wait_recv()

            @pl.when(to != NOBODY)
            def _():
                for copy in kv_copies(k_buf.at[slot], v_buf.at[slot], kv_rel.at[slot], to, chunk):
                    copy.start()

            @pl.when(me > slot)
            def _():
                kv_unit(slot, chunk)

            @pl.when(i == last_kv)
            def _():
                finish_dq()

        @pl.when((code >= 3 * NK) & (code < SEND))
        def _():
            slot, chunk = (code - 3 * NK) // NQ, (code - 3 * NK) % NQ
            to = pick(qd_on, slot)
            for copy in qd_copies(q_buf.at[slot], do_buf.at[slot], qd_rel.at[slot], me * 4 + slot + 1, chunk):
                copy.wait_recv()

            @pl.when(to != NOBODY)
            def _():
                for copy in qd_copies(q_buf.at[slot], do_buf.at[slot], qd_rel.at[slot], to, chunk):
                    copy.start()

            @pl.when(chunk == 0)
            def _():
                stat_copy(stat_buf.at[slot], stat_rel.at[slot], me * 4 + slot + 1).wait_recv()

                @pl.when(to != NOBODY)
                def _():
                    stat_copy(stat_buf.at[slot], stat_rel.at[slot], to).start()

            @pl.when(me + slot < 7)
            def _():
                qd_unit(slot, chunk)

        @pl.when(code == SEND)
        def _():
            send_later()

        last = (i % per_word) == per_word - 1
        rest = [jnp.where(last, (carry + (jnp.int32(0),))[w + 1], carry[w] // 32 if w == 0 else carry[w]) for w in range(words)]
        return tuple(rest)

    lax.fori_loop(0, steps, step, tuple(packed))

    dk_out[...] = (dk_acc[...] * scale).astype(jnp.bfloat16)
    dv_out[...] = dv_acc[...].astype(jnp.bfloat16)

    def sent(ref, sem):
        pltpu.make_async_remote_copy(src_ref=ref, dst_ref=ref, send_sem=sem, recv_sem=sem, device_id=place(me), device_id_type=MESH).wait_send()

    for targets, kv_sem in ((kv_to, kv_own), (kv_on, kv_rel)):
        for n, target in enumerate(targets):
            @pl.when(target != NOBODY)
            def _(n=n, kv_sem=kv_sem):
                sent(q_buf.at[0], kv_sem.at[n])
    for targets, qd_sem, stat_sem in ((qd_to, qd_own, stat_own), (qd_on, qd_rel, stat_rel)):
        for n, target in enumerate(targets):
            @pl.when(target != NOBODY)
            def _(n=n, qd_sem=qd_sem, stat_sem=stat_sem):
                sent(q_buf.at[0:2], qd_sem.at[n])
                sent(stat_loc, stat_sem.at[n])


def store_body(dq_ref, dk_ref, dv_ref, dq_out, dk_out, dv_out, sems):
    pairs = ((dq_ref, dq_out), (dk_ref, dk_out), (dv_ref, dv_out))
    copies = [pltpu.make_async_copy(src, dst, sems.at[i]) for i, (src, dst) in enumerate(pairs)]
    for copy in copies:
        copy.start()
    for copy in copies:
        copy.wait()


def solution(mesh):
    def local(queries, keys, values, attn_out, logsumexp, d_out, cu_seqlens):
        rows, heads, head = queries.shape
        qrows = rows * heads
        bf, f32 = jnp.bfloat16, jnp.float32
        dma = pltpu.SemaphoreType.DMA
        any_spec = pl.BlockSpec(memory_space=pl.ANY)
        vmem_spec = pl.BlockSpec(memory_space=pltpu.VMEM)
        shapes = ((qrows, head), (rows, head), (rows, head))
        results = pl.pallas_call(
            body,
            name="packed_backward",
            out_shape=tuple(pltpu.VMEM(shape, bf) for shape in shapes),
            in_specs=[any_spec] * 7,
            out_specs=(vmem_spec,) * 3,
            scratch_shapes=[
                pltpu.VMEM((qrows, head), bf), pltpu.VMEM((rows, head), bf), pltpu.VMEM((rows, head), bf),
                pltpu.VMEM((qrows, head), bf), pltpu.VMEM((heads, rows), f32), pltpu.VMEM((qrows, head), bf),
                pltpu.VMEM((2, qrows), f32), pltpu.VMEM((HOPS + 1, 1, qrows), jnp.int32),
                pltpu.VMEM((HOPS, rows, head), bf), pltpu.VMEM((HOPS, rows, head), bf),
                pltpu.VMEM((HOPS, qrows, head), bf), pltpu.VMEM((HOPS, qrows, head), bf), pltpu.VMEM((HOPS, 2, qrows), f32),
                pltpu.VMEM((head, qrows), f32), pltpu.VMEM((rows, head), f32), pltpu.VMEM((rows, head), f32),
                pltpu.SMEM(cu_seqlens.shape, jnp.int32), dma((7,)), pltpu.SemaphoreType.REGULAR,
                dma((HOPS, NK)), dma((HOPS, NK)), dma((HOPS, NQ)), dma((HOPS, NQ)), dma((HOPS,)),
                dma((2,)), dma((2,)), dma((2,)), dma((HOPS,)), dma((HOPS,)), dma((HOPS,)),
            ],
            compiler_params=pltpu.CompilerParams(collective_id=0, has_side_effects=True),
        )(cu_seqlens, queries.reshape(qrows, head), keys, values, attn_out.reshape(qrows, head), logsumexp.T, d_out.reshape(qrows, head))
        d_query, d_key, d_value = pl.pallas_call(
            store_body,
            name="store",
            out_shape=tuple(jax.ShapeDtypeStruct(shape, bf) for shape in shapes),
            in_specs=[vmem_spec] * 3,
            out_specs=(any_spec,) * 3,
            scratch_shapes=[dma((3,))],
        )(*[pltpu.with_memory_space_constraint(x, pltpu.VMEM) for x in results])
        return d_query.reshape(rows, heads, head), d_key, d_value

    seq_spec = P(("dp", "cpo", "cp"))
    return jax.shard_map(local, mesh=mesh, in_specs=(seq_spec,) * 6 + (P("dp"),), out_specs=(seq_spec,) * 3, check_vma=False)
```

```python
import functools
import math

import jax
import jax.numpy as jnp
from jax import lax
from jax.experimental import pallas as pl
from jax.experimental.pallas import tpu as pltpu
from jax.sharding import PartitionSpec as P

MESH = pl.DeviceIdType.MESH
HOPS = 3
NK = 2
NQ = 4
NONE = 31
NOBODY = 63
SEND = 18

KV_OWN = {0: [(1, 1), (2, 2)], 1: [(3, 2), (4, 3)], 2: [(3, 1), (5, 3)], 3: [(6, 3)], 4: [(5, 1), (6, 2)], 5: [(7, 2)], 6: [(7, 1)], 7: []}
QD_OWN = {0: [], 1: [(0, 1)], 2: [(0, 2)], 3: [(2, 1), (1, 2)], 4: [(1, 3)], 5: [(4, 1), (3, 2)], 6: [(5, 1), (3, 3)], 7: [(6, 1), (5, 2)]}
FIRST = {
    0: (0, 10, 1, 11),
    1: (0, 1, 100),
    2: (0, 1, 100),
    3: (100, 110),
    4: (0, 10, 1, 11, 100),
    5: (0, 100),
    6: (0, 1, 110, 100),
    7: (100, 110),
}
REST = {
    1: (101, 102, 103),
    2: (),
    3: (101, 111, 102, 112, 103),
    4: (101, 102, 103),
    5: (110, 101, 1, 111, 112, 113, 102, 103),
    6: (111, 112, 113, 101),
    7: (101, 111, 102, 112, 103),
}
AFTER = {
    1: (10, 11),
    2: (10, 101, 102, 103, 11),
    3: (0, 1),
}
LATER = {
    3: (113,),
    6: (102, 103),
    7: (113,),
}
TAIL = (2, 3, 0, 0, 2, 3, 0, 0)
LATE_KEYS = 4
GO = ((4, 1), (5, 2), (6, 3))
KV_REL = {(2, 2): (3, 3), (3, 2): (2, 1), (5, 3): (4, 2), (4, 1): (5, 2), (6, 3): (4, 1), (6, 2): (7, 3), (7, 2): (6, 1)}
QD_REL = {(0, 2): (1, 1), (1, 2): (0, 3), (1, 3): (3, 1), (3, 1): (2, 2), (3, 2): (2, 3), (5, 1): (4, 2), (5, 2): (4, 3)}
ORDER = ("ghijkoplmqnr", "aobkpqlrghminj", "ghijcadbkolpmqnr", "abcedfsgkhlimjnopqr", "gheijkfolpcabmqnrd", "abkglhecdminfj", "ghijceafsdb", "abcefds")


def step_codes(letters):
    return [ord(x) - ord("a") for x in letters]


def targets_of(table, pick):
    pairs = [table.get(pick(d), NOBODY) for d in range(8)]
    return [p if p == NOBODY else p[0] * 4 + p[1] for p in pairs]


def nth(table, n):
    return [NOBODY if len(table[d]) <= n else table[d][n][0] * 4 + table[d][n][1] for d in range(8)]


def partners():
    near = {d: set() for d in range(8)}
    pairs = [(d, target) for table in (KV_OWN, QD_OWN) for d in table for target, _ in table[d]]
    pairs += [(d, target) for table in (KV_REL, QD_REL) for (d, _), (target, _) in table.items()]
    for a, b in pairs:
        for here, there in ((a, b), (b, a)):
            if here >= 4 or there < 4:
                near[here].add(there)
    return near


def body(
    cu_hbm, q_hbm, k_hbm, v_hbm, o_hbm, lse_hbm, do_hbm,
    dq_out, dk_out, dv_out,
    q_loc, k_loc, v_loc, o_loc, lse_loc, do_loc, stat_loc, starts,
    k_buf, v_buf, q_buf, do_buf, stat_buf,
    dqt, dk_acc, dv_acc, cu_ref, in_sem, go_sem,
    k_recv, v_recv, q_recv, do_recv, stat_recv,
    kv_own, qd_own, stat_own, kv_rel, qd_rel, stat_rel,
):
    rows = k_loc.shape[0]
    qrows = q_loc.shape[0]
    head = k_loc.shape[1]
    kc_rows = rows // NK
    qc_rows = qrows // NQ
    scale = head ** -0.5
    factor = scale * math.log2(math.e)
    me = lax.axis_index("cpo") * 4 + lax.axis_index("cp")

    def lut(values):
        out = jnp.int32(values[0])
        for d in range(1, len(values)):
            out = jnp.where(me == d, jnp.int32(values[d]), out)
        return out

    def place(target):
        return {"cpo": target // 4, "cp": target % 4}

    barrier = pltpu.get_barrier_semaphore()
    near = partners()
    for d in range(8):
        @pl.when(me == d)
        def _(d=d):
            for other in [x for x in range(8) if d in near[x]]:
                pl.semaphore_signal(barrier, inc=1, device_id=place(other), device_id_type=MESH)
    loads = [
        pltpu.make_async_copy(src, dst, in_sem.at[i])
        for i, (src, dst) in enumerate(
            [(k_hbm, k_loc), (v_hbm, v_loc), (q_hbm, q_loc), (do_hbm, do_loc), (o_hbm, o_loc), (lse_hbm, lse_loc), (cu_hbm, cu_ref)]
        )
    ]
    for load in loads:
        load.start()
    for d in range(8):
        @pl.when(me == d)
        def _(d=d):
            pl.semaphore_wait(barrier, len(near[d]))
            for teller, told in GO:
                if teller == d:
                    pl.semaphore_signal(go_sem, inc=1, device_id=place(told), device_id_type=MESH)

    def kv_copies(src_k, src_v, sem, code, chunk):
        target, there = code // 4, code % 4 - 1
        part = pl.ds(chunk * kc_rows, kc_rows)
        return [
            pltpu.make_async_remote_copy(
                src_ref=src.at[part], dst_ref=buf.at[there, part], send_sem=sem, recv_sem=recv.at[there, chunk],
                device_id=place(target), device_id_type=MESH)
            for src, buf, recv in ((src_k, k_buf, k_recv), (src_v, v_buf, v_recv))
        ]

    def qd_copies(src_q, src_do, sem, code, chunk):
        target, there = code // 4, code % 4 - 1
        part = pl.ds(chunk * qc_rows, qc_rows)
        return [
            pltpu.make_async_remote_copy(
                src_ref=src.at[part], dst_ref=buf.at[there, part], send_sem=sem, recv_sem=recv.at[there, chunk],
                device_id=place(target), device_id_type=MESH)
            for src, buf, recv in ((src_q, q_buf, q_recv), (src_do, do_buf, do_recv))
        ]

    def stat_copy(src, sem, code):
        target, there = code // 4, code % 4 - 1
        return pltpu.make_async_remote_copy(
            src_ref=src, dst_ref=stat_buf.at[there], send_sem=sem, recv_sem=stat_recv.at[there],
            device_id=place(target), device_id_type=MESH)

    kv_to = [lut(nth(KV_OWN, n)) for n in range(2)]
    qd_to = [lut(nth(QD_OWN, n)) for n in range(2)]

    def send(d, item):
        kind, n, chunk = item // 100, item // 10 % 10, item % 10
        target, there = (KV_OWN, QD_OWN)[kind][d][n]
        code = target * 4 + there
        if kind == 0:
            copies = kv_copies(k_loc, v_loc, kv_own.at[n], code, chunk)
        else:
            copies = qd_copies(q_loc, do_loc, qd_own.at[n], code, chunk)
        for copy in copies:
            copy.start()

    def send_stat(d, n):
        target, there = QD_OWN[d][n]
        stat_copy(stat_loc, stat_own.at[n], target * 4 + there).start()

    loads[0].wait()
    loads[1].wait()
    for d in range(8):
        @pl.when(me == d)
        def _(d=d):
            for item in FIRST[d]:
                if item < 100:
                    send(d, item)
    loads[2].wait()
    loads[3].wait()
    for d in range(8):
        @pl.when(me == d)
        def _(d=d):
            for item in FIRST[d]:
                if item >= 100:
                    send(d, item)
    loads[4].wait()
    loads[5].wait()

    wide = lax.broadcasted_iota(jnp.int32, (2, 128), 1)
    for j in range(qrows // 128):
        src = lse_loc[:, 128 * (j // 2):128 * (j // 2 + 1)]
        both = jnp.take_along_axis(src, 64 * (j % 2) + wide // 2, axis=1, mode="promise_in_bounds")
        row = jnp.where(wide[0:1] % 2 == 0, both[0:1], both[1:2])
        stat_loc[0:1, 128 * j:128 * (j + 1)] = row * math.log2(math.e)
    ones = jnp.ones((8, head), jnp.bfloat16)
    for j in range(qrows // 256):
        part = pl.ds(256 * j, 256)
        prod = do_loc[part].astype(jnp.float32) * o_loc[part].astype(jnp.float32)
        hi = prod.astype(jnp.bfloat16)
        lo = (prod - hi.astype(jnp.float32)).astype(jnp.bfloat16)
        dims = (((1,), (1,)), ((), ()))
        total = lax.dot_general(ones, hi, dims, preferred_element_type=jnp.float32)
        total = total + lax.dot_general(ones, lo, dims, preferred_element_type=jnp.float32)
        stat_loc[1:2, 256 * j:256 * (j + 1)] = total[0:1]
    for d in range(8):
        @pl.when(me == d)
        def _(d=d):
            for n in range(len(QD_OWN[d])):
                send_stat(d, n)
            for item in REST.get(d, ()):
                send(d, item)

    loads[6].wait()
    lane = lax.broadcasted_iota(jnp.int32, (1, qrows), 1) // 2
    for h in range(HOPS + 1):
        pos = lane + (me + h) * rows
        start = jnp.zeros_like(pos)
        for j in range(cu_ref.shape[0]):
            start = jnp.maximum(start, jnp.where(pos >= cu_ref[j], cu_ref[j], 0))
        starts[h] = start

    def send_later():
        for d in LATER:
            @pl.when(me == d)
            def _(d=d):
                for item in LATER[d]:
                    send(d, item)

    def block(k_blk, v_blk, q_blk, do_blk, lse_row, d_row, keep):
        dims = (((1,), (1,)), ((), ()))
        scores = lax.dot_general(k_blk, q_blk, dims, preferred_element_type=jnp.float32)
        p_mat = jnp.where(keep, jnp.exp2(scores * factor - lse_row), 0.0)
        dp_mat = lax.dot_general(v_blk, do_blk, dims, preferred_element_type=jnp.float32)
        ds_mat = (p_mat * (dp_mat - d_row)).astype(jnp.bfloat16)
        return p_mat.astype(jnp.bfloat16), ds_mat

    def dq_term(k_blk, ds_mat):
        return lax.dot_general(k_blk, ds_mat, (((0,), (0,)), ((), ())), preferred_element_type=jnp.float32)

    def key_iota(keys, width):
        return lax.broadcasted_iota(jnp.int32, (keys, width), 0)

    half = qrows // 2

    def own_half(first, keys):
        cols = pl.ds(first, half)
        q_blk, do_blk, k_blk = q_loc[cols], do_loc[cols], k_loc[0:keys]
        key_pos = key_iota(keys, half)
        tok = lax.broadcasted_iota(jnp.int32, (keys, half), 1) // 2 + first // 2
        keep = (key_pos >= starts[0, :, cols] - me * rows) & (key_pos <= tok)
        p_low, ds_mat = block(k_blk, v_loc[0:keys], q_blk, do_blk, stat_loc[0:1, cols], stat_loc[1:2, cols], keep)
        dqt[:, cols] = dq_term(k_blk, ds_mat)
        dv_new = jnp.dot(p_low, do_blk, preferred_element_type=jnp.float32)
        dk_new = jnp.dot(ds_mat, q_blk, preferred_element_type=jnp.float32)
        if keys == rows:
            dv_acc[...] = dv_new
            dk_acc[...] = dk_new
        else:
            dv_acc[0:keys] = dv_acc[0:keys] + dv_new
            dk_acc[0:keys] = dk_acc[0:keys] + dk_new

    own_half(half, rows)
    for d in AFTER:
        @pl.when(me == d)
        def _(d=d):
            pl.semaphore_wait(go_sem, 1)
            for item in AFTER[d]:
                send(d, item)
    own_half(0, rows // 2)

    def finish_dq():
        dq_out[...] = (jnp.transpose(dqt[...]) * scale).astype(jnp.bfloat16)

    def kv_block(slot, count, first_key, width):
        cols = pl.ds(0, count)
        keys = pl.ds(first_key, width)
        base = (me - 1 - slot) * rows + first_key
        keep = key_iota(width, count) >= starts[0, :, cols] - base
        k_blk = k_buf[slot, keys]
        _, ds_mat = block(k_blk, v_buf[slot, keys], q_loc[cols], do_loc[cols], stat_loc[0:1, cols], stat_loc[1:2, cols], keep)
        dqt[:, cols] = dqt[:, cols] + dq_term(k_blk, ds_mat)

    def kv_unit(slot, chunk):
        far = slot == HOPS - 1
        late = (slot == 1) & (me == LATE_KEYS)

        @pl.when(far & (chunk == 0))
        def _():
            kv_block(slot, half, 0, kc_rows)

        @pl.when(late & (chunk == 0))
        def _():
            kv_block(slot, qrows, 0, kc_rows)

        @pl.when((far | late) & (chunk == 1))
        def _():
            kv_block(slot, qrows, kc_rows, kc_rows)

        @pl.when(jnp.logical_not(far | late) & (chunk == 1))
        def _():
            kv_block(slot, qrows, 0, rows)

    def qd_block(slot, first_row, count, first_key):
        cols = pl.ds(pl.multiple_of(first_row, 128), count)
        keys = pl.ds(first_key, rows - first_key)
        q_blk = q_buf[slot, cols]
        do_blk = do_buf[slot, cols]
        keep = key_iota(rows - first_key, count) >= starts[slot + 1, :, cols] - (me * rows + first_key)
        p_low, ds_mat = block(k_loc[keys], v_loc[keys], q_blk, do_blk, stat_buf[slot, 0:1, cols], stat_buf[slot, 1:2, cols], keep)
        dv_acc[keys] = dv_acc[keys] + jnp.dot(p_low, do_blk, preferred_element_type=jnp.float32)
        dk_acc[keys] = dk_acc[keys] + jnp.dot(ds_mat, q_blk, preferred_element_type=jnp.float32)

    def qd_unit(slot, chunk):
        quarters = (pick(tail, slot) == 1) & (chunk >= 2)
        short = (slot == HOPS - 1) & (chunk == 3)

        @pl.when(quarters)
        def _():
            qd_block(slot, chunk * qc_rows, qc_rows, 0)

        @pl.when((chunk % 2 == 1) & jnp.logical_not(quarters) & jnp.logical_not(short))
        def _():
            qd_block(slot, (chunk - 1) * qc_rows, half, 0)

        @pl.when(short & jnp.logical_not(quarters))
        def _():
            qd_block(slot, half, half, rows // 2)

    tail = [lut([(t >> h) % 2 for t in TAIL]) for h in range(HOPS)]
    last_kv = lut([max([-1] + [i for i, c in enumerate(step_codes(ORDER[d])) if c < 3 * NK and d > c // NK]) for d in range(8)])

    @pl.when(me == 0)
    def _():
        finish_dq()

    kv_on = [lut(targets_of(KV_REL, lambda d, h=h: (d, h + 1))) for h in range(HOPS)]
    qd_on = [lut(targets_of(QD_REL, lambda d, h=h: (d, h + 1))) for h in range(HOPS)]

    def pick(values, slot):
        return jnp.where(slot == 0, values[0], jnp.where(slot == 1, values[1], values[2]))

    per_word = 6
    codes = {d: step_codes(ORDER[d]) for d in range(8)}
    steps = max(len(c) for c in codes.values())
    words = -(-steps // per_word)
    packed = []
    for w in range(words):
        values = []
        for d in range(8):
            part = (codes[d] + [NONE] * (words * per_word))[w * per_word:(w + 1) * per_word]
            values.append(sum(c * 32 ** i for i, c in enumerate(part)))
        packed.append(lut(values))

    def step(i, carry):
        code = carry[0] % 32

        @pl.when(code < 3 * NK)
        def _():
            slot, chunk = code // NK, code % NK
            to = pick(kv_on, slot)
            for copy in kv_copies(k_buf.at[slot], v_buf.at[slot], kv_rel.at[slot], me * 4 + slot + 1, chunk):
                copy.wait_recv()

            @pl.when(to != NOBODY)
            def _():
                for copy in kv_copies(k_buf.at[slot], v_buf.at[slot], kv_rel.at[slot], to, chunk):
                    copy.start()

            @pl.when(me > slot)
            def _():
                kv_unit(slot, chunk)

            @pl.when(i == last_kv)
            def _():
                finish_dq()

        @pl.when((code >= 3 * NK) & (code < SEND))
        def _():
            slot, chunk = (code - 3 * NK) // NQ, (code - 3 * NK) % NQ
            to = pick(qd_on, slot)
            for copy in qd_copies(q_buf.at[slot], do_buf.at[slot], qd_rel.at[slot], me * 4 + slot + 1, chunk):
                copy.wait_recv()

            @pl.when(to != NOBODY)
            def _():
                for copy in qd_copies(q_buf.at[slot], do_buf.at[slot], qd_rel.at[slot], to, chunk):
                    copy.start()

            @pl.when(chunk == 0)
            def _():
                stat_copy(stat_buf.at[slot], stat_rel.at[slot], me * 4 + slot + 1).wait_recv()

                @pl.when(to != NOBODY)
                def _():
                    stat_copy(stat_buf.at[slot], stat_rel.at[slot], to).start()

            @pl.when(me + slot < 7)
            def _():
                qd_unit(slot, chunk)

        @pl.when(code == SEND)
        def _():
            send_later()

        last = (i % per_word) == per_word - 1
        rest = [jnp.where(last, (carry + (jnp.int32(0),))[w + 1], carry[w] // 32 if w == 0 else carry[w]) for w in range(words)]
        return tuple(rest)

    lax.fori_loop(0, steps, step, tuple(packed))

    dk_out[...] = (dk_acc[...] * scale).astype(jnp.bfloat16)
    dv_out[...] = dv_acc[...].astype(jnp.bfloat16)

    def sent(ref, sem):
        pltpu.make_async_remote_copy(src_ref=ref, dst_ref=ref, send_sem=sem, recv_sem=sem, device_id=place(me), device_id_type=MESH).wait_send()

    for targets, kv_sem in ((kv_to, kv_own), (kv_on, kv_rel)):
        for n, target in enumerate(targets):
            @pl.when(target != NOBODY)
            def _(n=n, kv_sem=kv_sem):
                sent(q_buf.at[0], kv_sem.at[n])
    for targets, qd_sem, stat_sem in ((qd_to, qd_own, stat_own), (qd_on, qd_rel, stat_rel)):
        for n, target in enumerate(targets):
            @pl.when(target != NOBODY)
            def _(n=n, qd_sem=qd_sem, stat_sem=stat_sem):
                sent(q_buf.at[0:2], qd_sem.at[n])
                sent(stat_loc, stat_sem.at[n])


def store_body(dq_ref, dk_ref, dv_ref, dq_out, dk_out, dv_out, sems):
    pairs = ((dq_ref, dq_out), (dk_ref, dk_out), (dv_ref, dv_out))
    copies = [pltpu.make_async_copy(src, dst, sems.at[i]) for i, (src, dst) in enumerate(pairs)]
    for copy in copies:
        copy.start()
    for copy in copies:
        copy.wait()


def solution(mesh):
    def local(queries, keys, values, attn_out, logsumexp, d_out, cu_seqlens):
        rows, heads, head = queries.shape
        qrows = rows * heads
        bf, f32 = jnp.bfloat16, jnp.float32
        dma = pltpu.SemaphoreType.DMA
        any_spec = pl.BlockSpec(memory_space=pl.ANY)
        vmem_spec = pl.BlockSpec(memory_space=pltpu.VMEM)
        shapes = ((qrows, head), (rows, head), (rows, head))
        results = pl.pallas_call(
            body,
            name="packed_backward",
            out_shape=tuple(pltpu.VMEM(shape, bf) for shape in shapes),
            in_specs=[any_spec] * 7,
            out_specs=(vmem_spec,) * 3,
            scratch_shapes=[
                pltpu.VMEM((qrows, head), bf), pltpu.VMEM((rows, head), bf), pltpu.VMEM((rows, head), bf),
                pltpu.VMEM((qrows, head), bf), pltpu.VMEM((heads, rows), f32), pltpu.VMEM((qrows, head), bf),
                pltpu.VMEM((2, qrows), f32), pltpu.VMEM((HOPS + 1, 1, qrows), jnp.int32),
                pltpu.VMEM((HOPS, rows, head), bf), pltpu.VMEM((HOPS, rows, head), bf),
                pltpu.VMEM((HOPS, qrows, head), bf), pltpu.VMEM((HOPS, qrows, head), bf), pltpu.VMEM((HOPS, 2, qrows), f32),
                pltpu.VMEM((head, qrows), f32), pltpu.VMEM((rows, head), f32), pltpu.VMEM((rows, head), f32),
                pltpu.SMEM(cu_seqlens.shape, jnp.int32), dma((7,)), pltpu.SemaphoreType.REGULAR,
                dma((HOPS, NK)), dma((HOPS, NK)), dma((HOPS, NQ)), dma((HOPS, NQ)), dma((HOPS,)),
                dma((2,)), dma((2,)), dma((2,)), dma((HOPS,)), dma((HOPS,)), dma((HOPS,)),
            ],
            compiler_params=pltpu.CompilerParams(collective_id=0, has_side_effects=True),
        )(cu_seqlens, queries.reshape(qrows, head), keys, values, attn_out.reshape(qrows, head), logsumexp.T, d_out.reshape(qrows, head))
        d_query, d_key, d_value = pl.pallas_call(
            store_body,
            name="store",
            out_shape=tuple(jax.ShapeDtypeStruct(shape, bf) for shape in shapes),
            in_specs=[vmem_spec] * 3,
            out_specs=(any_spec,) * 3,
            scratch_shapes=[dma((3,))],
        )(*[pltpu.with_memory_space_constraint(x, pltpu.VMEM) for x in results])
        return d_query.reshape(rows, heads, head), d_key, d_value

    seq_spec = P(("dp", "cpo", "cp"))
    return jax.shard_map(local, mesh=mesh, in_specs=(seq_spec,) * 6 + (P("dp"),), out_specs=(seq_spec,) * 3, check_vma=False)
```

```python
import functools
import math

import jax
import jax.numpy as jnp
from jax import lax
from jax.experimental import pallas as pl
from jax.experimental.pallas import tpu as pltpu
from jax.sharding import PartitionSpec as P

MESH = pl.DeviceIdType.MESH
HOPS = 3
NK = 2
NQ = 4
NONE = 31
NOBODY = 63
SEND = 18

KV_OWN = {0: [(1, 1), (2, 2)], 1: [(3, 2), (4, 3)], 2: [(3, 1), (5, 3)], 3: [(6, 3)], 4: [(5, 1), (6, 2)], 5: [(7, 2)], 6: [(7, 1)], 7: []}
QD_OWN = {0: [], 1: [(0, 1)], 2: [(0, 2)], 3: [(2, 1), (1, 2)], 4: [(1, 3)], 5: [(4, 1), (3, 2)], 6: [(4, 2), (3, 3)], 7: [(6, 1), (5, 2)]}
FIRST = {
    0: (0, 10, 1, 11),
    1: (0, 1, 100),
    2: (0, 1, 100),
    3: (100, 110),
    4: (0, 10, 1, 11, 100),
    5: (0, 100),
    6: (0, 1, 110, 100),
    7: (100, 110),
}
REST = {
    1: (101, 102, 103),
    2: (),
    3: (101, 111, 102, 112, 103),
    4: (101, 102, 103),
    5: (110, 101, 1, 111, 112, 113, 102, 103),
    6: (111, 112, 113, 101),
    7: (101, 111, 102, 112, 103),
}
AFTER = {
    1: (10, 11),
    2: (10, 101, 102, 103, 11),
    3: (0, 1),
}
LATER = {
    3: (113,),
    6: (102, 103),
    7: (113,),
}
TAIL = (2, 3, 0, 0, 2, 3, 0, 0)
LATE_KEYS = 4
GO = ((4, 1), (5, 2), (6, 3))
KV_REL = {(2, 2): (3, 3), (3, 2): (2, 1), (5, 3): (4, 2), (4, 1): (5, 2), (6, 3): (4, 1), (6, 2): (7, 3), (7, 2): (6, 1)}
QD_REL = {(0, 2): (1, 1), (1, 2): (0, 3), (1, 3): (3, 1), (3, 1): (2, 2), (3, 2): (2, 3), (4, 2): (5, 1), (5, 2): (4, 3)}
ORDER = ("ghijkoplmqnr", "aobkpqlrghminj", "ghijcadbkolpmqnr", "abcedfsgkhlimjnopqr", "gheijkfolpcabmnqrd", "abkglhecdminfj", "ghijceafsdb", "abcefds")


def step_codes(letters):
    return [ord(x) - ord("a") for x in letters]


def targets_of(table, pick):
    pairs = [table.get(pick(d), NOBODY) for d in range(8)]
    return [p if p == NOBODY else p[0] * 4 + p[1] for p in pairs]


def nth(table, n):
    return [NOBODY if len(table[d]) <= n else table[d][n][0] * 4 + table[d][n][1] for d in range(8)]


def partners():
    near = {d: set() for d in range(8)}
    pairs = [(d, target) for table in (KV_OWN, QD_OWN) for d in table for target, _ in table[d]]
    pairs += [(d, target) for table in (KV_REL, QD_REL) for (d, _), (target, _) in table.items()]
    for a, b in pairs:
        for here, there in ((a, b), (b, a)):
            if here >= 4 or there < 4:
                near[here].add(there)
    return near


def body(
    cu_hbm, q_hbm, k_hbm, v_hbm, o_hbm, lse_hbm, do_hbm,
    dq_out, dk_out, dv_out,
    q_loc, k_loc, v_loc, o_loc, lse_loc, do_loc, stat_loc, starts,
    k_buf, v_buf, q_buf, do_buf, stat_buf,
    dqt, dk_acc, dv_acc, cu_ref, in_sem, go_sem,
    k_recv, v_recv, q_recv, do_recv, stat_recv,
    kv_own, qd_own, stat_own, kv_rel, qd_rel, stat_rel,
):
    rows = k_loc.shape[0]
    qrows = q_loc.shape[0]
    head = k_loc.shape[1]
    kc_rows = rows // NK
    qc_rows = qrows // NQ
    scale = head ** -0.5
    factor = scale * math.log2(math.e)
    me = lax.axis_index("cpo") * 4 + lax.axis_index("cp")

    def lut(values):
        out = jnp.int32(values[0])
        for d in range(1, len(values)):
            out = jnp.where(me == d, jnp.int32(values[d]), out)
        return out

    def place(target):
        return {"cpo": target // 4, "cp": target % 4}

    barrier = pltpu.get_barrier_semaphore()
    near = partners()
    for d in range(8):
        @pl.when(me == d)
        def _(d=d):
            for other in [x for x in range(8) if d in near[x]]:
                pl.semaphore_signal(barrier, inc=1, device_id=place(other), device_id_type=MESH)
    loads = [
        pltpu.make_async_copy(src, dst, in_sem.at[i])
        for i, (src, dst) in enumerate(
            [
                (q_hbm.at[0:qc_rows], q_loc.at[0:qc_rows]), (do_hbm.at[0:qc_rows], do_loc.at[0:qc_rows]), (k_hbm, k_loc), (v_hbm, v_loc),
                (q_hbm.at[qc_rows:], q_loc.at[qc_rows:]), (do_hbm.at[qc_rows:], do_loc.at[qc_rows:]), (o_hbm, o_loc), (lse_hbm, lse_loc),
                (cu_hbm, cu_ref),
            ]
        )
    ]
    for load in loads:
        load.start()
    for d in range(8):
        @pl.when(me == d)
        def _(d=d):
            pl.semaphore_wait(barrier, len(near[d]))
            for teller, told in GO:
                if teller == d:
                    pl.semaphore_signal(go_sem, inc=1, device_id=place(told), device_id_type=MESH)

    def kv_copies(src_k, src_v, sem, code, chunk):
        target, there = code // 4, code % 4 - 1
        part = pl.ds(chunk * kc_rows, kc_rows)
        return [
            pltpu.make_async_remote_copy(
                src_ref=src.at[part], dst_ref=buf.at[there, part], send_sem=sem, recv_sem=recv.at[there, chunk],
                device_id=place(target), device_id_type=MESH)
            for src, buf, recv in ((src_k, k_buf, k_recv), (src_v, v_buf, v_recv))
        ]

    def qd_copies(src_q, src_do, sem, code, chunk):
        target, there = code // 4, code % 4 - 1
        part = pl.ds(chunk * qc_rows, qc_rows)
        return [
            pltpu.make_async_remote_copy(
                src_ref=src.at[part], dst_ref=buf.at[there, part], send_sem=sem, recv_sem=recv.at[there, chunk],
                device_id=place(target), device_id_type=MESH)
            for src, buf, recv in ((src_q, q_buf, q_recv), (src_do, do_buf, do_recv))
        ]

    def stat_copy(src, sem, code):
        target, there = code // 4, code % 4 - 1
        return pltpu.make_async_remote_copy(
            src_ref=src, dst_ref=stat_buf.at[there], send_sem=sem, recv_sem=stat_recv.at[there],
            device_id=place(target), device_id_type=MESH)

    kv_to = [lut(nth(KV_OWN, n)) for n in range(2)]
    qd_to = [lut(nth(QD_OWN, n)) for n in range(2)]

    def send(d, item):
        kind, n, chunk = item // 100, item // 10 % 10, item % 10
        target, there = (KV_OWN, QD_OWN)[kind][d][n]
        code = target * 4 + there
        if kind == 0:
            copies = kv_copies(k_loc, v_loc, kv_own.at[n], code, chunk)
        else:
            copies = qd_copies(q_loc, do_loc, qd_own.at[n], code, chunk)
        for copy in copies:
            copy.start()

    def send_stat(d, n):
        target, there = QD_OWN[d][n]
        stat_copy(stat_loc, stat_own.at[n], target * 4 + there).start()

    loads[0].wait()
    loads[1].wait()
    for d in range(8):
        @pl.when(me == d)
        def _(d=d):
            for item in FIRST[d]:
                if item >= 100:
                    send(d, item)
    loads[2].wait()
    loads[3].wait()
    for d in range(8):
        @pl.when(me == d)
        def _(d=d):
            for item in FIRST[d]:
                if item < 100:
                    send(d, item)
    for load in loads[4:8]:
        load.wait()

    wide = lax.broadcasted_iota(jnp.int32, (2, 128), 1)
    for j in range(qrows // 128):
        src = lse_loc[:, 128 * (j // 2):128 * (j // 2 + 1)]
        both = jnp.take_along_axis(src, 64 * (j % 2) + wide // 2, axis=1, mode="promise_in_bounds")
        row = jnp.where(wide[0:1] % 2 == 0, both[0:1], both[1:2])
        stat_loc[0:1, 128 * j:128 * (j + 1)] = row * math.log2(math.e)
    ones = jnp.ones((8, head), jnp.bfloat16)
    for j in range(qrows // 256):
        part = pl.ds(256 * j, 256)
        prod = do_loc[part].astype(jnp.float32) * o_loc[part].astype(jnp.float32)
        hi = prod.astype(jnp.bfloat16)
        lo = (prod - hi.astype(jnp.float32)).astype(jnp.bfloat16)
        dims = (((1,), (1,)), ((), ()))
        total = lax.dot_general(ones, hi, dims, preferred_element_type=jnp.float32)
        total = total + lax.dot_general(ones, lo, dims, preferred_element_type=jnp.float32)
        stat_loc[1:2, 256 * j:256 * (j + 1)] = total[0:1]
    for d in range(8):
        @pl.when(me == d)
        def _(d=d):
            for n in range(len(QD_OWN[d])):
                send_stat(d, n)
            for item in REST.get(d, ()):
                send(d, item)

    loads[8].wait()
    lane = lax.broadcasted_iota(jnp.int32, (1, qrows), 1) // 2
    for h in range(HOPS + 1):
        pos = lane + (me + h) * rows
        start = jnp.zeros_like(pos)
        for j in range(cu_ref.shape[0]):
            start = jnp.maximum(start, jnp.where(pos >= cu_ref[j], cu_ref[j], 0))
        starts[h] = start

    def send_later():
        for d in LATER:
            @pl.when(me == d)
            def _(d=d):
                for item in LATER[d]:
                    send(d, item)

    def block(k_blk, v_blk, q_blk, do_blk, lse_row, d_row, keep):
        dims = (((1,), (1,)), ((), ()))
        scores = lax.dot_general(k_blk, q_blk, dims, preferred_element_type=jnp.float32)
        p_mat = jnp.where(keep, jnp.exp2(scores * factor - lse_row), 0.0)
        dp_mat = lax.dot_general(v_blk, do_blk, dims, preferred_element_type=jnp.float32)
        ds_mat = (p_mat * (dp_mat - d_row)).astype(jnp.bfloat16)
        return p_mat.astype(jnp.bfloat16), ds_mat

    def dq_term(k_blk, ds_mat):
        return lax.dot_general(k_blk, ds_mat, (((0,), (0,)), ((), ())), preferred_element_type=jnp.float32)

    def key_iota(keys, width):
        return lax.broadcasted_iota(jnp.int32, (keys, width), 0)

    half = qrows // 2

    def own_half(first, keys):
        cols = pl.ds(first, half)
        q_blk, do_blk, k_blk = q_loc[cols], do_loc[cols], k_loc[0:keys]
        key_pos = key_iota(keys, half)
        tok = lax.broadcasted_iota(jnp.int32, (keys, half), 1) // 2 + first // 2
        keep = (key_pos >= starts[0, :, cols] - me * rows) & (key_pos <= tok)
        p_low, ds_mat = block(k_blk, v_loc[0:keys], q_blk, do_blk, stat_loc[0:1, cols], stat_loc[1:2, cols], keep)
        dqt[:, cols] = dq_term(k_blk, ds_mat)
        dv_new = jnp.dot(p_low, do_blk, preferred_element_type=jnp.float32)
        dk_new = jnp.dot(ds_mat, q_blk, preferred_element_type=jnp.float32)
        if keys == rows:
            dv_acc[...] = dv_new
            dk_acc[...] = dk_new
        else:
            dv_acc[0:keys] = dv_acc[0:keys] + dv_new
            dk_acc[0:keys] = dk_acc[0:keys] + dk_new

    own_half(half, rows)
    for d in AFTER:
        @pl.when(me == d)
        def _(d=d):
            pl.semaphore_wait(go_sem, 1)
            for item in AFTER[d]:
                send(d, item)
    own_half(0, rows // 2)

    def finish_dq():
        dq_out[...] = (jnp.transpose(dqt[...]) * scale).astype(jnp.bfloat16)

    def kv_block(slot, count, first_key, width):
        cols = pl.ds(0, count)
        keys = pl.ds(first_key, width)
        base = (me - 1 - slot) * rows + first_key
        keep = key_iota(width, count) >= starts[0, :, cols] - base
        k_blk = k_buf[slot, keys]
        _, ds_mat = block(k_blk, v_buf[slot, keys], q_loc[cols], do_loc[cols], stat_loc[0:1, cols], stat_loc[1:2, cols], keep)
        dqt[:, cols] = dqt[:, cols] + dq_term(k_blk, ds_mat)

    def kv_unit(slot, chunk):
        far = slot == HOPS - 1
        late = (slot == 1) & (me == LATE_KEYS)

        @pl.when(far & (chunk == 0))
        def _():
            kv_block(slot, half, 0, kc_rows)

        @pl.when(late & (chunk == 0))
        def _():
            kv_block(slot, qrows, 0, kc_rows)

        @pl.when((far | late) & (chunk == 1))
        def _():
            kv_block(slot, qrows, kc_rows, kc_rows)

        @pl.when(jnp.logical_not(far | late) & (chunk == 1))
        def _():
            kv_block(slot, qrows, 0, rows)

    def qd_block(slot, first_row, count, first_key):
        cols = pl.ds(pl.multiple_of(first_row, 128), count)
        keys = pl.ds(first_key, rows - first_key)
        q_blk = q_buf[slot, cols]
        do_blk = do_buf[slot, cols]
        keep = key_iota(rows - first_key, count) >= starts[slot + 1, :, cols] - (me * rows + first_key)
        p_low, ds_mat = block(k_loc[keys], v_loc[keys], q_blk, do_blk, stat_buf[slot, 0:1, cols], stat_buf[slot, 1:2, cols], keep)
        dv_acc[keys] = dv_acc[keys] + jnp.dot(p_low, do_blk, preferred_element_type=jnp.float32)
        dk_acc[keys] = dk_acc[keys] + jnp.dot(ds_mat, q_blk, preferred_element_type=jnp.float32)

    def qd_unit(slot, chunk):
        quarters = (pick(tail, slot) == 1) & (chunk >= 2)
        short = (slot == HOPS - 1) & (chunk == 3)

        @pl.when(quarters)
        def _():
            qd_block(slot, chunk * qc_rows, qc_rows, 0)

        @pl.when((chunk % 2 == 1) & jnp.logical_not(quarters) & jnp.logical_not(short))
        def _():
            qd_block(slot, (chunk - 1) * qc_rows, half, 0)

        @pl.when(short & jnp.logical_not(quarters))
        def _():
            qd_block(slot, half, half, rows // 2)

    tail = [lut([(t >> h) % 2 for t in TAIL]) for h in range(HOPS)]
    last_kv = lut([max([-1] + [i for i, c in enumerate(step_codes(ORDER[d])) if c < 3 * NK and d > c // NK]) for d in range(8)])

    @pl.when(me == 0)
    def _():
        finish_dq()

    kv_on = [lut(targets_of(KV_REL, lambda d, h=h: (d, h + 1))) for h in range(HOPS)]
    qd_on = [lut(targets_of(QD_REL, lambda d, h=h: (d, h + 1))) for h in range(HOPS)]

    def pick(values, slot):
        return jnp.where(slot == 0, values[0], jnp.where(slot == 1, values[1], values[2]))

    per_word = 6
    codes = {d: step_codes(ORDER[d]) for d in range(8)}
    steps = max(len(c) for c in codes.values())
    words = -(-steps // per_word)
    packed = []
    for w in range(words):
        values = []
        for d in range(8):
            part = (codes[d] + [NONE] * (words * per_word))[w * per_word:(w + 1) * per_word]
            values.append(sum(c * 32 ** i for i, c in enumerate(part)))
        packed.append(lut(values))

    def step(i, carry):
        code = carry[0] % 32

        @pl.when(code < 3 * NK)
        def _():
            slot, chunk = code // NK, code % NK
            to = pick(kv_on, slot)
            for copy in kv_copies(k_buf.at[slot], v_buf.at[slot], kv_rel.at[slot], me * 4 + slot + 1, chunk):
                copy.wait_recv()

            @pl.when(to != NOBODY)
            def _():
                for copy in kv_copies(k_buf.at[slot], v_buf.at[slot], kv_rel.at[slot], to, chunk):
                    copy.start()

            @pl.when(me > slot)
            def _():
                kv_unit(slot, chunk)

            @pl.when(i == last_kv)
            def _():
                finish_dq()

        @pl.when((code >= 3 * NK) & (code < SEND))
        def _():
            slot, chunk = (code - 3 * NK) // NQ, (code - 3 * NK) % NQ
            to = pick(qd_on, slot)
            for copy in qd_copies(q_buf.at[slot], do_buf.at[slot], qd_rel.at[slot], me * 4 + slot + 1, chunk):
                copy.wait_recv()

            @pl.when(to != NOBODY)
            def _():
                for copy in qd_copies(q_buf.at[slot], do_buf.at[slot], qd_rel.at[slot], to, chunk):
                    copy.start()

            @pl.when(chunk == 0)
            def _():
                stat_copy(stat_buf.at[slot], stat_rel.at[slot], me * 4 + slot + 1).wait_recv()

                @pl.when(to != NOBODY)
                def _():
                    stat_copy(stat_buf.at[slot], stat_rel.at[slot], to).start()

            @pl.when(me + slot < 7)
            def _():
                qd_unit(slot, chunk)

        @pl.when(code == SEND)
        def _():
            send_later()

        last = (i % per_word) == per_word - 1
        rest = [jnp.where(last, (carry + (jnp.int32(0),))[w + 1], carry[w] // 32 if w == 0 else carry[w]) for w in range(words)]
        return tuple(rest)

    lax.fori_loop(0, steps, step, tuple(packed))

    dk_out[...] = (dk_acc[...] * scale).astype(jnp.bfloat16)
    dv_out[...] = dv_acc[...].astype(jnp.bfloat16)

    def sent(ref, sem):
        pltpu.make_async_remote_copy(src_ref=ref, dst_ref=ref, send_sem=sem, recv_sem=sem, device_id=place(me), device_id_type=MESH).wait_send()

    for targets, kv_sem in ((kv_to, kv_own), (kv_on, kv_rel)):
        for n, target in enumerate(targets):
            @pl.when(target != NOBODY)
            def _(n=n, kv_sem=kv_sem):
                sent(q_buf.at[0], kv_sem.at[n])
    for targets, qd_sem, stat_sem in ((qd_to, qd_own, stat_own), (qd_on, qd_rel, stat_rel)):
        for n, target in enumerate(targets):
            @pl.when(target != NOBODY)
            def _(n=n, qd_sem=qd_sem, stat_sem=stat_sem):
                sent(q_buf.at[0:2], qd_sem.at[n])
                sent(stat_loc, stat_sem.at[n])


def store_body(dq_ref, dk_ref, dv_ref, dq_out, dk_out, dv_out, sems):
    pairs = ((dq_ref, dq_out), (dk_ref, dk_out), (dv_ref, dv_out))
    copies = [pltpu.make_async_copy(src, dst, sems.at[i]) for i, (src, dst) in enumerate(pairs)]
    for copy in copies:
        copy.start()
    for copy in copies:
        copy.wait()


def solution(mesh):
    def local(queries, keys, values, attn_out, logsumexp, d_out, cu_seqlens):
        rows, heads, head = queries.shape
        qrows = rows * heads
        bf, f32 = jnp.bfloat16, jnp.float32
        dma = pltpu.SemaphoreType.DMA
        any_spec = pl.BlockSpec(memory_space=pl.ANY)
        vmem_spec = pl.BlockSpec(memory_space=pltpu.VMEM)
        shapes = ((qrows, head), (rows, head), (rows, head))
        results = pl.pallas_call(
            body,
            name="packed_backward",
            out_shape=tuple(pltpu.VMEM(shape, bf) for shape in shapes),
            in_specs=[any_spec] * 7,
            out_specs=(vmem_spec,) * 3,
            scratch_shapes=[
                pltpu.VMEM((qrows, head), bf), pltpu.VMEM((rows, head), bf), pltpu.VMEM((rows, head), bf),
                pltpu.VMEM((qrows, head), bf), pltpu.VMEM((heads, rows), f32), pltpu.VMEM((qrows, head), bf),
                pltpu.VMEM((2, qrows), f32), pltpu.VMEM((HOPS + 1, 1, qrows), jnp.int32),
                pltpu.VMEM((HOPS, rows, head), bf), pltpu.VMEM((HOPS, rows, head), bf),
                pltpu.VMEM((HOPS, qrows, head), bf), pltpu.VMEM((HOPS, qrows, head), bf), pltpu.VMEM((HOPS, 2, qrows), f32),
                pltpu.VMEM((head, qrows), f32), pltpu.VMEM((rows, head), f32), pltpu.VMEM((rows, head), f32),
                pltpu.SMEM(cu_seqlens.shape, jnp.int32), dma((9,)), pltpu.SemaphoreType.REGULAR,
                dma((HOPS, NK)), dma((HOPS, NK)), dma((HOPS, NQ)), dma((HOPS, NQ)), dma((HOPS,)),
                dma((2,)), dma((2,)), dma((2,)), dma((HOPS,)), dma((HOPS,)), dma((HOPS,)),
            ],
            compiler_params=pltpu.CompilerParams(collective_id=0, has_side_effects=True),
        )(cu_seqlens, queries.reshape(qrows, head), keys, values, attn_out.reshape(qrows, head), logsumexp.T, d_out.reshape(qrows, head))
        d_query, d_key, d_value = pl.pallas_call(
            store_body,
            name="store",
            out_shape=tuple(jax.ShapeDtypeStruct(shape, bf) for shape in shapes),
            in_specs=[vmem_spec] * 3,
            out_specs=(any_spec,) * 3,
            scratch_shapes=[dma((3,))],
        )(*[pltpu.with_memory_space_constraint(x, pltpu.VMEM) for x in results])
        return d_query.reshape(rows, heads, head), d_key, d_value

    seq_spec = P(("dp", "cpo", "cp"))
    return jax.shard_map(local, mesh=mesh, in_specs=(seq_spec,) * 6 + (P("dp"),), out_specs=(seq_spec,) * 3, check_vma=False)
```

```python
import functools
import math

import jax
import jax.numpy as jnp
from jax import lax
from jax.experimental import pallas as pl
from jax.experimental.pallas import tpu as pltpu
from jax.sharding import PartitionSpec as P

MESH = pl.DeviceIdType.MESH
HOPS = 3
NK = 2
NQ = 4
NONE = 31
NOBODY = 63
SEND = 18

KV_OWN = {0: [(1, 1), (2, 2)], 1: [(3, 2), (4, 3)], 2: [(3, 1), (5, 3)], 3: [(6, 3)], 4: [(5, 1), (6, 2)], 5: [(7, 2)], 6: [(7, 1)], 7: []}
QD_OWN = {0: [], 1: [(0, 1)], 2: [(0, 2)], 3: [(2, 1), (1, 2)], 4: [(1, 3)], 5: [(4, 1), (3, 2)], 6: [(4, 2), (3, 3)], 7: [(6, 1), (5, 2)]}
FIRST = {
    0: (0, 10, 1, 11),
    1: (0, 1, 100),
    2: (0, 1, 100),
    3: (100, 110),
    4: (0, 10, 1, 11, 100),
    5: (0, 100),
    6: (0, 1, 110, 100),
    7: (100, 110),
}
REST = {
    1: (101, 102, 103),
    2: (),
    3: (101, 111, 102, 112, 103),
    4: (101, 102, 103),
    5: (110, 101, 1, 111, 112, 113, 102, 103),
    6: (111, 112, 113, 101),
    7: (101, 111, 102, 103),
}
AFTER = {
    1: (10, 11),
    2: (10, 101, 102, 103, 11),
    3: (0, 1),
}
LATER = {
    3: (113,),
    6: (102, 103),
    7: (112, 113),
}
TAIL = (2, 3, 0, 0, 2, 3, 0, 0)
LATE_KEYS = 4
GO = ((4, 1), (5, 2), (6, 3))
KV_REL = {(2, 2): (3, 3), (3, 2): (2, 1), (5, 3): (4, 2), (4, 1): (5, 2), (6, 3): (4, 1), (6, 2): (7, 3), (7, 2): (6, 1)}
QD_REL = {(0, 2): (1, 1), (1, 2): (0, 3), (1, 3): (3, 1), (3, 1): (2, 2), (3, 2): (2, 3), (4, 2): (5, 1), (5, 2): (4, 3)}
ORDER = ("ghijkoplmqnr", "aobkpqlrghminj", "ghijcadbkolpmqnr", "abcedfsgkhlimjnopqr", "gheijkfolpcabmnqrd", "abkglhecdimnfj", "ghijceafsdb", "abcefds")


def step_codes(letters):
    return [ord(x) - ord("a") for x in letters]


def targets_of(table, pick):
    pairs = [table.get(pick(d), NOBODY) for d in range(8)]
    return [p if p == NOBODY else p[0] * 4 + p[1] for p in pairs]


def nth(table, n):
    return [NOBODY if len(table[d]) <= n else table[d][n][0] * 4 + table[d][n][1] for d in range(8)]


def partners():
    near = {d: set() for d in range(8)}
    pairs = [(d, target) for table in (KV_OWN, QD_OWN) for d in table for target, _ in table[d]]
    pairs += [(d, target) for table in (KV_REL, QD_REL) for (d, _), (target, _) in table.items()]
    for a, b in pairs:
        for here, there in ((a, b), (b, a)):
            if here >= 4 or there < 4:
                near[here].add(there)
    return near


def body(
    cu_hbm, q_hbm, k_hbm, v_hbm, o_hbm, lse_hbm, do_hbm,
    dq_out, dk_out, dv_out,
    q_loc, k_loc, v_loc, o_loc, lse_loc, do_loc, stat_loc, starts,
    k_buf, v_buf, q_buf, do_buf, stat_buf,
    dqt, dk_acc, dv_acc, cu_ref, in_sem, go_sem,
    k_recv, v_recv, q_recv, do_recv, stat_recv,
    kv_own, qd_own, stat_own, kv_rel, qd_rel, stat_rel,
):
    rows = k_loc.shape[0]
    qrows = q_loc.shape[0]
    head = k_loc.shape[1]
    kc_rows = rows // NK
    qc_rows = qrows // NQ
    scale = head ** -0.5
    factor = scale * math.log2(math.e)
    me = lax.axis_index("cpo") * 4 + lax.axis_index("cp")

    def lut(values):
        out = jnp.int32(values[0])
        for d in range(1, len(values)):
            out = jnp.where(me == d, jnp.int32(values[d]), out)
        return out

    def place(target):
        return {"cpo": target // 4, "cp": target % 4}

    barrier = pltpu.get_barrier_semaphore()
    near = partners()
    for d in range(8):
        @pl.when(me == d)
        def _(d=d):
            for other in [x for x in range(8) if d in near[x]]:
                pl.semaphore_signal(barrier, inc=1, device_id=place(other), device_id_type=MESH)
    loads = [
        pltpu.make_async_copy(src, dst, in_sem.at[i])
        for i, (src, dst) in enumerate(
            [
                (q_hbm.at[0:qc_rows], q_loc.at[0:qc_rows]), (do_hbm.at[0:qc_rows], do_loc.at[0:qc_rows]), (k_hbm, k_loc), (v_hbm, v_loc),
                (q_hbm.at[qc_rows:], q_loc.at[qc_rows:]), (do_hbm.at[qc_rows:], do_loc.at[qc_rows:]), (o_hbm, o_loc), (lse_hbm, lse_loc),
                (cu_hbm, cu_ref),
            ]
        )
    ]
    for load in loads:
        load.start()
    for d in range(8):
        @pl.when(me == d)
        def _(d=d):
            pl.semaphore_wait(barrier, len(near[d]))
            for teller, told in GO:
                if teller == d:
                    pl.semaphore_signal(go_sem, inc=1, device_id=place(told), device_id_type=MESH)

    def kv_copies(src_k, src_v, sem, code, chunk):
        target, there = code // 4, code % 4 - 1
        part = pl.ds(chunk * kc_rows, kc_rows)
        return [
            pltpu.make_async_remote_copy(
                src_ref=src.at[part], dst_ref=buf.at[there, part], send_sem=sem, recv_sem=recv.at[there, chunk],
                device_id=place(target), device_id_type=MESH)
            for src, buf, recv in ((src_k, k_buf, k_recv), (src_v, v_buf, v_recv))
        ]

    def qd_copies(src_q, src_do, sem, code, chunk):
        target, there = code // 4, code % 4 - 1
        part = pl.ds(chunk * qc_rows, qc_rows)
        return [
            pltpu.make_async_remote_copy(
                src_ref=src.at[part], dst_ref=buf.at[there, part], send_sem=sem, recv_sem=recv.at[there, chunk],
                device_id=place(target), device_id_type=MESH)
            for src, buf, recv in ((src_q, q_buf, q_recv), (src_do, do_buf, do_recv))
        ]

    def stat_copy(src, sem, code):
        target, there = code // 4, code % 4 - 1
        return pltpu.make_async_remote_copy(
            src_ref=src, dst_ref=stat_buf.at[there], send_sem=sem, recv_sem=stat_recv.at[there],
            device_id=place(target), device_id_type=MESH)

    kv_to = [lut(nth(KV_OWN, n)) for n in range(2)]
    qd_to = [lut(nth(QD_OWN, n)) for n in range(2)]

    def send(d, item):
        kind, n, chunk = item // 100, item // 10 % 10, item % 10
        target, there = (KV_OWN, QD_OWN)[kind][d][n]
        code = target * 4 + there
        if kind == 0:
            copies = kv_copies(k_loc, v_loc, kv_own.at[n], code, chunk)
        else:
            copies = qd_copies(q_loc, do_loc, qd_own.at[n], code, chunk)
        for copy in copies:
            copy.start()

    def send_stat(d, n):
        target, there = QD_OWN[d][n]
        stat_copy(stat_loc, stat_own.at[n], target * 4 + there).start()

    loads[0].wait()
    loads[1].wait()
    for d in range(8):
        @pl.when(me == d)
        def _(d=d):
            for item in FIRST[d]:
                if item >= 100:
                    send(d, item)
    loads[2].wait()
    loads[3].wait()
    for d in range(8):
        @pl.when(me == d)
        def _(d=d):
            for item in FIRST[d]:
                if item < 100:
                    send(d, item)
    for load in loads[4:8]:
        load.wait()

    wide = lax.broadcasted_iota(jnp.int32, (2, 128), 1)
    for j in range(qrows // 128):
        src = lse_loc[:, 128 * (j // 2):128 * (j // 2 + 1)]
        both = jnp.take_along_axis(src, 64 * (j % 2) + wide // 2, axis=1, mode="promise_in_bounds")
        row = jnp.where(wide[0:1] % 2 == 0, both[0:1], both[1:2])
        stat_loc[0:1, 128 * j:128 * (j + 1)] = row * math.log2(math.e)
    ones = jnp.ones((8, head), jnp.bfloat16)
    for j in range(qrows // 256):
        part = pl.ds(256 * j, 256)
        prod = do_loc[part].astype(jnp.float32) * o_loc[part].astype(jnp.float32)
        hi = prod.astype(jnp.bfloat16)
        lo = (prod - hi.astype(jnp.float32)).astype(jnp.bfloat16)
        dims = (((1,), (1,)), ((), ()))
        total = lax.dot_general(ones, hi, dims, preferred_element_type=jnp.float32)
        total = total + lax.dot_general(ones, lo, dims, preferred_element_type=jnp.float32)
        stat_loc[1:2, 256 * j:256 * (j + 1)] = total[0:1]
    for d in range(8):
        @pl.when(me == d)
        def _(d=d):
            for n in range(len(QD_OWN[d])):
                send_stat(d, n)
            for item in REST.get(d, ()):
                send(d, item)

    loads[8].wait()
    lane = lax.broadcasted_iota(jnp.int32, (1, qrows), 1) // 2
    for h in range(HOPS + 1):
        pos = lane + (me + h) * rows
        start = jnp.zeros_like(pos)
        for j in range(cu_ref.shape[0]):
            start = jnp.maximum(start, jnp.where(pos >= cu_ref[j], cu_ref[j], 0))
        starts[h] = start

    def send_later():
        for d in LATER:
            @pl.when(me == d)
            def _(d=d):
                for item in LATER[d]:
                    send(d, item)

    def block(k_blk, v_blk, q_blk, do_blk, lse_row, d_row, keep):
        dims = (((1,), (1,)), ((), ()))
        scores = lax.dot_general(k_blk, q_blk, dims, preferred_element_type=jnp.float32)
        p_mat = jnp.where(keep, jnp.exp2(scores * factor - lse_row), 0.0)
        dp_mat = lax.dot_general(v_blk, do_blk, dims, preferred_element_type=jnp.float32)
        ds_mat = (p_mat * (dp_mat - d_row)).astype(jnp.bfloat16)
        return p_mat.astype(jnp.bfloat16), ds_mat

    def dq_term(k_blk, ds_mat):
        return lax.dot_general(k_blk, ds_mat, (((0,), (0,)), ((), ())), preferred_element_type=jnp.float32)

    def key_iota(keys, width):
        return lax.broadcasted_iota(jnp.int32, (keys, width), 0)

    half = qrows // 2

    def own_half(first, keys):
        cols = pl.ds(first, half)
        q_blk, do_blk, k_blk = q_loc[cols], do_loc[cols], k_loc[0:keys]
        key_pos = key_iota(keys, half)
        tok = lax.broadcasted_iota(jnp.int32, (keys, half), 1) // 2 + first // 2
        keep = (key_pos >= starts[0, :, cols] - me * rows) & (key_pos <= tok)
        p_low, ds_mat = block(k_blk, v_loc[0:keys], q_blk, do_blk, stat_loc[0:1, cols], stat_loc[1:2, cols], keep)
        dqt[:, cols] = dq_term(k_blk, ds_mat)
        dv_new = jnp.dot(p_low, do_blk, preferred_element_type=jnp.float32)
        dk_new = jnp.dot(ds_mat, q_blk, preferred_element_type=jnp.float32)
        if keys == rows:
            dv_acc[...] = dv_new
            dk_acc[...] = dk_new
        else:
            dv_acc[0:keys] = dv_acc[0:keys] + dv_new
            dk_acc[0:keys] = dk_acc[0:keys] + dk_new

    own_half(half, rows)
    for d in AFTER:
        @pl.when(me == d)
        def _(d=d):
            pl.semaphore_wait(go_sem, 1)
            for item in AFTER[d]:
                send(d, item)
    own_half(0, rows // 2)

    def finish_dq():
        dq_out[...] = (jnp.transpose(dqt[...]) * scale).astype(jnp.bfloat16)

    def kv_block(slot, count, first_key, width):
        cols = pl.ds(0, count)
        keys = pl.ds(first_key, width)
        base = (me - 1 - slot) * rows + first_key
        keep = key_iota(width, count) >= starts[0, :, cols] - base
        k_blk = k_buf[slot, keys]
        _, ds_mat = block(k_blk, v_buf[slot, keys], q_loc[cols], do_loc[cols], stat_loc[0:1, cols], stat_loc[1:2, cols], keep)
        dqt[:, cols] = dqt[:, cols] + dq_term(k_blk, ds_mat)

    def kv_unit(slot, chunk):
        far = slot == HOPS - 1
        late = (slot == 1) & (me == LATE_KEYS)

        @pl.when(far & (chunk == 0))
        def _():
            kv_block(slot, half, 0, kc_rows)

        @pl.when(late & (chunk == 0))
        def _():
            kv_block(slot, qrows, 0, kc_rows)

        @pl.when((far | late) & (chunk == 1))
        def _():
            kv_block(slot, qrows, kc_rows, kc_rows)

        @pl.when(jnp.logical_not(far | late) & (chunk == 1))
        def _():
            kv_block(slot, qrows, 0, rows)

    def qd_block(slot, first_row, count, first_key):
        cols = pl.ds(pl.multiple_of(first_row, 128), count)
        keys = pl.ds(first_key, rows - first_key)
        q_blk = q_buf[slot, cols]
        do_blk = do_buf[slot, cols]
        keep = key_iota(rows - first_key, count) >= starts[slot + 1, :, cols] - (me * rows + first_key)
        p_low, ds_mat = block(k_loc[keys], v_loc[keys], q_blk, do_blk, stat_buf[slot, 0:1, cols], stat_buf[slot, 1:2, cols], keep)
        dv_acc[keys] = dv_acc[keys] + jnp.dot(p_low, do_blk, preferred_element_type=jnp.float32)
        dk_acc[keys] = dk_acc[keys] + jnp.dot(ds_mat, q_blk, preferred_element_type=jnp.float32)

    def qd_unit(slot, chunk):
        quarters = (pick(tail, slot) == 1) & (chunk >= 2)
        short = (slot == HOPS - 1) & (chunk == 3)

        @pl.when(quarters)
        def _():
            qd_block(slot, chunk * qc_rows, qc_rows, 0)

        @pl.when((chunk % 2 == 1) & jnp.logical_not(quarters) & jnp.logical_not(short))
        def _():
            qd_block(slot, (chunk - 1) * qc_rows, half, 0)

        @pl.when(short & jnp.logical_not(quarters))
        def _():
            qd_block(slot, half, half, rows // 2)

    tail = [lut([(t >> h) % 2 for t in TAIL]) for h in range(HOPS)]
    last_kv = lut([max([-1] + [i for i, c in enumerate(step_codes(ORDER[d])) if c < 3 * NK and d > c // NK]) for d in range(8)])

    @pl.when(me == 0)
    def _():
        finish_dq()

    kv_on = [lut(targets_of(KV_REL, lambda d, h=h: (d, h + 1))) for h in range(HOPS)]
    qd_on = [lut(targets_of(QD_REL, lambda d, h=h: (d, h + 1))) for h in range(HOPS)]

    def pick(values, slot):
        return jnp.where(slot == 0, values[0], jnp.where(slot == 1, values[1], values[2]))

    per_word = 6
    codes = {d: step_codes(ORDER[d]) for d in range(8)}
    steps = max(len(c) for c in codes.values())
    words = -(-steps // per_word)
    packed = []
    for w in range(words):
        values = []
        for d in range(8):
            part = (codes[d] + [NONE] * (words * per_word))[w * per_word:(w + 1) * per_word]
            values.append(sum(c * 32 ** i for i, c in enumerate(part)))
        packed.append(lut(values))

    def step(i, carry):
        code = carry[0] % 32

        @pl.when(code < 3 * NK)
        def _():
            slot, chunk = code // NK, code % NK
            to = pick(kv_on, slot)
            for copy in kv_copies(k_buf.at[slot], v_buf.at[slot], kv_rel.at[slot], me * 4 + slot + 1, chunk):
                copy.wait_recv()

            @pl.when(to != NOBODY)
            def _():
                for copy in kv_copies(k_buf.at[slot], v_buf.at[slot], kv_rel.at[slot], to, chunk):
                    copy.start()

            @pl.when(me > slot)
            def _():
                kv_unit(slot, chunk)

            @pl.when(i == last_kv)
            def _():
                finish_dq()

        @pl.when((code >= 3 * NK) & (code < SEND))
        def _():
            slot, chunk = (code - 3 * NK) // NQ, (code - 3 * NK) % NQ
            to = pick(qd_on, slot)
            for copy in qd_copies(q_buf.at[slot], do_buf.at[slot], qd_rel.at[slot], me * 4 + slot + 1, chunk):
                copy.wait_recv()

            @pl.when(to != NOBODY)
            def _():
                for copy in qd_copies(q_buf.at[slot], do_buf.at[slot], qd_rel.at[slot], to, chunk):
                    copy.start()

            @pl.when(chunk == 0)
            def _():
                stat_copy(stat_buf.at[slot], stat_rel.at[slot], me * 4 + slot + 1).wait_recv()

                @pl.when(to != NOBODY)
                def _():
                    stat_copy(stat_buf.at[slot], stat_rel.at[slot], to).start()

            @pl.when(me + slot < 7)
            def _():
                qd_unit(slot, chunk)

        @pl.when(code == SEND)
        def _():
            send_later()

        last = (i % per_word) == per_word - 1
        rest = [jnp.where(last, (carry + (jnp.int32(0),))[w + 1], carry[w] // 32 if w == 0 else carry[w]) for w in range(words)]
        return tuple(rest)

    lax.fori_loop(0, steps, step, tuple(packed))

    dk_out[...] = (dk_acc[...] * scale).astype(jnp.bfloat16)
    dv_out[...] = dv_acc[...].astype(jnp.bfloat16)

    def sent(ref, sem):
        pltpu.make_async_remote_copy(src_ref=ref, dst_ref=ref, send_sem=sem, recv_sem=sem, device_id=place(me), device_id_type=MESH).wait_send()

    for targets, kv_sem in ((kv_to, kv_own), (kv_on, kv_rel)):
        for n, target in enumerate(targets):
            @pl.when(target != NOBODY)
            def _(n=n, kv_sem=kv_sem):
                sent(q_buf.at[0], kv_sem.at[n])
    for targets, qd_sem, stat_sem in ((qd_to, qd_own, stat_own), (qd_on, qd_rel, stat_rel)):
        for n, target in enumerate(targets):
            @pl.when(target != NOBODY)
            def _(n=n, qd_sem=qd_sem, stat_sem=stat_sem):
                sent(q_buf.at[0:2], qd_sem.at[n])
                sent(stat_loc, stat_sem.at[n])


def store_body(dq_ref, dk_ref, dv_ref, dq_out, dk_out, dv_out, sems):
    pairs = ((dq_ref, dq_out), (dk_ref, dk_out), (dv_ref, dv_out))
    copies = [pltpu.make_async_copy(src, dst, sems.at[i]) for i, (src, dst) in enumerate(pairs)]
    for copy in copies:
        copy.start()
    for copy in copies:
        copy.wait()


def solution(mesh):
    def local(queries, keys, values, attn_out, logsumexp, d_out, cu_seqlens):
        rows, heads, head = queries.shape
        qrows = rows * heads
        bf, f32 = jnp.bfloat16, jnp.float32
        dma = pltpu.SemaphoreType.DMA
        any_spec = pl.BlockSpec(memory_space=pl.ANY)
        vmem_spec = pl.BlockSpec(memory_space=pltpu.VMEM)
        shapes = ((qrows, head), (rows, head), (rows, head))
        results = pl.pallas_call(
            body,
            name="packed_backward",
            out_shape=tuple(pltpu.VMEM(shape, bf) for shape in shapes),
            in_specs=[any_spec] * 7,
            out_specs=(vmem_spec,) * 3,
            scratch_shapes=[
                pltpu.VMEM((qrows, head), bf), pltpu.VMEM((rows, head), bf), pltpu.VMEM((rows, head), bf),
                pltpu.VMEM((qrows, head), bf), pltpu.VMEM((heads, rows), f32), pltpu.VMEM((qrows, head), bf),
                pltpu.VMEM((2, qrows), f32), pltpu.VMEM((HOPS + 1, 1, qrows), jnp.int32),
                pltpu.VMEM((HOPS, rows, head), bf), pltpu.VMEM((HOPS, rows, head), bf),
                pltpu.VMEM((HOPS, qrows, head), bf), pltpu.VMEM((HOPS, qrows, head), bf), pltpu.VMEM((HOPS, 2, qrows), f32),
                pltpu.VMEM((head, qrows), f32), pltpu.VMEM((rows, head), f32), pltpu.VMEM((rows, head), f32),
                pltpu.SMEM(cu_seqlens.shape, jnp.int32), dma((9,)), pltpu.SemaphoreType.REGULAR,
                dma((HOPS, NK)), dma((HOPS, NK)), dma((HOPS, NQ)), dma((HOPS, NQ)), dma((HOPS,)),
                dma((2,)), dma((2,)), dma((2,)), dma((HOPS,)), dma((HOPS,)), dma((HOPS,)),
            ],
            compiler_params=pltpu.CompilerParams(collective_id=0, has_side_effects=True),
        )(cu_seqlens, queries.reshape(qrows, head), keys, values, attn_out.reshape(qrows, head), logsumexp.T, d_out.reshape(qrows, head))
        d_query, d_key, d_value = pl.pallas_call(
            store_body,
            name="store",
            out_shape=tuple(jax.ShapeDtypeStruct(shape, bf) for shape in shapes),
            in_specs=[vmem_spec] * 3,
            out_specs=(any_spec,) * 3,
            scratch_shapes=[dma((3,))],
        )(*[pltpu.with_memory_space_constraint(x, pltpu.VMEM) for x in results])
        return d_query.reshape(rows, heads, head), d_key, d_value

    seq_spec = P(("dp", "cpo", "cp"))
    return jax.shard_map(local, mesh=mesh, in_specs=(seq_spec,) * 6 + (P("dp"),), out_specs=(seq_spec,) * 3, check_vma=False)
```

```python
import functools
import math

import jax
import jax.numpy as jnp
from jax import lax
from jax.experimental import pallas as pl
from jax.experimental.pallas import tpu as pltpu
from jax.sharding import PartitionSpec as P

MESH = pl.DeviceIdType.MESH
HOPS = 3
NK = 2
NQ = 4
NONE = 31
NOBODY = 63
SEND = 18

KV_OWN = {0: [(1, 1), (2, 2)], 1: [(3, 2), (4, 3)], 2: [(3, 1), (5, 3)], 3: [(6, 3)], 4: [(5, 1), (6, 2)], 5: [(7, 2)], 6: [(7, 1)], 7: []}
QD_OWN = {0: [], 1: [(0, 1)], 2: [(0, 2)], 3: [(2, 1), (1, 2)], 4: [(1, 3)], 5: [(4, 1), (3, 2)], 6: [(4, 2), (3, 3)], 7: [(6, 1), (5, 2)]}
FIRST = {
    0: (0, 10, 1, 11),
    1: (0, 1, 100),
    2: (0, 1, 100),
    3: (100, 110),
    4: (0, 10, 1, 11, 100),
    5: (0, 100),
    6: (0, 1, 110, 100),
    7: (100, 110),
}
REST = {
    1: (101, 102, 103),
    2: (),
    3: (101, 111, 102, 112, 103),
    4: (101, 102, 103),
    5: (110, 101, 1, 111, 112, 113, 102, 103),
    6: (111, 112, 113, 101),
    7: (101, 111, 102, 112, 103),
}
AFTER = {
    1: (10, 11),
    2: (10, 101, 102, 103, 11),
    3: (0, 1),
}
LATER = {
    3: (113,),
    6: (102, 103),
    7: (113,),
}
TAIL = (2, 3, 0, 0, 2, 3, 0, 0)
LATE_KEYS = 4
GO = ((4, 1), (5, 2), (6, 3))
KV_REL = {(2, 2): (3, 3), (3, 2): (2, 1), (5, 3): (4, 2), (4, 1): (5, 2), (6, 3): (4, 1), (6, 2): (7, 3), (7, 2): (6, 1)}
QD_REL = {(0, 2): (1, 1), (1, 2): (0, 3), (1, 3): (3, 1), (3, 1): (2, 2), (3, 2): (2, 3), (4, 2): (5, 1), (5, 2): (4, 3)}
ORDER = ("ghijkoplmqnr", "aobkpqlrghminj", "ghijcadbkolpmqnr", "abcedfsgkhlimjnopqr", "gheijkfolpcabmnqrd", "abkglhecdminfj", "ghijcefsadb", "abcefds")


def step_codes(letters):
    return [ord(x) - ord("a") for x in letters]


def targets_of(table, pick):
    pairs = [table.get(pick(d), NOBODY) for d in range(8)]
    return [p if p == NOBODY else p[0] * 4 + p[1] for p in pairs]


def nth(table, n):
    return [NOBODY if len(table[d]) <= n else table[d][n][0] * 4 + table[d][n][1] for d in range(8)]


def partners():
    near = {d: set() for d in range(8)}
    pairs = [(d, target) for table in (KV_OWN, QD_OWN) for d in table for target, _ in table[d]]
    pairs += [(d, target) for table in (KV_REL, QD_REL) for (d, _), (target, _) in table.items()]
    for a, b in pairs:
        for here, there in ((a, b), (b, a)):
            if here >= 4 or there < 4:
                near[here].add(there)
    return near


def body(
    cu_hbm, q_hbm, k_hbm, v_hbm, o_hbm, lse_hbm, do_hbm,
    dq_out, dk_acc, dv_acc,
    q_loc, k_loc, v_loc, o_loc, lse_loc, do_loc, stat_loc, starts,
    k_buf, v_buf, q_buf, do_buf, stat_buf,
    dqt, cu_ref, in_sem, go_sem,
    k_recv, v_recv, q_recv, do_recv, stat_recv,
    kv_own, qd_own, stat_own, kv_rel, qd_rel, stat_rel,
):
    rows = k_loc.shape[0]
    qrows = q_loc.shape[0]
    head = k_loc.shape[1]
    kc_rows = rows // NK
    qc_rows = qrows // NQ
    scale = head ** -0.5
    factor = scale * math.log2(math.e)
    me = lax.axis_index("cpo") * 4 + lax.axis_index("cp")

    def lut(values):
        out = jnp.int32(values[0])
        for d in range(1, len(values)):
            out = jnp.where(me == d, jnp.int32(values[d]), out)
        return out

    def place(target):
        return {"cpo": target // 4, "cp": target % 4}

    barrier = pltpu.get_barrier_semaphore()
    near = partners()
    for d in range(8):
        @pl.when(me == d)
        def _(d=d):
            for other in [x for x in range(8) if d in near[x]]:
                pl.semaphore_signal(barrier, inc=1, device_id=place(other), device_id_type=MESH)
    loads = [
        pltpu.make_async_copy(src, dst, in_sem.at[i])
        for i, (src, dst) in enumerate(
            [
                (q_hbm.at[0:qc_rows], q_loc.at[0:qc_rows]), (do_hbm.at[0:qc_rows], do_loc.at[0:qc_rows]), (k_hbm, k_loc), (v_hbm, v_loc),
                (q_hbm.at[qc_rows:], q_loc.at[qc_rows:]), (do_hbm.at[qc_rows:], do_loc.at[qc_rows:]), (o_hbm, o_loc), (lse_hbm, lse_loc),
                (cu_hbm, cu_ref),
            ]
        )
    ]
    for load in loads:
        load.start()
    for d in range(8):
        @pl.when(me == d)
        def _(d=d):
            pl.semaphore_wait(barrier, len(near[d]))
            for teller, told in GO:
                if teller == d:
                    pl.semaphore_signal(go_sem, inc=1, device_id=place(told), device_id_type=MESH)

    def kv_copies(src_k, src_v, sem, code, chunk):
        target, there = code // 4, code % 4 - 1
        part = pl.ds(chunk * kc_rows, kc_rows)
        return [
            pltpu.make_async_remote_copy(
                src_ref=src.at[part], dst_ref=buf.at[there, part], send_sem=sem, recv_sem=recv.at[there, chunk],
                device_id=place(target), device_id_type=MESH)
            for src, buf, recv in ((src_k, k_buf, k_recv), (src_v, v_buf, v_recv))
        ]

    def qd_copies(src_q, src_do, sem, code, chunk):
        target, there = code // 4, code % 4 - 1
        part = pl.ds(chunk * qc_rows, qc_rows)
        return [
            pltpu.make_async_remote_copy(
                src_ref=src.at[part], dst_ref=buf.at[there, part], send_sem=sem, recv_sem=recv.at[there, chunk],
                device_id=place(target), device_id_type=MESH)
            for src, buf, recv in ((src_q, q_buf, q_recv), (src_do, do_buf, do_recv))
        ]

    def stat_copy(src, sem, code):
        target, there = code // 4, code % 4 - 1
        return pltpu.make_async_remote_copy(
            src_ref=src, dst_ref=stat_buf.at[there], send_sem=sem, recv_sem=stat_recv.at[there],
            device_id=place(target), device_id_type=MESH)

    kv_to = [lut(nth(KV_OWN, n)) for n in range(2)]
    qd_to = [lut(nth(QD_OWN, n)) for n in range(2)]

    def send(d, item):
        kind, n, chunk = item // 100, item // 10 % 10, item % 10
        target, there = (KV_OWN, QD_OWN)[kind][d][n]
        code = target * 4 + there
        if kind == 0:
            copies = kv_copies(k_loc, v_loc, kv_own.at[n], code, chunk)
        else:
            copies = qd_copies(q_loc, do_loc, qd_own.at[n], code, chunk)
        for copy in copies:
            copy.start()

    def send_stat(d, n):
        target, there = QD_OWN[d][n]
        stat_copy(stat_loc, stat_own.at[n], target * 4 + there).start()

    loads[0].wait()
    loads[1].wait()
    for d in range(8):
        @pl.when(me == d)
        def _(d=d):
            for item in FIRST[d]:
                if item >= 100:
                    send(d, item)
    loads[2].wait()
    loads[3].wait()
    for d in range(8):
        @pl.when(me == d)
        def _(d=d):
            for item in FIRST[d]:
                if item < 100:
                    send(d, item)
    for load in loads[4:8]:
        load.wait()

    wide = lax.broadcasted_iota(jnp.int32, (2, 128), 1)
    for j in range(qrows // 128):
        src = lse_loc[:, 128 * (j // 2):128 * (j // 2 + 1)]
        both = jnp.take_along_axis(src, 64 * (j % 2) + wide // 2, axis=1, mode="promise_in_bounds")
        row = jnp.where(wide[0:1] % 2 == 0, both[0:1], both[1:2])
        stat_loc[0:1, 128 * j:128 * (j + 1)] = row * math.log2(math.e)
    ones = jnp.ones((8, head), jnp.bfloat16)
    for j in range(qrows // 256):
        part = pl.ds(256 * j, 256)
        prod = do_loc[part].astype(jnp.float32) * o_loc[part].astype(jnp.float32)
        hi = prod.astype(jnp.bfloat16)
        lo = (prod - hi.astype(jnp.float32)).astype(jnp.bfloat16)
        dims = (((1,), (1,)), ((), ()))
        total = lax.dot_general(ones, hi, dims, preferred_element_type=jnp.float32)
        total = total + lax.dot_general(ones, lo, dims, preferred_element_type=jnp.float32)
        stat_loc[1:2, 256 * j:256 * (j + 1)] = total[0:1]
    for d in range(8):
        @pl.when(me == d)
        def _(d=d):
            for n in range(len(QD_OWN[d])):
                send_stat(d, n)
            for item in REST.get(d, ()):
                send(d, item)

    loads[8].wait()
    lane = lax.broadcasted_iota(jnp.int32, (1, qrows), 1) // 2
    for h in range(HOPS + 1):
        pos = lane + (me + h) * rows
        start = jnp.zeros_like(pos)
        for j in range(cu_ref.shape[0]):
            start = jnp.maximum(start, jnp.where(pos >= cu_ref[j], cu_ref[j], 0))
        starts[h] = start

    def send_later():
        for d in LATER:
            @pl.when(me == d)
            def _(d=d):
                for item in LATER[d]:
                    send(d, item)

    def block(k_blk, v_blk, q_blk, do_blk, lse_row, d_row, keep):
        dims = (((1,), (1,)), ((), ()))
        scores = lax.dot_general(k_blk, q_blk, dims, preferred_element_type=jnp.float32)
        p_mat = jnp.where(keep, jnp.exp2(scores * factor - lse_row), 0.0)
        dp_mat = lax.dot_general(v_blk, do_blk, dims, preferred_element_type=jnp.float32)
        ds_mat = (p_mat * (dp_mat - d_row)).astype(jnp.bfloat16)
        return p_mat.astype(jnp.bfloat16), ds_mat

    def dq_term(k_blk, ds_mat):
        return lax.dot_general(k_blk, ds_mat, (((0,), (0,)), ((), ())), preferred_element_type=jnp.float32)

    def key_iota(keys, width):
        return lax.broadcasted_iota(jnp.int32, (keys, width), 0)

    half = qrows // 2

    def own_half(first, keys):
        cols = pl.ds(first, half)
        q_blk, do_blk, k_blk = q_loc[cols], do_loc[cols], k_loc[0:keys]
        key_pos = key_iota(keys, half)
        tok = lax.broadcasted_iota(jnp.int32, (keys, half), 1) // 2 + first // 2
        keep = (key_pos >= starts[0, :, cols] - me * rows) & (key_pos <= tok)
        p_low, ds_mat = block(k_blk, v_loc[0:keys], q_blk, do_blk, stat_loc[0:1, cols], stat_loc[1:2, cols], keep)
        dqt[:, cols] = dq_term(k_blk, ds_mat)
        dv_new = jnp.dot(p_low, do_blk, preferred_element_type=jnp.float32)
        dk_new = jnp.dot(ds_mat, q_blk, preferred_element_type=jnp.float32)
        if keys == rows:
            dv_acc[...] = dv_new
            dk_acc[...] = dk_new
        else:
            dv_acc[0:keys] = dv_acc[0:keys] + dv_new
            dk_acc[0:keys] = dk_acc[0:keys] + dk_new

    own_half(half, rows)
    for d in AFTER:
        @pl.when(me == d)
        def _(d=d):
            pl.semaphore_wait(go_sem, 1)
            for item in AFTER[d]:
                send(d, item)
    own_half(0, rows // 2)

    def finish_dq():
        dq_out[...] = (jnp.transpose(dqt[...]) * scale).astype(jnp.bfloat16)

    def kv_block(slot, count, first_key, width):
        cols = pl.ds(0, count)
        keys = pl.ds(first_key, width)
        base = (me - 1 - slot) * rows + first_key
        keep = key_iota(width, count) >= starts[0, :, cols] - base
        k_blk = k_buf[slot, keys]
        _, ds_mat = block(k_blk, v_buf[slot, keys], q_loc[cols], do_loc[cols], stat_loc[0:1, cols], stat_loc[1:2, cols], keep)
        dqt[:, cols] = dqt[:, cols] + dq_term(k_blk, ds_mat)

    def kv_unit(slot, chunk):
        far = slot == HOPS - 1
        late = (slot == 1) & (me == LATE_KEYS)

        @pl.when(far & (chunk == 0))
        def _():
            kv_block(slot, half, 0, kc_rows)

        @pl.when(late & (chunk == 0))
        def _():
            kv_block(slot, qrows, 0, kc_rows)

        @pl.when((far | late) & (chunk == 1))
        def _():
            kv_block(slot, qrows, kc_rows, kc_rows)

        @pl.when(jnp.logical_not(far | late) & (chunk == 1))
        def _():
            kv_block(slot, qrows, 0, rows)

    def qd_block(slot, first_row, count, first_key):
        cols = pl.ds(pl.multiple_of(first_row, 128), count)
        keys = pl.ds(first_key, rows - first_key)
        q_blk = q_buf[slot, cols]
        do_blk = do_buf[slot, cols]
        keep = key_iota(rows - first_key, count) >= starts[slot + 1, :, cols] - (me * rows + first_key)
        p_low, ds_mat = block(k_loc[keys], v_loc[keys], q_blk, do_blk, stat_buf[slot, 0:1, cols], stat_buf[slot, 1:2, cols], keep)
        dv_acc[keys] = dv_acc[keys] + jnp.dot(p_low, do_blk, preferred_element_type=jnp.float32)
        dk_acc[keys] = dk_acc[keys] + jnp.dot(ds_mat, q_blk, preferred_element_type=jnp.float32)

    def qd_unit(slot, chunk):
        quarters = (pick(tail, slot) == 1) & (chunk >= 2)
        short = (slot == HOPS - 1) & (chunk == 3)

        @pl.when(quarters)
        def _():
            qd_block(slot, chunk * qc_rows, qc_rows, 0)

        @pl.when((chunk % 2 == 1) & jnp.logical_not(quarters) & jnp.logical_not(short))
        def _():
            qd_block(slot, (chunk - 1) * qc_rows, half, 0)

        @pl.when(short & jnp.logical_not(quarters))
        def _():
            qd_block(slot, half, half, rows // 2)

    tail = [lut([(t >> h) % 2 for t in TAIL]) for h in range(HOPS)]
    last_kv = lut([max([-1] + [i for i, c in enumerate(step_codes(ORDER[d])) if c < 3 * NK and d > c // NK]) for d in range(8)])

    @pl.when(me == 0)
    def _():
        finish_dq()

    kv_on = [lut(targets_of(KV_REL, lambda d, h=h: (d, h + 1))) for h in range(HOPS)]
    qd_on = [lut(targets_of(QD_REL, lambda d, h=h: (d, h + 1))) for h in range(HOPS)]

    def pick(values, slot):
        return jnp.where(slot == 0, values[0], jnp.where(slot == 1, values[1], values[2]))

    per_word = 6
    codes = {d: step_codes(ORDER[d]) for d in range(8)}
    steps = max(len(c) for c in codes.values())
    words = -(-steps // per_word)
    packed = []
    for w in range(words):
        values = []
        for d in range(8):
            part = (codes[d] + [NONE] * (words * per_word))[w * per_word:(w + 1) * per_word]
            values.append(sum(c * 32 ** i for i, c in enumerate(part)))
        packed.append(lut(values))

    def step(i, carry):
        code = carry[0] % 32

        @pl.when(code < 3 * NK)
        def _():
            slot, chunk = code // NK, code % NK
            to = pick(kv_on, slot)
            for copy in kv_copies(k_buf.at[slot], v_buf.at[slot], kv_rel.at[slot], me * 4 + slot + 1, chunk):
                copy.wait_recv()

            @pl.when(to != NOBODY)
            def _():
                for copy in kv_copies(k_buf.at[slot], v_buf.at[slot], kv_rel.at[slot], to, chunk):
                    copy.start()

            @pl.when(me > slot)
            def _():
                kv_unit(slot, chunk)

            @pl.when(i == last_kv)
            def _():
                finish_dq()

        @pl.when((code >= 3 * NK) & (code < SEND))
        def _():
            slot, chunk = (code - 3 * NK) // NQ, (code - 3 * NK) % NQ
            to = pick(qd_on, slot)
            for copy in qd_copies(q_buf.at[slot], do_buf.at[slot], qd_rel.at[slot], me * 4 + slot + 1, chunk):
                copy.wait_recv()

            @pl.when(to != NOBODY)
            def _():
                for copy in qd_copies(q_buf.at[slot], do_buf.at[slot], qd_rel.at[slot], to, chunk):
                    copy.start()

            @pl.when(chunk == 0)
            def _():
                stat_copy(stat_buf.at[slot], stat_rel.at[slot], me * 4 + slot + 1).wait_recv()

                @pl.when(to != NOBODY)
                def _():
                    stat_copy(stat_buf.at[slot], stat_rel.at[slot], to).start()

            @pl.when(me + slot < 7)
            def _():
                qd_unit(slot, chunk)

        @pl.when(code == SEND)
        def _():
            send_later()

        last = (i % per_word) == per_word - 1
        rest = [jnp.where(last, (carry + (jnp.int32(0),))[w + 1], carry[w] // 32 if w == 0 else carry[w]) for w in range(words)]
        return tuple(rest)

    lax.fori_loop(0, steps, step, tuple(packed))

    def sent(ref, sem):
        pltpu.make_async_remote_copy(src_ref=ref, dst_ref=ref, send_sem=sem, recv_sem=sem, device_id=place(me), device_id_type=MESH).wait_send()

    for targets, kv_sem in ((kv_to, kv_own), (kv_on, kv_rel)):
        for n, target in enumerate(targets):
            @pl.when(target != NOBODY)
            def _(n=n, kv_sem=kv_sem):
                sent(q_buf.at[0], kv_sem.at[n])
    for targets, qd_sem, stat_sem in ((qd_to, qd_own, stat_own), (qd_on, qd_rel, stat_rel)):
        for n, target in enumerate(targets):
            @pl.when(target != NOBODY)
            def _(n=n, qd_sem=qd_sem, stat_sem=stat_sem):
                sent(q_buf.at[0:2], qd_sem.at[n])
                sent(stat_loc, stat_sem.at[n])


def store_body(dq_ref, dk_ref, dv_ref, dq_out, dk_out, dv_out, dk_st, dv_st, sems):
    pairs = ((dq_ref, dq_out), (dk_st, dk_out), (dv_st, dv_out))
    copies = [pltpu.make_async_copy(src, dst, sems.at[i]) for i, (src, dst) in enumerate(pairs)]
    copies[0].start()
    dk_st[...] = (dk_ref[...] * dk_ref.shape[1] ** -0.5).astype(jnp.bfloat16)
    copies[1].start()
    dv_st[...] = dv_ref[...].astype(jnp.bfloat16)
    copies[2].start()
    for copy in copies:
        copy.wait()


def solution(mesh):
    def local(queries, keys, values, attn_out, logsumexp, d_out, cu_seqlens):
        rows, heads, head = queries.shape
        qrows = rows * heads
        bf, f32 = jnp.bfloat16, jnp.float32
        dma = pltpu.SemaphoreType.DMA
        any_spec = pl.BlockSpec(memory_space=pl.ANY)
        vmem_spec = pl.BlockSpec(memory_space=pltpu.VMEM)
        shapes = ((qrows, head), (rows, head), (rows, head))
        results = pl.pallas_call(
            body,
            name="packed_backward",
            out_shape=tuple(pltpu.VMEM(shape, kind) for shape, kind in zip(shapes, (bf, f32, f32))),
            in_specs=[any_spec] * 7,
            out_specs=(vmem_spec,) * 3,
            scratch_shapes=[
                pltpu.VMEM((qrows, head), bf), pltpu.VMEM((rows, head), bf), pltpu.VMEM((rows, head), bf),
                pltpu.VMEM((qrows, head), bf), pltpu.VMEM((heads, rows), f32), pltpu.VMEM((qrows, head), bf),
                pltpu.VMEM((2, qrows), f32), pltpu.VMEM((HOPS + 1, 1, qrows), jnp.int32),
                pltpu.VMEM((HOPS, rows, head), bf), pltpu.VMEM((HOPS, rows, head), bf),
                pltpu.VMEM((HOPS, qrows, head), bf), pltpu.VMEM((HOPS, qrows, head), bf), pltpu.VMEM((HOPS, 2, qrows), f32),
                pltpu.VMEM((head, qrows), f32),
                pltpu.SMEM(cu_seqlens.shape, jnp.int32), dma((9,)), pltpu.SemaphoreType.REGULAR,
                dma((HOPS, NK)), dma((HOPS, NK)), dma((HOPS, NQ)), dma((HOPS, NQ)), dma((HOPS,)),
                dma((2,)), dma((2,)), dma((2,)), dma((HOPS,)), dma((HOPS,)), dma((HOPS,)),
            ],
            compiler_params=pltpu.CompilerParams(collective_id=0, has_side_effects=True),
        )(cu_seqlens, queries.reshape(qrows, head), keys, values, attn_out.reshape(qrows, head), logsumexp.T, d_out.reshape(qrows, head))
        d_query, d_key, d_value = pl.pallas_call(
            store_body,
            name="store",
            out_shape=tuple(jax.ShapeDtypeStruct(shape, bf) for shape in shapes),
            in_specs=[vmem_spec] * 3,
            out_specs=(any_spec,) * 3,
            scratch_shapes=[pltpu.VMEM((rows, head), bf), pltpu.VMEM((rows, head), bf), dma((3,))],
        )(*[pltpu.with_memory_space_constraint(x, pltpu.VMEM) for x in results])
        return d_query.reshape(rows, heads, head), d_key, d_value

    seq_spec = P(("dp", "cpo", "cp"))
    return jax.shard_map(local, mesh=mesh, in_specs=(seq_spec,) * 6 + (P("dp"),), out_specs=(seq_spec,) * 3, check_vma=False)
```

```python
import functools
import math

import jax
import jax.numpy as jnp
from jax import lax
from jax.experimental import pallas as pl
from jax.experimental.pallas import tpu as pltpu
from jax.sharding import PartitionSpec as P

MESH = pl.DeviceIdType.MESH
HOPS = 3
NK = 2
NQ = 4
NONE = 31
NOBODY = 63
SEND = 18

KV_OWN = {0: [(1, 1), (2, 2)], 1: [(3, 2), (4, 3)], 2: [(3, 1), (5, 3)], 3: [(6, 3)], 4: [(5, 1), (6, 2)], 5: [(7, 2)], 6: [(7, 1)], 7: []}
QD_OWN = {0: [], 1: [(0, 1)], 2: [(0, 2)], 3: [(2, 1), (1, 2)], 4: [(1, 3)], 5: [(4, 1), (3, 2)], 6: [(4, 2), (3, 3)], 7: [(6, 1), (5, 2)]}
FIRST = {
    0: (0, 10, 1, 11),
    1: (0, 1, 100),
    2: (0, 1, 100),
    3: (110, 100),
    4: (0, 10, 1, 11, 100),
    5: (0, 100),
    6: (0, 1, 100, 110),
    7: (110, 100),
}
REST = {
    1: (101, 102, 103),
    2: (),
    3: (101, 111, 102, 112, 103),
    4: (101, 102, 103),
    5: (110, 101, 1, 111, 112, 113, 102, 103),
    6: (111, 112, 113, 101),
    7: (101, 111, 102, 112, 103),
}
AFTER = {
    1: (10, 11),
    2: (10, 101, 102, 103, 11),
    3: (0, 1),
}
LATER = {
    3: (113,),
    6: (102, 103),
    7: (113,),
}
TAIL = (2, 3, 0, 0, 2, 3, 0, 0)
LATE_KEYS = 4
GO = ((4, 1), (5, 2), (6, 3))
KV_REL = {(2, 2): (3, 3), (3, 2): (2, 1), (5, 3): (4, 2), (4, 1): (5, 2), (6, 3): (4, 1), (6, 2): (7, 3), (7, 2): (6, 1)}
QD_REL = {(0, 2): (1, 1), (1, 2): (0, 3), (1, 3): (3, 1), (3, 1): (2, 2), (3, 2): (2, 3), (4, 2): (5, 1), (5, 2): (4, 3)}
ORDER = ("ghijkoplmqnr", "aobkpqlrghminj", "ghijcadbkolpmqnr", "abcedfsgkhlimjnopqr", "gheijkfolpcabmnqrd", "abkglhecdminfj", "ghijceafsdb", "abcefds")


def step_codes(letters):
    return [ord(x) - ord("a") for x in letters]


def targets_of(table, pick):
    pairs = [table.get(pick(d), NOBODY) for d in range(8)]
    return [p if p == NOBODY else p[0] * 4 + p[1] for p in pairs]


def partners():
    near = {d: set() for d in range(8)}
    pairs = [(d, target) for table in (KV_OWN, QD_OWN) for d in table for target, _ in table[d]]
    pairs += [(d, target) for table in (KV_REL, QD_REL) for (d, _), (target, _) in table.items()]
    for a, b in pairs:
        for here, there in ((a, b), (b, a)):
            if here >= 4 or there < 4:
                near[here].add(there)
    return near


def body(
    cu_hbm, q_hbm, k_hbm, v_hbm, o_hbm, lse_hbm, do_hbm,
    dq_out, dk_out, dv_out,
    q_loc, k_loc, v_loc, o_loc, lse_loc, do_loc, stat_loc, starts,
    k_buf, v_buf, q_buf, do_buf, stat_buf,
    dqt, dk_acc, dv_acc, cu_ref, in_sem, go_sem,
    k_recv, v_recv, q_recv, do_recv, stat_recv,
    kv_own, qd_own, stat_own, kv_rel, qd_rel, stat_rel,
):
    rows = k_loc.shape[0]
    qrows = q_loc.shape[0]
    head = k_loc.shape[1]
    kc_rows = rows // NK
    qc_rows = qrows // NQ
    scale = head ** -0.5
    factor = scale * math.log2(math.e)
    me = lax.axis_index("cpo") * 4 + lax.axis_index("cp")

    def lut(values):
        out = jnp.int32(values[0])
        for d in range(1, len(values)):
            out = jnp.where(me == d, jnp.int32(values[d]), out)
        return out

    def place(target):
        return {"cpo": target // 4, "cp": target % 4}

    loads = [
        pltpu.make_async_copy(src, dst, in_sem.at[i])
        for i, (src, dst) in enumerate(
            [
                (q_hbm.at[0:qc_rows], q_loc.at[0:qc_rows]), (do_hbm.at[0:qc_rows], do_loc.at[0:qc_rows]), (k_hbm, k_loc), (v_hbm, v_loc),
                (q_hbm.at[qc_rows:], q_loc.at[qc_rows:]), (do_hbm.at[qc_rows:], do_loc.at[qc_rows:]), (o_hbm, o_loc), (lse_hbm, lse_loc),
                (cu_hbm, cu_ref),
            ]
        )
    ]
    for load in loads:
        load.start()
    barrier = pltpu.get_barrier_semaphore()
    near = partners()
    for d in range(8):
        @pl.when(me == d)
        def _(d=d):
            for other in [x for x in range(8) if d in near[x]]:
                pl.semaphore_signal(barrier, inc=1, device_id=place(other), device_id_type=MESH)
    for d in range(8):
        @pl.when(me == d)
        def _(d=d):
            pl.semaphore_wait(barrier, len(near[d]))
            for teller, told in GO:
                if teller == d:
                    pl.semaphore_signal(go_sem, inc=1, device_id=place(told), device_id_type=MESH)

    def kv_copies(src_k, src_v, sem, code, chunk):
        target, there = code // 4, code % 4 - 1
        part = pl.ds(chunk * kc_rows, kc_rows)
        return [
            pltpu.make_async_remote_copy(
                src_ref=src.at[part], dst_ref=buf.at[there, part], send_sem=sem, recv_sem=recv.at[there, chunk],
                device_id=place(target), device_id_type=MESH)
            for src, buf, recv in ((src_k, k_buf, k_recv), (src_v, v_buf, v_recv))
        ]

    def qd_copies(src_q, src_do, sem, code, chunk):
        target, there = code // 4, code % 4 - 1
        part = pl.ds(chunk * qc_rows, qc_rows)
        return [
            pltpu.make_async_remote_copy(
                src_ref=src.at[part], dst_ref=buf.at[there, part], send_sem=sem, recv_sem=recv.at[there, chunk],
                device_id=place(target), device_id_type=MESH)
            for src, buf, recv in ((src_q, q_buf, q_recv), (src_do, do_buf, do_recv))
        ]

    def stat_copy(src, sem, code):
        target, there = code // 4, code % 4 - 1
        return pltpu.make_async_remote_copy(
            src_ref=src, dst_ref=stat_buf.at[there], send_sem=sem, recv_sem=stat_recv.at[there],
            device_id=place(target), device_id_type=MESH)

    def send(d, item):
        kind, n, chunk = item // 100, item // 10 % 10, item % 10
        target, there = (KV_OWN, QD_OWN)[kind][d][n]
        code = target * 4 + there
        if kind == 0:
            copies = kv_copies(k_loc, v_loc, kv_own.at[n], code, chunk)
        else:
            copies = qd_copies(q_loc, do_loc, qd_own.at[n], code, chunk)
        for copy in copies:
            copy.start()

    def send_stat(d, n):
        target, there = QD_OWN[d][n]
        stat_copy(stat_loc, stat_own.at[n], target * 4 + there).start()

    loads[0].wait()
    loads[1].wait()
    for d in range(8):
        @pl.when(me == d)
        def _(d=d):
            for item in FIRST[d]:
                if item >= 100:
                    send(d, item)
    loads[2].wait()
    loads[3].wait()
    for d in range(8):
        @pl.when(me == d)
        def _(d=d):
            for item in FIRST[d]:
                if item < 100:
                    send(d, item)
    for load in loads[4:8]:
        load.wait()

    wide = lax.broadcasted_iota(jnp.int32, (2, 128), 1)
    for j in range(qrows // 128):
        src = lse_loc[:, 128 * (j // 2):128 * (j // 2 + 1)]
        both = jnp.take_along_axis(src, 64 * (j % 2) + wide // 2, axis=1, mode="promise_in_bounds")
        row = jnp.where(wide[0:1] % 2 == 0, both[0:1], both[1:2])
        stat_loc[0:1, 128 * j:128 * (j + 1)] = row * math.log2(math.e)
    ones = jnp.ones((8, head), jnp.bfloat16)
    for j in range(qrows // 256):
        part = pl.ds(256 * j, 256)
        prod = do_loc[part].astype(jnp.float32) * o_loc[part].astype(jnp.float32)
        hi = prod.astype(jnp.bfloat16)
        lo = (prod - hi.astype(jnp.float32)).astype(jnp.bfloat16)
        dims = (((1,), (1,)), ((), ()))
        total = lax.dot_general(ones, hi, dims, preferred_element_type=jnp.float32)
        total = total + lax.dot_general(ones, lo, dims, preferred_element_type=jnp.float32)
        stat_loc[1:2, 256 * j:256 * (j + 1)] = total[0:1]
    for d in range(8):
        @pl.when(me == d)
        def _(d=d):
            for n in range(len(QD_OWN[d])):
                send_stat(d, n)
            for item in REST.get(d, ()):
                send(d, item)

    loads[8].wait()
    lane = lax.broadcasted_iota(jnp.int32, (1, qrows), 1) // 2
    for h in range(HOPS + 1):
        pos = lane + (me + h) * rows
        start = jnp.zeros_like(pos)
        for j in range(cu_ref.shape[0]):
            start = jnp.maximum(start, jnp.where(pos >= cu_ref[j], cu_ref[j], 0))
        starts[h] = start

    def send_later():
        for d in LATER:
            @pl.when(me == d)
            def _(d=d):
                for item in LATER[d]:
                    send(d, item)

    def block(k_blk, v_blk, q_blk, do_blk, lse_row, d_row, keep):
        dims = (((1,), (1,)), ((), ()))
        scores = lax.dot_general(k_blk, q_blk, dims, preferred_element_type=jnp.float32)
        p_mat = jnp.where(keep, jnp.exp2(scores * factor - lse_row), 0.0)
        dp_mat = lax.dot_general(v_blk, do_blk, dims, preferred_element_type=jnp.float32)
        ds_mat = (p_mat * (dp_mat - d_row)).astype(jnp.bfloat16)
        return p_mat.astype(jnp.bfloat16), ds_mat

    def dq_term(k_blk, ds_mat):
        return lax.dot_general(k_blk, ds_mat, (((0,), (0,)), ((), ())), preferred_element_type=jnp.float32)

    def key_iota(keys, width):
        return lax.broadcasted_iota(jnp.int32, (keys, width), 0)

    half = qrows // 2

    def own_half(first, keys):
        cols = pl.ds(first, half)
        q_blk, do_blk, k_blk = q_loc[cols], do_loc[cols], k_loc[0:keys]
        key_pos = key_iota(keys, half)
        tok = lax.broadcasted_iota(jnp.int32, (keys, half), 1) // 2 + first // 2
        keep = (key_pos >= starts[0, :, cols] - me * rows) & (key_pos <= tok)
        p_low, ds_mat = block(k_blk, v_loc[0:keys], q_blk, do_blk, stat_loc[0:1, cols], stat_loc[1:2, cols], keep)
        dqt[:, cols] = dq_term(k_blk, ds_mat)
        dv_new = jnp.dot(p_low, do_blk, preferred_element_type=jnp.float32)
        dk_new = jnp.dot(ds_mat, q_blk, preferred_element_type=jnp.float32)
        if keys == rows:
            dv_acc[...] = dv_new
            dk_acc[...] = dk_new
        else:
            dv_acc[0:keys] = dv_acc[0:keys] + dv_new
            dk_acc[0:keys] = dk_acc[0:keys] + dk_new

    own_half(half, rows)
    for d in AFTER:
        @pl.when(me == d)
        def _(d=d):
            pl.semaphore_wait(go_sem, 1)
            for item in AFTER[d]:
                send(d, item)
    own_half(0, rows // 2)

    def finish_dq():
        dq_out[...] = (jnp.transpose(dqt[...]) * scale).astype(jnp.bfloat16)

    def kv_block(slot, count, first_key, width):
        cols = pl.ds(0, count)
        keys = pl.ds(first_key, width)
        base = (me - 1 - slot) * rows + first_key
        keep = key_iota(width, count) >= starts[0, :, cols] - base
        k_blk = k_buf[slot, keys]
        _, ds_mat = block(k_blk, v_buf[slot, keys], q_loc[cols], do_loc[cols], stat_loc[0:1, cols], stat_loc[1:2, cols], keep)
        dqt[:, cols] = dqt[:, cols] + dq_term(k_blk, ds_mat)

    def kv_unit(slot, chunk):
        far = slot == HOPS - 1
        late = (slot == 1) & (me == LATE_KEYS)

        @pl.when(far & (chunk == 0))
        def _():
            kv_block(slot, half, 0, kc_rows)

        @pl.when(late & (chunk == 0))
        def _():
            kv_block(slot, qrows, 0, kc_rows)

        @pl.when((far | late) & (chunk == 1))
        def _():
            kv_block(slot, qrows, kc_rows, kc_rows)

        @pl.when(jnp.logical_not(far | late) & (chunk == 1))
        def _():
            kv_block(slot, qrows, 0, rows)

    def qd_block(slot, first_row, count, first_key):
        cols = pl.ds(pl.multiple_of(first_row, 128), count)
        keys = pl.ds(first_key, rows - first_key)
        q_blk = q_buf[slot, cols]
        do_blk = do_buf[slot, cols]
        keep = key_iota(rows - first_key, count) >= starts[slot + 1, :, cols] - (me * rows + first_key)
        p_low, ds_mat = block(k_loc[keys], v_loc[keys], q_blk, do_blk, stat_buf[slot, 0:1, cols], stat_buf[slot, 1:2, cols], keep)
        dv_acc[keys] = dv_acc[keys] + jnp.dot(p_low, do_blk, preferred_element_type=jnp.float32)
        dk_acc[keys] = dk_acc[keys] + jnp.dot(ds_mat, q_blk, preferred_element_type=jnp.float32)

    def qd_unit(slot, chunk):
        quarters = (pick(tail, slot) == 1) & (chunk >= 2)
        short = (slot == HOPS - 1) & (chunk == 3)

        @pl.when(quarters)
        def _():
            qd_block(slot, chunk * qc_rows, qc_rows, 0)

        @pl.when((chunk % 2 == 1) & jnp.logical_not(quarters) & jnp.logical_not(short))
        def _():
            qd_block(slot, (chunk - 1) * qc_rows, half, 0)

        @pl.when(short & jnp.logical_not(quarters))
        def _():
            qd_block(slot, half, half, rows // 2)

    tail = [lut([(t >> h) % 2 for t in TAIL]) for h in range(HOPS)]
    last_kv = lut([max([-1] + [i for i, c in enumerate(step_codes(ORDER[d])) if c < 3 * NK and d > c // NK]) for d in range(8)])

    @pl.when(me == 0)
    def _():
        finish_dq()

    kv_on = [lut(targets_of(KV_REL, lambda d, h=h: (d, h + 1))) for h in range(HOPS)]
    qd_on = [lut(targets_of(QD_REL, lambda d, h=h: (d, h + 1))) for h in range(HOPS)]

    def pick(values, slot):
        return jnp.where(slot == 0, values[0], jnp.where(slot == 1, values[1], values[2]))

    per_word = 6
    codes = {d: step_codes(ORDER[d]) for d in range(8)}
    steps = max(len(c) for c in codes.values())
    words = -(-steps // per_word)
    packed = []
    for w in range(words):
        values = []
        for d in range(8):
            part = (codes[d] + [NONE] * (words * per_word))[w * per_word:(w + 1) * per_word]
            values.append(sum(c * 32 ** i for i, c in enumerate(part)))
        packed.append(lut(values))

    def step(i, carry):
        code = carry[0] % 32

        @pl.when(code < 3 * NK)
        def _():
            slot, chunk = code // NK, code % NK
            to = pick(kv_on, slot)
            for copy in kv_copies(k_buf.at[slot], v_buf.at[slot], kv_rel.at[slot], me * 4 + slot + 1, chunk):
                copy.wait_recv()

            @pl.when(to != NOBODY)
            def _():
                for copy in kv_copies(k_buf.at[slot], v_buf.at[slot], kv_rel.at[slot], to, chunk):
                    copy.start()

            @pl.when(me > slot)
            def _():
                kv_unit(slot, chunk)

            @pl.when(i == last_kv)
            def _():
                finish_dq()

        @pl.when((code >= 3 * NK) & (code < SEND))
        def _():
            slot, chunk = (code - 3 * NK) // NQ, (code - 3 * NK) % NQ
            to = pick(qd_on, slot)
            for copy in qd_copies(q_buf.at[slot], do_buf.at[slot], qd_rel.at[slot], me * 4 + slot + 1, chunk):
                copy.wait_recv()

            @pl.when(to != NOBODY)
            def _():
                for copy in qd_copies(q_buf.at[slot], do_buf.at[slot], qd_rel.at[slot], to, chunk):
                    copy.start()

            @pl.when(chunk == 0)
            def _():
                stat_copy(stat_buf.at[slot], stat_rel.at[slot], me * 4 + slot + 1).wait_recv()

                @pl.when(to != NOBODY)
                def _():
                    stat_copy(stat_buf.at[slot], stat_rel.at[slot], to).start()

            @pl.when(me + slot < 7)
            def _():
                qd_unit(slot, chunk)

        @pl.when(code == SEND)
        def _():
            send_later()

        last = (i % per_word) == per_word - 1
        rest = [jnp.where(last, (carry + (jnp.int32(0),))[w + 1], carry[w] // 32 if w == 0 else carry[w]) for w in range(words)]
        return tuple(rest)

    lax.fori_loop(0, steps, step, tuple(packed))

    dk_out[...] = (dk_acc[...] * scale).astype(jnp.bfloat16)
    dv_out[...] = dv_acc[...].astype(jnp.bfloat16)

    def sent(ref, sem):
        pltpu.make_async_remote_copy(src_ref=ref, dst_ref=ref, send_sem=sem, recv_sem=sem, device_id=place(me), device_id_type=MESH).wait_send()

    for d in range(8):
        @pl.when(me == d)
        def _(d=d):
            keys_sent = [kv_own.at[n] for n in range(len(KV_OWN[d]))] + [kv_rel.at[h] for h in range(HOPS) if (d, h + 1) in KV_REL]
            queries_sent = [(qd_own.at[n], stat_own.at[n]) for n in range(len(QD_OWN[d]))]
            queries_sent += [(qd_rel.at[h], stat_rel.at[h]) for h in range(HOPS) if (d, h + 1) in QD_REL]
            for sem in keys_sent:
                sent(q_buf.at[0], sem)
            for sem, stat_sem in queries_sent:
                sent(q_buf.at[0:2], sem)
                sent(stat_loc, stat_sem)


def store_body(dq_ref, dk_ref, dv_ref, dq_out, dk_out, dv_out, sems):
    pairs = ((dq_ref, dq_out), (dk_ref, dk_out), (dv_ref, dv_out))
    copies = [pltpu.make_async_copy(src, dst, sems.at[i]) for i, (src, dst) in enumerate(pairs)]
    for copy in copies:
        copy.start()
    for copy in copies:
        copy.wait()


def solution(mesh):
    def local(queries, keys, values, attn_out, logsumexp, d_out, cu_seqlens):
        rows, heads, head = queries.shape
        qrows = rows * heads
        bf, f32 = jnp.bfloat16, jnp.float32
        dma = pltpu.SemaphoreType.DMA
        any_spec = pl.BlockSpec(memory_space=pl.ANY)
        vmem_spec = pl.BlockSpec(memory_space=pltpu.VMEM)
        shapes = ((qrows, head), (rows, head), (rows, head))
        results = pl.pallas_call(
            body,
            name="packed_backward",
            out_shape=tuple(pltpu.VMEM(shape, bf) for shape in shapes),
            in_specs=[any_spec] * 7,
            out_specs=(vmem_spec,) * 3,
            scratch_shapes=[
                pltpu.VMEM((qrows, head), bf), pltpu.VMEM((rows, head), bf), pltpu.VMEM((rows, head), bf),
                pltpu.VMEM((qrows, head), bf), pltpu.VMEM((heads, rows), f32), pltpu.VMEM((qrows, head), bf),
                pltpu.VMEM((2, qrows), f32), pltpu.VMEM((HOPS + 1, 1, qrows), jnp.int32),
                pltpu.VMEM((HOPS, rows, head), bf), pltpu.VMEM((HOPS, rows, head), bf),
                pltpu.VMEM((HOPS, qrows, head), bf), pltpu.VMEM((HOPS, qrows, head), bf), pltpu.VMEM((HOPS, 2, qrows), f32),
                pltpu.VMEM((head, qrows), f32), pltpu.VMEM((rows, head), f32), pltpu.VMEM((rows, head), f32),
                pltpu.SMEM(cu_seqlens.shape, jnp.int32), dma((9,)), pltpu.SemaphoreType.REGULAR,
                dma((HOPS, NK)), dma((HOPS, NK)), dma((HOPS, NQ)), dma((HOPS, NQ)), dma((HOPS,)),
                dma((2,)), dma((2,)), dma((2,)), dma((HOPS,)), dma((HOPS,)), dma((HOPS,)),
            ],
            compiler_params=pltpu.CompilerParams(collective_id=0, has_side_effects=True),
        )(cu_seqlens, queries.reshape(qrows, head), keys, values, attn_out.reshape(qrows, head), logsumexp.T, d_out.reshape(qrows, head))
        d_query, d_key, d_value = pl.pallas_call(
            store_body,
            name="store",
            out_shape=tuple(jax.ShapeDtypeStruct(shape, bf) for shape in shapes),
            in_specs=[vmem_spec] * 3,
            out_specs=(any_spec,) * 3,
            scratch_shapes=[dma((3,))],
        )(*[pltpu.with_memory_space_constraint(x, pltpu.VMEM) for x in results])
        return d_query.reshape(rows, heads, head), d_key, d_value

    seq_spec = P(("dp", "cpo", "cp"))
    return jax.shard_map(local, mesh=mesh, in_specs=(seq_spec,) * 6 + (P("dp"),), out_specs=(seq_spec,) * 3, check_vma=False)
```

```python
import functools
import math

import jax
import jax.numpy as jnp
from jax import lax
from jax.experimental import pallas as pl
from jax.experimental.pallas import tpu as pltpu
from jax.sharding import PartitionSpec as P

MESH = pl.DeviceIdType.MESH
HOPS = 3
NK = 2
NQ = 4
NONE = 31
NOBODY = 63
SEND = 18

KV_OWN = {0: [(1, 1), (2, 2)], 1: [(3, 2), (4, 3)], 2: [(3, 1), (5, 3)], 3: [(6, 3)], 4: [(5, 1), (6, 2)], 5: [(7, 2)], 6: [(7, 1)], 7: []}
QD_OWN = {0: [], 1: [(0, 1)], 2: [(0, 2)], 3: [(2, 1), (1, 2)], 4: [(1, 3)], 5: [(4, 1), (3, 2)], 6: [(4, 2), (3, 3)], 7: [(6, 1), (5, 2)]}
FIRST = {
    0: (0, 10, 1, 11),
    1: (0, 1, 100),
    2: (0, 1, 100),
    3: (110, 100),
    4: (0, 10, 1, 11, 100),
    5: (0, 100),
    6: (0, 1, 100, 110),
    7: (110, 100),
}
REST = {
    1: (101, 102, 103),
    2: (),
    3: (101, 111, 102, 112, 103),
    4: (101, 102, 103),
    5: (110, 101, 1, 111, 112, 113, 102, 103),
    6: (111, 112, 113, 101),
    7: (101, 111, 102, 112, 103),
}
AFTER = {
    1: (10, 11),
    2: (10, 101, 102, 103, 11),
    3: (0, 1),
}
LATER = {
    3: (113,),
    6: (102, 103),
    7: (113,),
}
TAIL = (2, 3, 0, 0, 2, 3, 0, 0)
LATE_KEYS = 4
GO = ((4, 1), (5, 2), (6, 3))
KV_REL = {(2, 2): (3, 3), (3, 2): (2, 1), (5, 3): (4, 2), (4, 1): (5, 2), (6, 3): (4, 1), (6, 2): (7, 3), (7, 2): (6, 1)}
QD_REL = {(0, 2): (1, 1), (1, 2): (0, 3), (1, 3): (3, 1), (3, 1): (2, 2), (3, 2): (2, 3), (4, 2): (5, 1), (5, 2): (4, 3)}
ORDER = ("ghijkoplmqnr", "aobkpqlrghminj", "ghijcadbkolpmqnr", "abcedfgkhslimjnopqr", "gheijkfolpcabmnqrd", "abkglhecdminfj", "ghijceafsdb", "abcefds")


def step_codes(letters):
    return [ord(x) - ord("a") for x in letters]


def targets_of(table, pick):
    pairs = [table.get(pick(d), NOBODY) for d in range(8)]
    return [p if p == NOBODY else p[0] * 4 + p[1] for p in pairs]


def partners():
    near = {d: set() for d in range(8)}
    pairs = [(d, target) for table in (KV_OWN, QD_OWN) for d in table for target, _ in table[d]]
    pairs += [(d, target) for table in (KV_REL, QD_REL) for (d, _), (target, _) in table.items()]
    for a, b in pairs:
        for here, there in ((a, b), (b, a)):
            if here >= 4 or there < 4:
                near[here].add(there)
    return near


def body(
    cu_hbm, q_hbm, k_hbm, v_hbm, o_hbm, lse_hbm, do_hbm,
    dq_out, dk_out, dv_out,
    q_loc, k_loc, v_loc, o_loc, lse_loc, do_loc, stat_loc, starts,
    k_buf, v_buf, q_buf, do_buf, stat_buf,
    dqt, dk_acc, dv_acc, cu_ref, in_sem, go_sem,
    k_recv, v_recv, q_recv, do_recv, stat_recv,
    kv_own, qd_own, stat_own, kv_rel, qd_rel, stat_rel,
):
    rows = k_loc.shape[0]
    qrows = q_loc.shape[0]
    head = k_loc.shape[1]
    kc_rows = rows // NK
    qc_rows = qrows // NQ
    scale = head ** -0.5
    factor = scale * math.log2(math.e)
    me = lax.axis_index("cpo") * 4 + lax.axis_index("cp")

    def lut(values):
        out = jnp.int32(values[0])
        for d in range(1, len(values)):
            out = jnp.where(me == d, jnp.int32(values[d]), out)
        return out

    def place(target):
        return {"cpo": target // 4, "cp": target % 4}

    loads = [
        pltpu.make_async_copy(src, dst, in_sem.at[i])
        for i, (src, dst) in enumerate(
            [
                (q_hbm.at[0:qc_rows], q_loc.at[0:qc_rows]), (do_hbm.at[0:qc_rows], do_loc.at[0:qc_rows]), (k_hbm, k_loc), (v_hbm, v_loc),
                (q_hbm.at[qc_rows:], q_loc.at[qc_rows:]), (do_hbm.at[qc_rows:], do_loc.at[qc_rows:]), (o_hbm, o_loc), (lse_hbm, lse_loc),
                (cu_hbm, cu_ref),
            ]
        )
    ]
    for load in loads:
        load.start()
    barrier = pltpu.get_barrier_semaphore()
    near = partners()
    for d in range(8):
        @pl.when(me == d)
        def _(d=d):
            for other in [x for x in range(8) if d in near[x]]:
                pl.semaphore_signal(barrier, inc=1, device_id=place(other), device_id_type=MESH)
    for d in range(8):
        @pl.when(me == d)
        def _(d=d):
            pl.semaphore_wait(barrier, len(near[d]))
            for teller, told in GO:
                if teller == d:
                    pl.semaphore_signal(go_sem, inc=1, device_id=place(told), device_id_type=MESH)

    def kv_copies(src_k, src_v, sem, code, chunk):
        target, there = code // 4, code % 4 - 1
        part = pl.ds(chunk * kc_rows, kc_rows)
        return [
            pltpu.make_async_remote_copy(
                src_ref=src.at[part], dst_ref=buf.at[there, part], send_sem=sem, recv_sem=recv.at[there, chunk],
                device_id=place(target), device_id_type=MESH)
            for src, buf, recv in ((src_k, k_buf, k_recv), (src_v, v_buf, v_recv))
        ]

    def qd_copies(src_q, src_do, sem, code, chunk):
        target, there = code // 4, code % 4 - 1
        part = pl.ds(chunk * qc_rows, qc_rows)
        return [
            pltpu.make_async_remote_copy(
                src_ref=src.at[part], dst_ref=buf.at[there, part], send_sem=sem, recv_sem=recv.at[there, chunk],
                device_id=place(target), device_id_type=MESH)
            for src, buf, recv in ((src_q, q_buf, q_recv), (src_do, do_buf, do_recv))
        ]

    def stat_copy(src, sem, code):
        target, there = code // 4, code % 4 - 1
        return pltpu.make_async_remote_copy(
            src_ref=src, dst_ref=stat_buf.at[there], send_sem=sem, recv_sem=stat_recv.at[there],
            device_id=place(target), device_id_type=MESH)

    def send(d, item):
        kind, n, chunk = item // 100, item // 10 % 10, item % 10
        target, there = (KV_OWN, QD_OWN)[kind][d][n]
        code = target * 4 + there
        if kind == 0:
            copies = kv_copies(k_loc, v_loc, kv_own.at[n], code, chunk)
        else:
            copies = qd_copies(q_loc, do_loc, qd_own.at[n], code, chunk)
        for copy in copies:
            copy.start()

    def send_stat(d, n):
        target, there = QD_OWN[d][n]
        stat_copy(stat_loc, stat_own.at[n], target * 4 + there).start()

    loads[0].wait()
    loads[1].wait()
    for d in range(8):
        @pl.when(me == d)
        def _(d=d):
            for item in FIRST[d]:
                if item >= 100:
                    send(d, item)
    loads[2].wait()
    loads[3].wait()
    for d in range(8):
        @pl.when(me == d)
        def _(d=d):
            for item in FIRST[d]:
                if item < 100:
                    send(d, item)
    for load in loads[4:8]:
        load.wait()

    wide = lax.broadcasted_iota(jnp.int32, (2, 128), 1)
    for j in range(qrows // 128):
        src = lse_loc[:, 128 * (j // 2):128 * (j // 2 + 1)]
        both = jnp.take_along_axis(src, 64 * (j % 2) + wide // 2, axis=1, mode="promise_in_bounds")
        row = jnp.where(wide[0:1] % 2 == 0, both[0:1], both[1:2])
        stat_loc[0:1, 128 * j:128 * (j + 1)] = row * math.log2(math.e)
    ones = jnp.ones((8, head), jnp.bfloat16)
    for j in range(qrows // 256):
        part = pl.ds(256 * j, 256)
        prod = do_loc[part].astype(jnp.float32) * o_loc[part].astype(jnp.float32)
        hi = prod.astype(jnp.bfloat16)
        lo = (prod - hi.astype(jnp.float32)).astype(jnp.bfloat16)
        dims = (((1,), (1,)), ((), ()))
        total = lax.dot_general(ones, hi, dims, preferred_element_type=jnp.float32)
        total = total + lax.dot_general(ones, lo, dims, preferred_element_type=jnp.float32)
        stat_loc[1:2, 256 * j:256 * (j + 1)] = total[0:1]
    for d in range(8):
        @pl.when(me == d)
        def _(d=d):
            for n in range(len(QD_OWN[d])):
                send_stat(d, n)
            for item in REST.get(d, ()):
                send(d, item)

    loads[8].wait()
    lane = lax.broadcasted_iota(jnp.int32, (1, qrows), 1) // 2
    for h in range(HOPS + 1):
        pos = lane + (me + h) * rows
        start = jnp.zeros_like(pos)
        for j in range(cu_ref.shape[0]):
            start = jnp.maximum(start, jnp.where(pos >= cu_ref[j], cu_ref[j], 0))
        starts[h] = start

    def send_later():
        for d in LATER:
            @pl.when(me == d)
            def _(d=d):
                for item in LATER[d]:
                    send(d, item)

    def block(k_blk, v_blk, q_blk, do_blk, lse_row, d_row, keep):
        dims = (((1,), (1,)), ((), ()))
        scores = lax.dot_general(k_blk, q_blk, dims, preferred_element_type=jnp.float32)
        p_mat = jnp.where(keep, jnp.exp2(scores * factor - lse_row), 0.0)
        dp_mat = lax.dot_general(v_blk, do_blk, dims, preferred_element_type=jnp.float32)
        ds_mat = (p_mat * (dp_mat - d_row)).astype(jnp.bfloat16)
        return p_mat.astype(jnp.bfloat16), ds_mat

    def dq_term(k_blk, ds_mat):
        return lax.dot_general(k_blk, ds_mat, (((0,), (0,)), ((), ())), preferred_element_type=jnp.float32)

    def key_iota(keys, width):
        return lax.broadcasted_iota(jnp.int32, (keys, width), 0)

    half = qrows // 2

    def own_half(first, keys):
        cols = pl.ds(first, half)
        q_blk, do_blk, k_blk = q_loc[cols], do_loc[cols], k_loc[0:keys]
        key_pos = key_iota(keys, half)
        tok = lax.broadcasted_iota(jnp.int32, (keys, half), 1) // 2 + first // 2
        keep = (key_pos >= starts[0, :, cols] - me * rows) & (key_pos <= tok)
        p_low, ds_mat = block(k_blk, v_loc[0:keys], q_blk, do_blk, stat_loc[0:1, cols], stat_loc[1:2, cols], keep)
        dqt[:, cols] = dq_term(k_blk, ds_mat)
        dv_new = jnp.dot(p_low, do_blk, preferred_element_type=jnp.float32)
        dk_new = jnp.dot(ds_mat, q_blk, preferred_element_type=jnp.float32)
        if keys == rows:
            dv_acc[...] = dv_new
            dk_acc[...] = dk_new
        else:
            dv_acc[0:keys] = dv_acc[0:keys] + dv_new
            dk_acc[0:keys] = dk_acc[0:keys] + dk_new

    own_half(half, rows)
    for d in AFTER:
        @pl.when(me == d)
        def _(d=d):
            pl.semaphore_wait(go_sem, 1)
            for item in AFTER[d]:
                send(d, item)
    own_half(0, rows // 2)

    def finish_dq():
        dq_out[...] = (jnp.transpose(dqt[...]) * scale).astype(jnp.bfloat16)

    def kv_block(slot, count, first_key, width):
        cols = pl.ds(0, count)
        keys = pl.ds(first_key, width)
        base = (me - 1 - slot) * rows + first_key
        keep = key_iota(width, count) >= starts[0, :, cols] - base
        k_blk = k_buf[slot, keys]
        _, ds_mat = block(k_blk, v_buf[slot, keys], q_loc[cols], do_loc[cols], stat_loc[0:1, cols], stat_loc[1:2, cols], keep)
        dqt[:, cols] = dqt[:, cols] + dq_term(k_blk, ds_mat)

    def kv_unit(slot, chunk):
        far = slot == HOPS - 1
        late = (slot == 1) & (me == LATE_KEYS)

        @pl.when(far & (chunk == 0))
        def _():
            kv_block(slot, half, 0, kc_rows)

        @pl.when(late & (chunk == 0))
        def _():
            kv_block(slot, qrows, 0, kc_rows)

        @pl.when((far | late) & (chunk == 1))
        def _():
            kv_block(slot, qrows, kc_rows, kc_rows)

        @pl.when(jnp.logical_not(far | late) & (chunk == 1))
        def _():
            kv_block(slot, qrows, 0, rows)

    def qd_block(slot, first_row, count, first_key):
        cols = pl.ds(pl.multiple_of(first_row, 128), count)
        keys = pl.ds(first_key, rows - first_key)
        q_blk = q_buf[slot, cols]
        do_blk = do_buf[slot, cols]
        keep = key_iota(rows - first_key, count) >= starts[slot + 1, :, cols] - (me * rows + first_key)
        p_low, ds_mat = block(k_loc[keys], v_loc[keys], q_blk, do_blk, stat_buf[slot, 0:1, cols], stat_buf[slot, 1:2, cols], keep)
        dv_acc[keys] = dv_acc[keys] + jnp.dot(p_low, do_blk, preferred_element_type=jnp.float32)
        dk_acc[keys] = dk_acc[keys] + jnp.dot(ds_mat, q_blk, preferred_element_type=jnp.float32)

    def qd_unit(slot, chunk):
        quarters = (pick(tail, slot) == 1) & (chunk >= 2)
        short = (slot == HOPS - 1) & (chunk == 3)

        @pl.when(quarters)
        def _():
            qd_block(slot, chunk * qc_rows, qc_rows, 0)

        @pl.when((chunk % 2 == 1) & jnp.logical_not(quarters) & jnp.logical_not(short))
        def _():
            qd_block(slot, (chunk - 1) * qc_rows, half, 0)

        @pl.when(short & jnp.logical_not(quarters))
        def _():
            qd_block(slot, half, half, rows // 2)

    tail = [lut([(t >> h) % 2 for t in TAIL]) for h in range(HOPS)]
    last_kv = lut([max([-1] + [i for i, c in enumerate(step_codes(ORDER[d])) if c < 3 * NK and d > c // NK]) for d in range(8)])

    @pl.when(me == 0)
    def _():
        finish_dq()

    kv_on = [lut(targets_of(KV_REL, lambda d, h=h: (d, h + 1))) for h in range(HOPS)]
    qd_on = [lut(targets_of(QD_REL, lambda d, h=h: (d, h + 1))) for h in range(HOPS)]

    def pick(values, slot):
        return jnp.where(slot == 0, values[0], jnp.where(slot == 1, values[1], values[2]))

    per_word = 6
    codes = {d: step_codes(ORDER[d]) for d in range(8)}
    steps = max(len(c) for c in codes.values())
    words = -(-steps // per_word)
    packed = []
    for w in range(words):
        values = []
        for d in range(8):
            part = (codes[d] + [NONE] * (words * per_word))[w * per_word:(w + 1) * per_word]
            values.append(sum(c * 32 ** i for i, c in enumerate(part)))
        packed.append(lut(values))

    def step(i, carry):
        code = carry[0] % 32

        @pl.when(code < 3 * NK)
        def _():
            slot, chunk = code // NK, code % NK
            to = pick(kv_on, slot)
            for copy in kv_copies(k_buf.at[slot], v_buf.at[slot], kv_rel.at[slot], me * 4 + slot + 1, chunk):
                copy.wait_recv()

            @pl.when(to != NOBODY)
            def _():
                for copy in kv_copies(k_buf.at[slot], v_buf.at[slot], kv_rel.at[slot], to, chunk):
                    copy.start()

            @pl.when(me > slot)
            def _():
                kv_unit(slot, chunk)

            @pl.when(i == last_kv)
            def _():
                finish_dq()

        @pl.when((code >= 3 * NK) & (code < SEND))
        def _():
            slot, chunk = (code - 3 * NK) // NQ, (code - 3 * NK) % NQ
            to = pick(qd_on, slot)
            for copy in qd_copies(q_buf.at[slot], do_buf.at[slot], qd_rel.at[slot], me * 4 + slot + 1, chunk):
                copy.wait_recv()

            @pl.when(to != NOBODY)
            def _():
                for copy in qd_copies(q_buf.at[slot], do_buf.at[slot], qd_rel.at[slot], to, chunk):
                    copy.start()

            @pl.when(chunk == 0)
            def _():
                stat_copy(stat_buf.at[slot], stat_rel.at[slot], me * 4 + slot + 1).wait_recv()

                @pl.when(to != NOBODY)
                def _():
                    stat_copy(stat_buf.at[slot], stat_rel.at[slot], to).start()

            @pl.when(me + slot < 7)
            def _():
                qd_unit(slot, chunk)

        @pl.when(code == SEND)
        def _():
            send_later()

        last = (i % per_word) == per_word - 1
        rest = [jnp.where(last, (carry + (jnp.int32(0),))[w + 1], carry[w] // 32 if w == 0 else carry[w]) for w in range(words)]
        return tuple(rest)

    lax.fori_loop(0, steps, step, tuple(packed))

    dk_out[...] = (dk_acc[...] * scale).astype(jnp.bfloat16)
    dv_out[...] = dv_acc[...].astype(jnp.bfloat16)

    def sent(ref, sem):
        pltpu.make_async_remote_copy(src_ref=ref, dst_ref=ref, send_sem=sem, recv_sem=sem, device_id=place(me), device_id_type=MESH).wait_send()

    for d in range(8):
        @pl.when(me == d)
        def _(d=d):
            keys_sent = [kv_own.at[n] for n in range(len(KV_OWN[d]))] + [kv_rel.at[h] for h in range(HOPS) if (d, h + 1) in KV_REL]
            queries_sent = [(qd_own.at[n], stat_own.at[n]) for n in range(len(QD_OWN[d]))]
            queries_sent += [(qd_rel.at[h], stat_rel.at[h]) for h in range(HOPS) if (d, h + 1) in QD_REL]
            for sem in keys_sent:
                sent(q_buf.at[0], sem)
            for sem, stat_sem in queries_sent:
                sent(q_buf.at[0:2], sem)
                sent(stat_loc, stat_sem)


def store_body(dq_ref, dk_ref, dv_ref, dq_out, dk_out, dv_out, sems):
    pairs = ((dq_ref, dq_out), (dk_ref, dk_out), (dv_ref, dv_out))
    copies = [pltpu.make_async_copy(src, dst, sems.at[i]) for i, (src, dst) in enumerate(pairs)]
    for copy in copies:
        copy.start()
    for copy in copies:
        copy.wait()


def solution(mesh):
    def local(queries, keys, values, attn_out, logsumexp, d_out, cu_seqlens):
        rows, heads, head = queries.shape
        qrows = rows * heads
        bf, f32 = jnp.bfloat16, jnp.float32
        dma = pltpu.SemaphoreType.DMA
        any_spec = pl.BlockSpec(memory_space=pl.ANY)
        vmem_spec = pl.BlockSpec(memory_space=pltpu.VMEM)
        shapes = ((qrows, head), (rows, head), (rows, head))
        results = pl.pallas_call(
            body,
            name="packed_backward",
            out_shape=tuple(pltpu.VMEM(shape, bf) for shape in shapes),
            in_specs=[any_spec] * 7,
            out_specs=(vmem_spec,) * 3,
            scratch_shapes=[
                pltpu.VMEM((qrows, head), bf), pltpu.VMEM((rows, head), bf), pltpu.VMEM((rows, head), bf),
                pltpu.VMEM((qrows, head), bf), pltpu.VMEM((heads, rows), f32), pltpu.VMEM((qrows, head), bf),
                pltpu.VMEM((2, qrows), f32), pltpu.VMEM((HOPS + 1, 1, qrows), jnp.int32),
                pltpu.VMEM((HOPS, rows, head), bf), pltpu.VMEM((HOPS, rows, head), bf),
                pltpu.VMEM((HOPS, qrows, head), bf), pltpu.VMEM((HOPS, qrows, head), bf), pltpu.VMEM((HOPS, 2, qrows), f32),
                pltpu.VMEM((head, qrows), f32), pltpu.VMEM((rows, head), f32), pltpu.VMEM((rows, head), f32),
                pltpu.SMEM(cu_seqlens.shape, jnp.int32), dma((9,)), pltpu.SemaphoreType.REGULAR,
                dma((HOPS, NK)), dma((HOPS, NK)), dma((HOPS, NQ)), dma((HOPS, NQ)), dma((HOPS,)),
                dma((2,)), dma((2,)), dma((2,)), dma((HOPS,)), dma((HOPS,)), dma((HOPS,)),
            ],
            compiler_params=pltpu.CompilerParams(collective_id=0, has_side_effects=True),
        )(cu_seqlens, queries.reshape(qrows, head), keys, values, attn_out.reshape(qrows, head), logsumexp.T, d_out.reshape(qrows, head))
        d_query, d_key, d_value = pl.pallas_call(
            store_body,
            name="store",
            out_shape=tuple(jax.ShapeDtypeStruct(shape, bf) for shape in shapes),
            in_specs=[vmem_spec] * 3,
            out_specs=(any_spec,) * 3,
            scratch_shapes=[dma((3,))],
        )(*[pltpu.with_memory_space_constraint(x, pltpu.VMEM) for x in results])
        return d_query.reshape(rows, heads, head), d_key, d_value

    seq_spec = P(("dp", "cpo", "cp"))
    return jax.shard_map(local, mesh=mesh, in_specs=(seq_spec,) * 6 + (P("dp"),), out_specs=(seq_spec,) * 3, check_vma=False)
```

```python
import functools
import math

import jax
import jax.numpy as jnp
from jax import lax
from jax.experimental import pallas as pl
from jax.experimental.pallas import tpu as pltpu
from jax.sharding import PartitionSpec as P

MESH = pl.DeviceIdType.MESH
HOPS = 3
NK = 2
NQ = 4
NONE = 31
NOBODY = 63
SEND = 18

KV_OWN = {0: [(1, 1), (2, 2)], 1: [(3, 2), (4, 3)], 2: [(3, 1), (5, 3)], 3: [(6, 3)], 4: [(5, 1), (6, 2)], 5: [(7, 2)], 6: [(7, 1)], 7: []}
QD_OWN = {0: [], 1: [(0, 1)], 2: [(0, 2)], 3: [(2, 1), (1, 2)], 4: [(1, 3)], 5: [(4, 1), (3, 2)], 6: [(4, 2), (3, 3)], 7: [(6, 1), (5, 2)]}
FIRST = {
    0: (0, 10, 1, 11),
    1: (0, 1, 100),
    2: (0, 1, 100),
    3: (110, 100),
    4: (0, 10, 1, 11, 100),
    5: (0, 100),
    6: (0, 1, 100, 110),
    7: (110, 100),
}
REST = {
    1: (101, 102, 103),
    2: (),
    3: (101, 111, 102, 112, 103),
    4: (101, 102, 103),
    5: (110, 101, 1, 111, 112, 113, 102, 103),
    6: (111, 112, 113, 101),
    7: (101, 111, 102, 112, 103),
}
AFTER = {
    1: (10, 11),
    2: (10, 101, 102, 103, 11),
    3: (0, 1),
}
LATER = {
    3: (113,),
    6: (102, 103),
    7: (113,),
}
TAIL = (2, 3, 0, 0, 2, 3, 0, 0)
LATE_KEYS = 4
GO = ((4, 1), (5, 2), (6, 3))
KV_REL = {(2, 2): (3, 3), (3, 2): (2, 1), (5, 3): (4, 2), (4, 1): (5, 2), (6, 3): (4, 1), (6, 2): (7, 3), (7, 2): (6, 1)}
QD_REL = {(0, 2): (1, 1), (1, 2): (0, 3), (1, 3): (3, 1), (3, 1): (2, 2), (3, 2): (2, 3), (4, 2): (5, 1), (5, 2): (4, 3)}
ORDER = ("ghijkoplmqnr", "aobkpqlrghminj", "ghijcadbkolpmqnr", "abcedfsgkhlimjnopqr", "gheijkfolpcabmnqdr", "abkglhecdmifnj", "ghijceafsdb", "abcefds")


def step_codes(letters):
    return [ord(x) - ord("a") for x in letters]


def targets_of(table, pick):
    pairs = [table.get(pick(d), NOBODY) for d in range(8)]
    return [p if p == NOBODY else p[0] * 4 + p[1] for p in pairs]


def partners():
    near = {d: set() for d in range(8)}
    pairs = [(d, target) for table in (KV_OWN, QD_OWN) for d in table for target, _ in table[d]]
    pairs += [(d, target) for table in (KV_REL, QD_REL) for (d, _), (target, _) in table.items()]
    for a, b in pairs:
        for here, there in ((a, b), (b, a)):
            if here >= 4 or there < 4:
                near[here].add(there)
    return near


def body(
    cu_hbm, q_hbm, k_hbm, v_hbm, o_hbm, lse_hbm, do_hbm,
    dq_out, dk_out, dv_out,
    q_loc, k_loc, v_loc, o_loc, lse_loc, do_loc, stat_loc, starts,
    k_buf, v_buf, q_buf, do_buf, stat_buf,
    dqt, dk_acc, dv_acc, cu_ref, in_sem, go_sem,
    k_recv, v_recv, q_recv, do_recv, stat_recv,
    kv_own, qd_own, stat_own, kv_rel, qd_rel, stat_rel,
):
    rows = k_loc.shape[0]
    qrows = q_loc.shape[0]
    head = k_loc.shape[1]
    kc_rows = rows // NK
    qc_rows = qrows // NQ
    scale = head ** -0.5
    factor = scale * math.log2(math.e)
    me = lax.axis_index("cpo") * 4 + lax.axis_index("cp")

    def lut(values):
        out = jnp.int32(values[0])
        for d in range(1, len(values)):
            out = jnp.where(me == d, jnp.int32(values[d]), out)
        return out

    def place(target):
        return {"cpo": target // 4, "cp": target % 4}

    loads = [
        pltpu.make_async_copy(src, dst, in_sem.at[i])
        for i, (src, dst) in enumerate(
            [
                (q_hbm.at[0:qc_rows], q_loc.at[0:qc_rows]), (do_hbm.at[0:qc_rows], do_loc.at[0:qc_rows]), (k_hbm, k_loc), (v_hbm, v_loc),
                (q_hbm.at[qc_rows:], q_loc.at[qc_rows:]), (do_hbm.at[qc_rows:], do_loc.at[qc_rows:]), (o_hbm, o_loc), (lse_hbm, lse_loc),
                (cu_hbm, cu_ref),
            ]
        )
    ]
    for load in loads:
        load.start()
    barrier = pltpu.get_barrier_semaphore()
    near = partners()
    for d in range(8):
        @pl.when(me == d)
        def _(d=d):
            for other in [x for x in range(8) if d in near[x]]:
                pl.semaphore_signal(barrier, inc=1, device_id=place(other), device_id_type=MESH)
    for d in range(8):
        @pl.when(me == d)
        def _(d=d):
            pl.semaphore_wait(barrier, len(near[d]))
            for teller, told in GO:
                if teller == d:
                    pl.semaphore_signal(go_sem, inc=1, device_id=place(told), device_id_type=MESH)

    def kv_copies(src_k, src_v, sem, code, chunk):
        target, there = code // 4, code % 4 - 1
        part = pl.ds(chunk * kc_rows, kc_rows)
        return [
            pltpu.make_async_remote_copy(
                src_ref=src.at[part], dst_ref=buf.at[there, part], send_sem=sem, recv_sem=recv.at[there, chunk],
                device_id=place(target), device_id_type=MESH)
            for src, buf, recv in ((src_k, k_buf, k_recv), (src_v, v_buf, v_recv))
        ]

    def qd_copies(src_q, src_do, sem, code, chunk):
        target, there = code // 4, code % 4 - 1
        part = pl.ds(chunk * qc_rows, qc_rows)
        return [
            pltpu.make_async_remote_copy(
                src_ref=src.at[part], dst_ref=buf.at[there, part], send_sem=sem, recv_sem=recv.at[there, chunk],
                device_id=place(target), device_id_type=MESH)
            for src, buf, recv in ((src_q, q_buf, q_recv), (src_do, do_buf, do_recv))
        ]

    def stat_copy(src, sem, code):
        target, there = code // 4, code % 4 - 1
        return pltpu.make_async_remote_copy(
            src_ref=src, dst_ref=stat_buf.at[there], send_sem=sem, recv_sem=stat_recv.at[there],
            device_id=place(target), device_id_type=MESH)

    def send(d, item):
        kind, n, chunk = item // 100, item // 10 % 10, item % 10
        target, there = (KV_OWN, QD_OWN)[kind][d][n]
        code = target * 4 + there
        if kind == 0:
            copies = kv_copies(k_loc, v_loc, kv_own.at[n], code, chunk)
        else:
            copies = qd_copies(q_loc, do_loc, qd_own.at[n], code, chunk)
        for copy in copies:
            copy.start()

    def send_stat(d, n):
        target, there = QD_OWN[d][n]
        stat_copy(stat_loc, stat_own.at[n], target * 4 + there).start()

    loads[0].wait()
    loads[1].wait()
    for d in range(8):
        @pl.when(me == d)
        def _(d=d):
            for item in FIRST[d]:
                if item >= 100:
                    send(d, item)
    loads[2].wait()
    loads[3].wait()
    for d in range(8):
        @pl.when(me == d)
        def _(d=d):
            for item in FIRST[d]:
                if item < 100:
                    send(d, item)
    for load in loads[4:8]:
        load.wait()

    wide = lax.broadcasted_iota(jnp.int32, (2, 128), 1)
    for j in range(qrows // 128):
        src = lse_loc[:, 128 * (j // 2):128 * (j // 2 + 1)]
        both = jnp.take_along_axis(src, 64 * (j % 2) + wide // 2, axis=1, mode="promise_in_bounds")
        row = jnp.where(wide[0:1] % 2 == 0, both[0:1], both[1:2])
        stat_loc[0:1, 128 * j:128 * (j + 1)] = row * math.log2(math.e)
    ones = jnp.ones((8, head), jnp.bfloat16)
    for j in range(qrows // 256):
        part = pl.ds(256 * j, 256)
        prod = do_loc[part].astype(jnp.float32) * o_loc[part].astype(jnp.float32)
        hi = prod.astype(jnp.bfloat16)
        lo = (prod - hi.astype(jnp.float32)).astype(jnp.bfloat16)
        dims = (((1,), (1,)), ((), ()))
        total = lax.dot_general(ones, hi, dims, preferred_element_type=jnp.float32)
        total = total + lax.dot_general(ones, lo, dims, preferred_element_type=jnp.float32)
        stat_loc[1:2, 256 * j:256 * (j + 1)] = total[0:1]
    for d in range(8):
        @pl.when(me == d)
        def _(d=d):
            for n in range(len(QD_OWN[d])):
                send_stat(d, n)
            for item in REST.get(d, ()):
                send(d, item)

    loads[8].wait()
    lane = lax.broadcasted_iota(jnp.int32, (1, qrows), 1) // 2
    for h in range(HOPS + 1):
        pos = lane + (me + h) * rows
        start = jnp.zeros_like(pos)
        for j in range(cu_ref.shape[0]):
            start = jnp.maximum(start, jnp.where(pos >= cu_ref[j], cu_ref[j], 0))
        starts[h] = start

    def send_later():
        for d in LATER:
            @pl.when(me == d)
            def _(d=d):
                for item in LATER[d]:
                    send(d, item)

    def block(k_blk, v_blk, q_blk, do_blk, lse_row, d_row, keep):
        dims = (((1,), (1,)), ((), ()))
        scores = lax.dot_general(k_blk, q_blk, dims, preferred_element_type=jnp.float32)
        p_mat = jnp.where(keep, jnp.exp2(scores * factor - lse_row), 0.0)
        dp_mat = lax.dot_general(v_blk, do_blk, dims, preferred_element_type=jnp.float32)
        ds_mat = (p_mat * (dp_mat - d_row)).astype(jnp.bfloat16)
        return p_mat.astype(jnp.bfloat16), ds_mat

    def dq_term(k_blk, ds_mat):
        return lax.dot_general(k_blk, ds_mat, (((0,), (0,)), ((), ())), preferred_element_type=jnp.float32)

    def key_iota(keys, width):
        return lax.broadcasted_iota(jnp.int32, (keys, width), 0)

    half = qrows // 2

    def own_half(first, keys):
        cols = pl.ds(first, half)
        q_blk, do_blk, k_blk = q_loc[cols], do_loc[cols], k_loc[0:keys]
        key_pos = key_iota(keys, half)
        tok = lax.broadcasted_iota(jnp.int32, (keys, half), 1) // 2 + first // 2
        keep = (key_pos >= starts[0, :, cols] - me * rows) & (key_pos <= tok)
        p_low, ds_mat = block(k_blk, v_loc[0:keys], q_blk, do_blk, stat_loc[0:1, cols], stat_loc[1:2, cols], keep)
        dqt[:, cols] = dq_term(k_blk, ds_mat)
        dv_new = jnp.dot(p_low, do_blk, preferred_element_type=jnp.float32)
        dk_new = jnp.dot(ds_mat, q_blk, preferred_element_type=jnp.float32)
        if keys == rows:
            dv_acc[...] = dv_new
            dk_acc[...] = dk_new
        else:
            dv_acc[0:keys] = dv_acc[0:keys] + dv_new
            dk_acc[0:keys] = dk_acc[0:keys] + dk_new

    own_half(half, rows)
    for d in AFTER:
        @pl.when(me == d)
        def _(d=d):
            pl.semaphore_wait(go_sem, 1)
            for item in AFTER[d]:
                send(d, item)
    own_half(0, rows // 2)

    def finish_dq():
        dq_out[...] = (jnp.transpose(dqt[...]) * scale).astype(jnp.bfloat16)

    def kv_block(slot, count, first_key, width):
        cols = pl.ds(0, count)
        keys = pl.ds(first_key, width)
        base = (me - 1 - slot) * rows + first_key
        keep = key_iota(width, count) >= starts[0, :, cols] - base
        k_blk = k_buf[slot, keys]
        _, ds_mat = block(k_blk, v_buf[slot, keys], q_loc[cols], do_loc[cols], stat_loc[0:1, cols], stat_loc[1:2, cols], keep)
        dqt[:, cols] = dqt[:, cols] + dq_term(k_blk, ds_mat)

    def kv_unit(slot, chunk):
        far = slot == HOPS - 1
        late = (slot == 1) & (me == LATE_KEYS)

        @pl.when(far & (chunk == 0))
        def _():
            kv_block(slot, half, 0, kc_rows)

        @pl.when(late & (chunk == 0))
        def _():
            kv_block(slot, qrows, 0, kc_rows)

        @pl.when((far | late) & (chunk == 1))
        def _():
            kv_block(slot, qrows, kc_rows, kc_rows)

        @pl.when(jnp.logical_not(far | late) & (chunk == 1))
        def _():
            kv_block(slot, qrows, 0, rows)

    def qd_block(slot, first_row, count, first_key):
        cols = pl.ds(pl.multiple_of(first_row, 128), count)
        keys = pl.ds(first_key, rows - first_key)
        q_blk = q_buf[slot, cols]
        do_blk = do_buf[slot, cols]
        keep = key_iota(rows - first_key, count) >= starts[slot + 1, :, cols] - (me * rows + first_key)
        p_low, ds_mat = block(k_loc[keys], v_loc[keys], q_blk, do_blk, stat_buf[slot, 0:1, cols], stat_buf[slot, 1:2, cols], keep)
        dv_acc[keys] = dv_acc[keys] + jnp.dot(p_low, do_blk, preferred_element_type=jnp.float32)
        dk_acc[keys] = dk_acc[keys] + jnp.dot(ds_mat, q_blk, preferred_element_type=jnp.float32)

    def qd_unit(slot, chunk):
        quarters = (pick(tail, slot) == 1) & (chunk >= 2)
        short = (slot == HOPS - 1) & (chunk == 3)

        @pl.when(quarters)
        def _():
            qd_block(slot, chunk * qc_rows, qc_rows, 0)

        @pl.when((chunk % 2 == 1) & jnp.logical_not(quarters) & jnp.logical_not(short))
        def _():
            qd_block(slot, (chunk - 1) * qc_rows, half, 0)

        @pl.when(short & jnp.logical_not(quarters))
        def _():
            qd_block(slot, half, half, rows // 2)

    tail = [lut([(t >> h) % 2 for t in TAIL]) for h in range(HOPS)]
    last_kv = lut([max([-1] + [i for i, c in enumerate(step_codes(ORDER[d])) if c < 3 * NK and d > c // NK]) for d in range(8)])

    @pl.when(me == 0)
    def _():
        finish_dq()

    kv_on = [lut(targets_of(KV_REL, lambda d, h=h: (d, h + 1))) for h in range(HOPS)]
    qd_on = [lut(targets_of(QD_REL, lambda d, h=h: (d, h + 1))) for h in range(HOPS)]

    def pick(values, slot):
        return jnp.where(slot == 0, values[0], jnp.where(slot == 1, values[1], values[2]))

    per_word = 6
    codes = {d: step_codes(ORDER[d]) for d in range(8)}
    steps = max(len(c) for c in codes.values())
    words = -(-steps // per_word)
    packed = []
    for w in range(words):
        values = []
        for d in range(8):
            part = (codes[d] + [NONE] * (words * per_word))[w * per_word:(w + 1) * per_word]
            values.append(sum(c * 32 ** i for i, c in enumerate(part)))
        packed.append(lut(values))

    def step(i, carry):
        code = carry[0] % 32

        @pl.when(code < 3 * NK)
        def _():
            slot, chunk = code // NK, code % NK
            to = pick(kv_on, slot)
            for copy in kv_copies(k_buf.at[slot], v_buf.at[slot], kv_rel.at[slot], me * 4 + slot + 1, chunk):
                copy.wait_recv()

            @pl.when(to != NOBODY)
            def _():
                for copy in kv_copies(k_buf.at[slot], v_buf.at[slot], kv_rel.at[slot], to, chunk):
                    copy.start()

            @pl.when(me > slot)
            def _():
                kv_unit(slot, chunk)

            @pl.when(i == last_kv)
            def _():
                finish_dq()

        @pl.when((code >= 3 * NK) & (code < SEND))
        def _():
            slot, chunk = (code - 3 * NK) // NQ, (code - 3 * NK) % NQ
            to = pick(qd_on, slot)
            for copy in qd_copies(q_buf.at[slot], do_buf.at[slot], qd_rel.at[slot], me * 4 + slot + 1, chunk):
                copy.wait_recv()

            @pl.when(to != NOBODY)
            def _():
                for copy in qd_copies(q_buf.at[slot], do_buf.at[slot], qd_rel.at[slot], to, chunk):
                    copy.start()

            @pl.when(chunk == 0)
            def _():
                stat_copy(stat_buf.at[slot], stat_rel.at[slot], me * 4 + slot + 1).wait_recv()

                @pl.when(to != NOBODY)
                def _():
                    stat_copy(stat_buf.at[slot], stat_rel.at[slot], to).start()

            @pl.when(me + slot < 7)
            def _():
                qd_unit(slot, chunk)

        @pl.when(code == SEND)
        def _():
            send_later()

        last = (i % per_word) == per_word - 1
        rest = [jnp.where(last, (carry + (jnp.int32(0),))[w + 1], carry[w] // 32 if w == 0 else carry[w]) for w in range(words)]
        return tuple(rest)

    lax.fori_loop(0, steps, step, tuple(packed))

    dk_out[...] = (dk_acc[...] * scale).astype(jnp.bfloat16)
    dv_out[...] = dv_acc[...].astype(jnp.bfloat16)

    def sent(ref, sem):
        pltpu.make_async_remote_copy(src_ref=ref, dst_ref=ref, send_sem=sem, recv_sem=sem, device_id=place(me), device_id_type=MESH).wait_send()

    for d in range(8):
        @pl.when(me == d)
        def _(d=d):
            keys_sent = [kv_own.at[n] for n in range(len(KV_OWN[d]))] + [kv_rel.at[h] for h in range(HOPS) if (d, h + 1) in KV_REL]
            queries_sent = [(qd_own.at[n], stat_own.at[n]) for n in range(len(QD_OWN[d]))]
            queries_sent += [(qd_rel.at[h], stat_rel.at[h]) for h in range(HOPS) if (d, h + 1) in QD_REL]
            for sem in keys_sent:
                sent(q_buf.at[0], sem)
            for sem, stat_sem in queries_sent:
                sent(q_buf.at[0:2], sem)
                sent(stat_loc, stat_sem)


def store_body(dq_ref, dk_ref, dv_ref, dq_out, dk_out, dv_out, sems):
    pairs = ((dq_ref, dq_out), (dk_ref, dk_out), (dv_ref, dv_out))
    copies = [pltpu.make_async_copy(src, dst, sems.at[i]) for i, (src, dst) in enumerate(pairs)]
    for copy in copies:
        copy.start()
    for copy in copies:
        copy.wait()


def solution(mesh):
    def local(queries, keys, values, attn_out, logsumexp, d_out, cu_seqlens):
        rows, heads, head = queries.shape
        qrows = rows * heads
        bf, f32 = jnp.bfloat16, jnp.float32
        dma = pltpu.SemaphoreType.DMA
        any_spec = pl.BlockSpec(memory_space=pl.ANY)
        vmem_spec = pl.BlockSpec(memory_space=pltpu.VMEM)
        shapes = ((qrows, head), (rows, head), (rows, head))
        results = pl.pallas_call(
            body,
            name="packed_backward",
            out_shape=tuple(pltpu.VMEM(shape, bf) for shape in shapes),
            in_specs=[any_spec] * 7,
            out_specs=(vmem_spec,) * 3,
            scratch_shapes=[
                pltpu.VMEM((qrows, head), bf), pltpu.VMEM((rows, head), bf), pltpu.VMEM((rows, head), bf),
                pltpu.VMEM((qrows, head), bf), pltpu.VMEM((heads, rows), f32), pltpu.VMEM((qrows, head), bf),
                pltpu.VMEM((2, qrows), f32), pltpu.VMEM((HOPS + 1, 1, qrows), jnp.int32),
                pltpu.VMEM((HOPS, rows, head), bf), pltpu.VMEM((HOPS, rows, head), bf),
                pltpu.VMEM((HOPS, qrows, head), bf), pltpu.VMEM((HOPS, qrows, head), bf), pltpu.VMEM((HOPS, 2, qrows), f32),
                pltpu.VMEM((head, qrows), f32), pltpu.VMEM((rows, head), f32), pltpu.VMEM((rows, head), f32),
                pltpu.SMEM(cu_seqlens.shape, jnp.int32), dma((9,)), pltpu.SemaphoreType.REGULAR,
                dma((HOPS, NK)), dma((HOPS, NK)), dma((HOPS, NQ)), dma((HOPS, NQ)), dma((HOPS,)),
                dma((2,)), dma((2,)), dma((2,)), dma((HOPS,)), dma((HOPS,)), dma((HOPS,)),
            ],
            compiler_params=pltpu.CompilerParams(collective_id=0, has_side_effects=True),
        )(cu_seqlens, queries.reshape(qrows, head), keys, values, attn_out.reshape(qrows, head), logsumexp.T, d_out.reshape(qrows, head))
        d_query, d_key, d_value = pl.pallas_call(
            store_body,
            name="store",
            out_shape=tuple(jax.ShapeDtypeStruct(shape, bf) for shape in shapes),
            in_specs=[vmem_spec] * 3,
            out_specs=(any_spec,) * 3,
            scratch_shapes=[dma((3,))],
        )(*[pltpu.with_memory_space_constraint(x, pltpu.VMEM) for x in results])
        return d_query.reshape(rows, heads, head), d_key, d_value

    seq_spec = P(("dp", "cpo", "cp"))
    return jax.shard_map(local, mesh=mesh, in_specs=(seq_spec,) * 6 + (P("dp"),), out_specs=(seq_spec,) * 3, check_vma=False)
```

```python
import functools
import math

import jax
import jax.numpy as jnp
from jax import lax
from jax.experimental import pallas as pl
from jax.experimental.pallas import tpu as pltpu
from jax.sharding import PartitionSpec as P

MESH = pl.DeviceIdType.MESH
HOPS = 3
NK = 2
NQ = 4
NONE = 31
NOBODY = 63
SEND = 18

KV_OWN = {0: [(1, 1), (2, 2)], 1: [(3, 2), (4, 3)], 2: [(3, 1), (5, 3)], 3: [(6, 3)], 4: [(5, 1), (6, 2)], 5: [(7, 2)], 6: [(7, 1)], 7: []}
QD_OWN = {0: [], 1: [(0, 1)], 2: [(0, 2)], 3: [(2, 1), (1, 2)], 4: [(1, 3)], 5: [(4, 1), (3, 2)], 6: [(4, 2), (3, 3)], 7: [(6, 1), (5, 2)]}
FIRST = {
    0: (0, 10, 1, 11),
    1: (0, 1, 100),
    2: (0, 1, 100),
    3: (110, 100),
    4: (0, 10, 1, 11, 100),
    5: (0, 100),
    6: (0, 1, 100, 110),
    7: (110, 100),
}
REST = {
    1: (101, 102, 103),
    2: (),
    3: (101, 111, 102, 112, 103),
    4: (101, 102, 103),
    5: (110, 101, 1, 111, 112, 113, 102, 103),
    6: (111, 112, 113, 101),
    7: (101, 111, 102, 112, 103),
}
AFTER = {
    1: (10, 11),
    2: (10, 101, 102, 103, 11),
    3: (0, 1),
}
LATER = {
    3: (113,),
    6: (102, 103),
    7: (113,),
}
TAIL = (2, 3, 0, 0, 2, 3, 0, 0)
LATE_KEYS = 4
GO = ((4, 1), (5, 2), (6, 3))
KV_REL = {(2, 2): (3, 3), (3, 2): (2, 1), (5, 3): (4, 2), (4, 1): (5, 2), (6, 3): (4, 1), (6, 2): (7, 3), (7, 2): (6, 1)}
QD_REL = {(0, 2): (1, 1), (1, 2): (0, 3), (1, 3): (3, 1), (3, 1): (2, 2), (3, 2): (2, 3), (4, 2): (5, 1), (5, 2): (4, 3)}
ORDER = ("ghijkoplmqnr", "aobkpqlrghminj", "ghijcadbkolpmqnr", "abcedfsgkhlimjnopqr", "gheijkfolpcabmnqdr", "abkglhecdmifnj", "ghijceafsdb", "abcefsd")


def step_codes(letters):
    return [ord(x) - ord("a") for x in letters]


def targets_of(table, pick):
    pairs = [table.get(pick(d), NOBODY) for d in range(8)]
    return [p if p == NOBODY else p[0] * 4 + p[1] for p in pairs]


def partners():
    near = {d: set() for d in range(8)}
    pairs = [(d, target) for table in (KV_OWN, QD_OWN) for d in table for target, _ in table[d]]
    pairs += [(d, target) for table in (KV_REL, QD_REL) for (d, _), (target, _) in table.items()]
    for a, b in pairs:
        for here, there in ((a, b), (b, a)):
            if here >= 4 or there < 4:
                near[here].add(there)
    return near


def body(
    cu_hbm, q_hbm, k_hbm, v_hbm, o_hbm, lse_hbm, do_hbm,
    dq_out, dk_out, dv_out,
    q_loc, k_loc, v_loc, o_loc, lse_loc, do_loc, stat_loc, starts,
    k_buf, v_buf, q_buf, do_buf, stat_buf,
    dqt, dk_acc, dv_acc, cu_ref, in_sem, go_sem,
    k_recv, v_recv, q_recv, do_recv, stat_recv,
    kv_own, qd_own, stat_own, kv_rel, qd_rel, stat_rel,
):
    rows = k_loc.shape[0]
    qrows = q_loc.shape[0]
    head = k_loc.shape[1]
    kc_rows = rows // NK
    qc_rows = qrows // NQ
    scale = head ** -0.5
    factor = scale * math.log2(math.e)
    me = lax.axis_index("cpo") * 4 + lax.axis_index("cp")

    def lut(values):
        out = jnp.int32(values[0])
        for d in range(1, len(values)):
            out = jnp.where(me == d, jnp.int32(values[d]), out)
        return out

    def place(target):
        return {"cpo": target // 4, "cp": target % 4}

    loads = [
        pltpu.make_async_copy(src, dst, in_sem.at[i])
        for i, (src, dst) in enumerate(
            [
                (q_hbm.at[0:qc_rows], q_loc.at[0:qc_rows]), (do_hbm.at[0:qc_rows], do_loc.at[0:qc_rows]), (k_hbm, k_loc), (v_hbm, v_loc),
                (q_hbm.at[qc_rows:], q_loc.at[qc_rows:]), (do_hbm.at[qc_rows:], do_loc.at[qc_rows:]), (o_hbm, o_loc), (lse_hbm, lse_loc),
                (cu_hbm, cu_ref),
            ]
        )
    ]
    for load in loads:
        load.start()
    barrier = pltpu.get_barrier_semaphore()
    near = partners()
    for d in range(8):
        @pl.when(me == d)
        def _(d=d):
            for other in [x for x in range(8) if d in near[x]]:
                pl.semaphore_signal(barrier, inc=1, device_id=place(other), device_id_type=MESH)
    for d in range(8):
        @pl.when(me == d)
        def _(d=d):
            pl.semaphore_wait(barrier, len(near[d]))
            for teller, told in GO:
                if teller == d:
                    pl.semaphore_signal(go_sem, inc=1, device_id=place(told), device_id_type=MESH)

    def kv_copies(src_k, src_v, sem, code, chunk):
        target, there = code // 4, code % 4 - 1
        part = pl.ds(chunk * kc_rows, kc_rows)
        return [
            pltpu.make_async_remote_copy(
                src_ref=src.at[part], dst_ref=buf.at[there, part], send_sem=sem, recv_sem=recv.at[there, chunk],
                device_id=place(target), device_id_type=MESH)
            for src, buf, recv in ((src_k, k_buf, k_recv), (src_v, v_buf, v_recv))
        ]

    def qd_copies(src_q, src_do, sem, code, chunk):
        target, there = code // 4, code % 4 - 1
        part = pl.ds(chunk * qc_rows, qc_rows)
        return [
            pltpu.make_async_remote_copy(
                src_ref=src.at[part], dst_ref=buf.at[there, part], send_sem=sem, recv_sem=recv.at[there, chunk],
                device_id=place(target), device_id_type=MESH)
            for src, buf, recv in ((src_q, q_buf, q_recv), (src_do, do_buf, do_recv))
        ]

    def stat_copy(src, sem, code):
        target, there = code // 4, code % 4 - 1
        return pltpu.make_async_remote_copy(
            src_ref=src, dst_ref=stat_buf.at[there], send_sem=sem, recv_sem=stat_recv.at[there],
            device_id=place(target), device_id_type=MESH)

    def send(d, item):
        kind, n, chunk = item // 100, item // 10 % 10, item % 10
        target, there = (KV_OWN, QD_OWN)[kind][d][n]
        code = target * 4 + there
        if kind == 0:
            copies = kv_copies(k_loc, v_loc, kv_own.at[n], code, chunk)
        else:
            copies = qd_copies(q_loc, do_loc, qd_own.at[n], code, chunk)
        for copy in copies:
            copy.start()

    def send_stat(d, n):
        target, there = QD_OWN[d][n]
        stat_copy(stat_loc, stat_own.at[n], target * 4 + there).start()

    loads[0].wait()
    loads[1].wait()
    for d in range(8):
        @pl.when(me == d)
        def _(d=d):
            for item in FIRST[d]:
                if item >= 100:
                    send(d, item)
    loads[2].wait()
    loads[3].wait()
    for d in range(8):
        @pl.when(me == d)
        def _(d=d):
            for item in FIRST[d]:
                if item < 100:
                    send(d, item)
    for load in loads[4:8]:
        load.wait()

    wide = lax.broadcasted_iota(jnp.int32, (2, 128), 1)
    for j in range(qrows // 128):
        src = lse_loc[:, 128 * (j // 2):128 * (j // 2 + 1)]
        both = jnp.take_along_axis(src, 64 * (j % 2) + wide // 2, axis=1, mode="promise_in_bounds")
        row = jnp.where(wide[0:1] % 2 == 0, both[0:1], both[1:2])
        stat_loc[0:1, 128 * j:128 * (j + 1)] = row * math.log2(math.e)
    ones = jnp.ones((8, head), jnp.bfloat16)
    for j in range(qrows // 256):
        part = pl.ds(256 * j, 256)
        prod = do_loc[part].astype(jnp.float32) * o_loc[part].astype(jnp.float32)
        hi = prod.astype(jnp.bfloat16)
        lo = (prod - hi.astype(jnp.float32)).astype(jnp.bfloat16)
        dims = (((1,), (1,)), ((), ()))
        total = lax.dot_general(ones, hi, dims, preferred_element_type=jnp.float32)
        total = total + lax.dot_general(ones, lo, dims, preferred_element_type=jnp.float32)
        stat_loc[1:2, 256 * j:256 * (j + 1)] = total[0:1]
    for d in range(8):
        @pl.when(me == d)
        def _(d=d):
            for n in range(len(QD_OWN[d])):
                send_stat(d, n)
            for item in REST.get(d, ()):
                send(d, item)

    loads[8].wait()
    lane = lax.broadcasted_iota(jnp.int32, (1, qrows), 1) // 2
    for h in range(HOPS + 1):
        pos = lane + (me + h) * rows
        start = jnp.zeros_like(pos)
        for j in range(cu_ref.shape[0]):
            start = jnp.maximum(start, jnp.where(pos >= cu_ref[j], cu_ref[j], 0))
        starts[h] = start

    def send_later():
        for d in LATER:
            @pl.when(me == d)
            def _(d=d):
                for item in LATER[d]:
                    send(d, item)

    def block(k_blk, v_blk, q_blk, do_blk, lse_row, d_row, keep):
        dims = (((1,), (1,)), ((), ()))
        scores = lax.dot_general(k_blk, q_blk, dims, preferred_element_type=jnp.float32)
        p_mat = jnp.where(keep, jnp.exp2(scores * factor - lse_row), 0.0)
        dp_mat = lax.dot_general(v_blk, do_blk, dims, preferred_element_type=jnp.float32)
        ds_mat = (p_mat * (dp_mat - d_row)).astype(jnp.bfloat16)
        return p_mat.astype(jnp.bfloat16), ds_mat

    def dq_term(k_blk, ds_mat):
        return lax.dot_general(k_blk, ds_mat, (((0,), (0,)), ((), ())), preferred_element_type=jnp.float32)

    def key_iota(keys, width):
        return lax.broadcasted_iota(jnp.int32, (keys, width), 0)

    half = qrows // 2

    def own_half(first, keys):
        cols = pl.ds(first, half)
        q_blk, do_blk, k_blk = q_loc[cols], do_loc[cols], k_loc[0:keys]
        key_pos = key_iota(keys, half)
        tok = lax.broadcasted_iota(jnp.int32, (keys, half), 1) // 2 + first // 2
        keep = (key_pos >= starts[0, :, cols] - me * rows) & (key_pos <= tok)
        p_low, ds_mat = block(k_blk, v_loc[0:keys], q_blk, do_blk, stat_loc[0:1, cols], stat_loc[1:2, cols], keep)
        dqt[:, cols] = dq_term(k_blk, ds_mat)
        dv_new = jnp.dot(p_low, do_blk, preferred_element_type=jnp.float32)
        dk_new = jnp.dot(ds_mat, q_blk, preferred_element_type=jnp.float32)
        if keys == rows:
            dv_acc[...] = dv_new
            dk_acc[...] = dk_new
        else:
            dv_acc[0:keys] = dv_acc[0:keys] + dv_new
            dk_acc[0:keys] = dk_acc[0:keys] + dk_new

    own_half(half, rows)
    for d in AFTER:
        @pl.when(me == d)
        def _(d=d):
            pl.semaphore_wait(go_sem, 1)
            for item in AFTER[d]:
                send(d, item)
    own_half(0, rows // 2)

    def finish_dq():
        dq_out[...] = (jnp.transpose(dqt[...]) * scale).astype(jnp.bfloat16)

    def kv_block(slot, count, first_key, width):
        cols = pl.ds(0, count)
        keys = pl.ds(first_key, width)
        base = (me - 1 - slot) * rows + first_key
        keep = key_iota(width, count) >= starts[0, :, cols] - base
        k_blk = k_buf[slot, keys]
        _, ds_mat = block(k_blk, v_buf[slot, keys], q_loc[cols], do_loc[cols], stat_loc[0:1, cols], stat_loc[1:2, cols], keep)
        dqt[:, cols] = dqt[:, cols] + dq_term(k_blk, ds_mat)

    def kv_unit(slot, chunk):
        far = slot == HOPS - 1
        late = (slot == 1) & (me == LATE_KEYS)

        @pl.when(far & (chunk == 0))
        def _():
            kv_block(slot, half, 0, kc_rows)

        @pl.when(late & (chunk == 0))
        def _():
            kv_block(slot, qrows, 0, kc_rows)

        @pl.when((far | late) & (chunk == 1))
        def _():
            kv_block(slot, qrows, kc_rows, kc_rows)

        @pl.when(jnp.logical_not(far | late) & (chunk == 1))
        def _():
            kv_block(slot, qrows, 0, rows)

    def qd_block(slot, first_row, count, first_key):
        cols = pl.ds(pl.multiple_of(first_row, 128), count)
        keys = pl.ds(first_key, rows - first_key)
        q_blk = q_buf[slot, cols]
        do_blk = do_buf[slot, cols]
        keep = key_iota(rows - first_key, count) >= starts[slot + 1, :, cols] - (me * rows + first_key)
        p_low, ds_mat = block(k_loc[keys], v_loc[keys], q_blk, do_blk, stat_buf[slot, 0:1, cols], stat_buf[slot, 1:2, cols], keep)
        dv_acc[keys] = dv_acc[keys] + jnp.dot(p_low, do_blk, preferred_element_type=jnp.float32)
        dk_acc[keys] = dk_acc[keys] + jnp.dot(ds_mat, q_blk, preferred_element_type=jnp.float32)

    def qd_unit(slot, chunk):
        quarters = (pick(tail, slot) == 1) & (chunk >= 2)
        short = (slot == HOPS - 1) & (chunk == 3)

        @pl.when(quarters)
        def _():
            qd_block(slot, chunk * qc_rows, qc_rows, 0)

        @pl.when((chunk % 2 == 1) & jnp.logical_not(quarters) & jnp.logical_not(short))
        def _():
            qd_block(slot, (chunk - 1) * qc_rows, half, 0)

        @pl.when(short & jnp.logical_not(quarters))
        def _():
            qd_block(slot, half, half, rows // 2)

    tail = [lut([(t >> h) % 2 for t in TAIL]) for h in range(HOPS)]
    last_kv = lut([max([-1] + [i for i, c in enumerate(step_codes(ORDER[d])) if c < 3 * NK and d > c // NK]) for d in range(8)])

    @pl.when(me == 0)
    def _():
        finish_dq()

    kv_on = [lut(targets_of(KV_REL, lambda d, h=h: (d, h + 1))) for h in range(HOPS)]
    qd_on = [lut(targets_of(QD_REL, lambda d, h=h: (d, h + 1))) for h in range(HOPS)]

    def pick(values, slot):
        return jnp.where(slot == 0, values[0], jnp.where(slot == 1, values[1], values[2]))

    per_word = 6
    codes = {d: step_codes(ORDER[d]) for d in range(8)}
    steps = max(len(c) for c in codes.values())
    words = -(-steps // per_word)
    packed = []
    for w in range(words):
        values = []
        for d in range(8):
            part = (codes[d] + [NONE] * (words * per_word))[w * per_word:(w + 1) * per_word]
            values.append(sum(c * 32 ** i for i, c in enumerate(part)))
        packed.append(lut(values))

    def step(i, carry):
        code = carry[0] % 32

        @pl.when(code < 3 * NK)
        def _():
            slot, chunk = code // NK, code % NK
            to = pick(kv_on, slot)
            for copy in kv_copies(k_buf.at[slot], v_buf.at[slot], kv_rel.at[slot], me * 4 + slot + 1, chunk):
                copy.wait_recv()

            @pl.when(to != NOBODY)
            def _():
                for copy in kv_copies(k_buf.at[slot], v_buf.at[slot], kv_rel.at[slot], to, chunk):
                    copy.start()

            @pl.when(me > slot)
            def _():
                kv_unit(slot, chunk)

            @pl.when(i == last_kv)
            def _():
                finish_dq()

        @pl.when((code >= 3 * NK) & (code < SEND))
        def _():
            slot, chunk = (code - 3 * NK) // NQ, (code - 3 * NK) % NQ
            to = pick(qd_on, slot)
            for copy in qd_copies(q_buf.at[slot], do_buf.at[slot], qd_rel.at[slot], me * 4 + slot + 1, chunk):
                copy.wait_recv()

            @pl.when(to != NOBODY)
            def _():
                for copy in qd_copies(q_buf.at[slot], do_buf.at[slot], qd_rel.at[slot], to, chunk):
                    copy.start()

            @pl.when(chunk == 0)
            def _():
                stat_copy(stat_buf.at[slot], stat_rel.at[slot], me * 4 + slot + 1).wait_recv()

                @pl.when(to != NOBODY)
                def _():
                    stat_copy(stat_buf.at[slot], stat_rel.at[slot], to).start()

            @pl.when(me + slot < 7)
            def _():
                qd_unit(slot, chunk)

        @pl.when(code == SEND)
        def _():
            send_later()

        last = (i % per_word) == per_word - 1
        rest = [jnp.where(last, (carry + (jnp.int32(0),))[w + 1], carry[w] // 32 if w == 0 else carry[w]) for w in range(words)]
        return tuple(rest)

    lax.fori_loop(0, steps, step, tuple(packed))

    dk_out[...] = (dk_acc[...] * scale).astype(jnp.bfloat16)
    dv_out[...] = dv_acc[...].astype(jnp.bfloat16)

    def sent(ref, sem):
        pltpu.make_async_remote_copy(src_ref=ref, dst_ref=ref, send_sem=sem, recv_sem=sem, device_id=place(me), device_id_type=MESH).wait_send()

    for d in range(8):
        @pl.when(me == d)
        def _(d=d):
            keys_sent = [kv_own.at[n] for n in range(len(KV_OWN[d]))] + [kv_rel.at[h] for h in range(HOPS) if (d, h + 1) in KV_REL]
            queries_sent = [(qd_own.at[n], stat_own.at[n]) for n in range(len(QD_OWN[d]))]
            queries_sent += [(qd_rel.at[h], stat_rel.at[h]) for h in range(HOPS) if (d, h + 1) in QD_REL]
            for sem in keys_sent:
                sent(q_buf.at[0], sem)
            for sem, stat_sem in queries_sent:
                sent(q_buf.at[0:2], sem)
                sent(stat_loc, stat_sem)


def store_body(dq_ref, dk_ref, dv_ref, dq_out, dk_out, dv_out, sems):
    pairs = ((dq_ref, dq_out), (dk_ref, dk_out), (dv_ref, dv_out))
    copies = [pltpu.make_async_copy(src, dst, sems.at[i]) for i, (src, dst) in enumerate(pairs)]
    for copy in copies:
        copy.start()
    for copy in copies:
        copy.wait()


def solution(mesh):
    def local(queries, keys, values, attn_out, logsumexp, d_out, cu_seqlens):
        rows, heads, head = queries.shape
        qrows = rows * heads
        bf, f32 = jnp.bfloat16, jnp.float32
        dma = pltpu.SemaphoreType.DMA
        any_spec = pl.BlockSpec(memory_space=pl.ANY)
        vmem_spec = pl.BlockSpec(memory_space=pltpu.VMEM)
        shapes = ((qrows, head), (rows, head), (rows, head))
        results = pl.pallas_call(
            body,
            name="packed_backward",
            out_shape=tuple(pltpu.VMEM(shape, bf) for shape in shapes),
            in_specs=[any_spec] * 7,
            out_specs=(vmem_spec,) * 3,
            scratch_shapes=[
                pltpu.VMEM((qrows, head), bf), pltpu.VMEM((rows, head), bf), pltpu.VMEM((rows, head), bf),
                pltpu.VMEM((qrows, head), bf), pltpu.VMEM((heads, rows), f32), pltpu.VMEM((qrows, head), bf),
                pltpu.VMEM((2, qrows), f32), pltpu.VMEM((HOPS + 1, 1, qrows), jnp.int32),
                pltpu.VMEM((HOPS, rows, head), bf), pltpu.VMEM((HOPS, rows, head), bf),
                pltpu.VMEM((HOPS, qrows, head), bf), pltpu.VMEM((HOPS, qrows, head), bf), pltpu.VMEM((HOPS, 2, qrows), f32),
                pltpu.VMEM((head, qrows), f32), pltpu.VMEM((rows, head), f32), pltpu.VMEM((rows, head), f32),
                pltpu.SMEM(cu_seqlens.shape, jnp.int32), dma((9,)), pltpu.SemaphoreType.REGULAR,
                dma((HOPS, NK)), dma((HOPS, NK)), dma((HOPS, NQ)), dma((HOPS, NQ)), dma((HOPS,)),
                dma((2,)), dma((2,)), dma((2,)), dma((HOPS,)), dma((HOPS,)), dma((HOPS,)),
            ],
            compiler_params=pltpu.CompilerParams(collective_id=0, has_side_effects=True),
        )(cu_seqlens, queries.reshape(qrows, head), keys, values, attn_out.reshape(qrows, head), logsumexp.T, d_out.reshape(qrows, head))
        d_query, d_key, d_value = pl.pallas_call(
            store_body,
            name="store",
            out_shape=tuple(jax.ShapeDtypeStruct(shape, bf) for shape in shapes),
            in_specs=[vmem_spec] * 3,
            out_specs=(any_spec,) * 3,
            scratch_shapes=[dma((3,))],
        )(*[pltpu.with_memory_space_constraint(x, pltpu.VMEM) for x in results])
        return d_query.reshape(rows, heads, head), d_key, d_value

    seq_spec = P(("dp", "cpo", "cp"))
    return jax.shard_map(local, mesh=mesh, in_specs=(seq_spec,) * 6 + (P("dp"),), out_specs=(seq_spec,) * 3, check_vma=False)
```
